16 devices in a mesh: grp: 4 (over z, y), data: 4 (over x, core).
Axes of the slice: x: 2, y: 2, z: 2, core: 2. Of those that a mesh axis runs over, the one named last changes fastest.
Arguments:
- hidden: bfloat16 [1024, 768], P(('grp', 'data')), parts along dimension 0
- w_qkv: bfloat16 [4, 768, 1280], replicated
- w_out: bfloat16 [4, 768, 768], replicated
- norm_attn: float32 [4, 768], replicated
- norm_ffn: float32 [4, 768], replicated
- k_cache: bfloat16 [4, 1024, 256, 2, 128], P(None, ('grp', 'data')), parts along dimension 1
- v_cache: bfloat16 [4, 1024, 256, 2, 128], P(None, ('grp', 'data')), parts along dimension 1
- seq_lens: int32 [1024], P(('grp', 'data')), parts along dimension 0
- w_gate: bfloat16 [4, 768, 2048], P('data')
- w_up: bfloat16 [4, 768, 2048], P('data')
- w_down: bfloat16 [4, 2048, 768], P('data')
Outputs:
- output: bfloat16 [1024, 768], P(('grp', 'data')), parts along dimension 0
There are 4 independent parts. The reference program is written for one: setup_inputs(seed, part) draws one part's arguments, and reference() takes and returns one part's arrays. A program takes and returns all parts, laid end to end along the dimension named above; an argument that names none is the same for every part.
All inputs are finite; a program needn't handle non-finite values.
Results may differ from the reference program's by a relative error of at most 0.02.
Values are sent between devices in bfloat16 or wider.
A program may use at most 1 GiB of HBM per device.

```python
import jax
import jax.numpy as jnp
from jax import lax

D_MODEL = 768
FFN_DIM = 2048
NUM_HEADS = 6
KV_HEADS = 2
HEAD_DIM = 128
TOK_DEV = 64
CACHE_LEN = 256
LAYERS_DEV = 1
GROUP_DEVS = 4

LAYERS = LAYERS_DEV * GROUP_DEVS
TOKENS = GROUP_DEVS * TOK_DEV
NORM_EPS = 1e-5


def rms_norm(tok_rows, gain_vec):
    row_vals = tok_rows.astype(jnp.float32)
    inv_rms = lax.rsqrt(jnp.mean(row_vals * row_vals, axis=-1, keepdims=True) + NORM_EPS)
    return (row_vals * inv_rms * gain_vec).astype(jnp.bfloat16)


def attention_block(tok_rows, gain_vec, layer_qkv, layer_out, layer_keys, layer_vals, seq_lens):
    row_count = tok_rows.shape[0]
    cache_len = layer_keys.shape[1]
    kv_heads = layer_keys.shape[2]
    head_dim = layer_keys.shape[3]
    q_width = layer_out.shape[0]
    group_size = q_width // (head_dim * kv_heads)
    kv_width = kv_heads * head_dim
    score_scale = head_dim ** -0.5
    normed = rms_norm(tok_rows, gain_vec)
    qkv_rows = jnp.dot(normed, layer_qkv, preferred_element_type=jnp.float32).astype(jnp.bfloat16)
    q_heads = qkv_rows[:, :q_width].reshape(row_count, kv_heads, group_size, head_dim).astype(jnp.float32)
    k_new = qkv_rows[:, q_width:q_width + kv_width].reshape(row_count, kv_heads, head_dim).astype(jnp.float32)
    v_new = qkv_rows[:, q_width + kv_width:].reshape(row_count, kv_heads, head_dim).astype(jnp.float32)
    s_cache = jnp.einsum('bkgd,bskd->bkgs', q_heads, layer_keys.astype(jnp.float32)) * score_scale
    s_self = jnp.einsum('bkgd,bkd->bkg', q_heads, k_new) * score_scale
    positions = lax.broadcasted_iota(jnp.int32, (1, 1, 1, cache_len), 3)
    s_cache = jnp.where(positions < seq_lens[:, None, None, None], s_cache, -1e30)
    row_max = jnp.maximum(jnp.max(s_cache, axis=-1), s_self)
    e_cache = jnp.exp(s_cache - row_max[..., None])
    e_self = jnp.exp(s_self - row_max)
    denom_sum = jnp.sum(e_cache, axis=-1) + e_self
    p_cache = (e_cache / denom_sum[..., None]).astype(jnp.bfloat16)
    p_self = (e_self / denom_sum).astype(jnp.bfloat16)
    mixed_out = jnp.einsum('bkgs,bskd->bkgd', p_cache.astype(jnp.float32), layer_vals.astype(jnp.float32))
    mixed_out = mixed_out + p_self.astype(jnp.float32)[..., None] * v_new[:, :, None, :]
    attn_rows = mixed_out.astype(jnp.bfloat16).reshape(row_count, q_width)
    attn_proj = jnp.dot(attn_rows, layer_out, preferred_element_type=jnp.float32)
    return (tok_rows.astype(jnp.float32) + attn_proj).astype(jnp.bfloat16)


def ffn_block(mid_rows, gain_vec, layer_gate, layer_up, layer_down):
    normed = rms_norm(mid_rows, gain_vec)
    gate_val = jnp.dot(normed, layer_gate, preferred_element_type=jnp.float32)
    up_val = jnp.dot(normed, layer_up, preferred_element_type=jnp.float32)
    act_rows = (jax.nn.silu(gate_val) * up_val).astype(jnp.bfloat16)
    down_val = jnp.dot(act_rows, layer_down, preferred_element_type=jnp.float32)
    return (mid_rows.astype(jnp.float32) + down_val).astype(jnp.bfloat16)


def draw_lengths(len_key):
    key_perm, key_hot, key_cold = jax.random.split(len_key, 3)
    rep_order = jax.random.permutation(key_perm, GROUP_DEVS)
    hot_len = jax.random.randint(key_hot, (GROUP_DEVS, TOK_DEV), CACHE_LEN - CACHE_LEN // 4, CACHE_LEN + 1)
    cold_len = jax.random.randint(key_cold, (GROUP_DEVS, TOK_DEV), 1, CACHE_LEN // 8 + 1)
    lengths = jnp.where((rep_order < GROUP_DEVS // 2)[:, None], hot_len, cold_len)
    first_tok = lax.broadcasted_iota(jnp.int32, (GROUP_DEVS, TOK_DEV), 1) == 0
    lengths = jnp.where(first_tok & (rep_order == 0)[:, None], CACHE_LEN, lengths)
    lengths = jnp.where(first_tok & (rep_order == GROUP_DEVS - 1)[:, None], 1, lengths)
    return lengths.reshape(TOKENS).astype(jnp.int32)


def setup_inputs(seed: int = 0, part: int = 0) -> dict:
    own_keys = jax.random.split(jax.random.fold_in(jax.random.key(seed), part), 4)
    shared = jax.random.split(jax.random.key(seed + 1), 7)
    qkv_width = (NUM_HEADS + 2 * KV_HEADS) * HEAD_DIM
    q_width = NUM_HEADS * HEAD_DIM
    cache_shape = (LAYERS, TOKENS, CACHE_LEN, KV_HEADS, HEAD_DIM)
    hidden = jax.random.normal(own_keys[0], (TOKENS, D_MODEL), jnp.float32).astype(jnp.bfloat16)
    k_cache = jax.random.normal(own_keys[1], cache_shape, jnp.float32).astype(jnp.bfloat16)
    v_cache = jax.random.normal(own_keys[2], cache_shape, jnp.float32).astype(jnp.bfloat16)
    seq_lens = draw_lengths(own_keys[3])
    w_qkv = (jax.random.normal(shared[0], (LAYERS, D_MODEL, qkv_width), jnp.float32) * D_MODEL ** -0.5).astype(jnp.bfloat16)
    w_out = (jax.random.normal(shared[1], (LAYERS, q_width, D_MODEL), jnp.float32) * q_width ** -0.5).astype(jnp.bfloat16)
    norm_attn = 1.0 + 0.4 * jax.random.normal(shared[2], (LAYERS, D_MODEL), jnp.float32)
    norm_ffn = 1.0 + 0.4 * jax.random.normal(shared[3], (LAYERS, D_MODEL), jnp.float32)
    w_gate = (jax.random.normal(shared[4], (LAYERS, D_MODEL, FFN_DIM), jnp.float32) * D_MODEL ** -0.5).astype(jnp.bfloat16)
    w_up = (jax.random.normal(shared[5], (LAYERS, D_MODEL, FFN_DIM), jnp.float32) * D_MODEL ** -0.5).astype(jnp.bfloat16)
    w_down = (jax.random.normal(shared[6], (LAYERS, FFN_DIM, D_MODEL), jnp.float32) * FFN_DIM ** -0.5).astype(jnp.bfloat16)
    return {'hidden': hidden, 'w_qkv': w_qkv, 'w_out': w_out, 'norm_attn': norm_attn, 'norm_ffn': norm_ffn, 'k_cache': k_cache, 'v_cache': v_cache, 'seq_lens': seq_lens, 'w_gate': w_gate, 'w_up': w_up, 'w_down': w_down}


def reference(hidden, w_qkv, w_out, norm_attn, norm_ffn, k_cache, v_cache, seq_lens, w_gate, w_up, w_down):
    def layer_step(tok_rows, layer_args):
        layer_qkv, layer_out, gain_attn, gain_ffn, layer_keys, layer_vals, layer_gate, layer_up, layer_down = layer_args
        mid_rows = attention_block(tok_rows, gain_attn, layer_qkv, layer_out, layer_keys, layer_vals, seq_lens)
        return ffn_block(mid_rows, gain_ffn, layer_gate, layer_up, layer_down), None
    return lax.scan(layer_step, hidden, (w_qkv, w_out, norm_attn, norm_ffn, k_cache, v_cache, w_gate, w_up, w_down))[0]
```

```python
import jax
import jax.numpy as jnp
from jax import lax
from jax.experimental import pallas as pl
from jax.experimental.pallas import tpu as pltpu
from jax.sharding import PartitionSpec as P

NORM_EPS = 1e-5
F32 = jnp.float32
BF16 = jnp.bfloat16
LAYERS = 4
ROWS = 64
D = 768
HD = 128
HEADS = 6
CACHE = 256
QKV = 1280
FFN = 2048
CHUNK = 16
CHUNKS = ROWS // CHUNK
SLOTS = 7
FBLK = 512
NT = (((1,), (1,)), ((), ()))


def rms(rows_bf16, gain):
    vals = rows_bf16.astype(F32)
    inv = lax.rsqrt(jnp.mean(vals * vals, axis=-1, keepdims=True) + NORM_EPS)
    return (vals * inv * gain).astype(BF16)


def kernel(hid, ga, gf, lens, wqkv, wout, kc, vc, wg, wu, wd, out,
           kbuf, vbuf, qkvw, outw, fg, fu, fd, q3, k3, v3, o3, len3, xbuf, hbuf, hg, xg, zbuf,
           ksem, vsem, wsem, fsem, hs_sem, hr_sem, xs_sem, xr_sem):
    me = lax.axis_index("data")

    def kcopy(c):
        layer, part, slot = c // CHUNKS, c % CHUNKS, c % SLOTS
        src = pl.ds(pl.multiple_of(part * CHUNK, CHUNK), CHUNK)
        return (pltpu.make_async_copy(kc.at[layer, src], kbuf.at[slot], ksem.at[slot]),
                pltpu.make_async_copy(vc.at[layer, src], vbuf.at[slot], vsem.at[slot]))

    def wcopy(layer):
        slot = layer % 2
        return (pltpu.make_async_copy(wqkv.at[layer], qkvw.at[slot], wsem.at[slot, 0]),
                pltpu.make_async_copy(wout.at[layer], outw.at[slot], wsem.at[slot, 1]))

    def fcopy():
        return (pltpu.make_async_copy(wg.at[0], fg, fsem.at[0]),
                pltpu.make_async_copy(wu.at[0], fu, fsem.at[1]),
                pltpu.make_async_copy(wd.at[0], fd, fsem.at[2]))

    def send_h(layer):
        return pltpu.make_async_remote_copy(
            src_ref=hbuf.at[layer], dst_ref=hg.at[me], send_sem=hs_sem.at[layer], recv_sem=hr_sem.at[me],
            device_id={"data": layer}, device_id_type=pl.DeviceIdType.MESH)

    def recv_h(src):
        return pltpu.make_async_remote_copy(
            src_ref=hbuf.at[0], dst_ref=hg.at[src], send_sem=hs_sem.at[0], recv_sem=hr_sem.at[src],
            device_id={"data": src}, device_id_type=pl.DeviceIdType.MESH)

    def send_x(layer, dst):
        return pltpu.make_async_remote_copy(
            src_ref=xg.at[dst], dst_ref=xbuf.at[layer + 1], send_sem=xs_sem.at[dst], recv_sem=xr_sem.at[layer],
            device_id={"data": dst}, device_id_type=pl.DeviceIdType.MESH)

    wcopy(0)[0].start()
    for c in range(CHUNKS):
        for cp in kcopy(c):
            cp.start()
    wcopy(0)[1].start()
    for cp in fcopy():
        cp.start()
    for c in range(CHUNKS, SLOTS):
        for cp in kcopy(c):
            cp.start()

    barrier = pltpu.get_barrier_semaphore()
    for step in range(1, 4):
        pl.semaphore_signal(barrier, inc=1, device_id={"data": (me + step) % 4}, device_id_type=pl.DeviceIdType.MESH)
    pl.semaphore_wait(barrier, 3)

    pick = (lax.broadcasted_iota(jnp.int32, (ROWS * 8, ROWS), 0) // 8 == lax.broadcasted_iota(jnp.int32, (ROWS * 8, ROWS), 1))
    lrow = jnp.broadcast_to(lens[...].astype(F32), (HD, ROWS)).astype(BF16)
    len3[...] = 2.0 * lax.dot_general(pick.astype(F32).astype(BF16), lrow, NT, preferred_element_type=F32)
    zrow = jnp.zeros((ROWS, HD), F32)
    for j in (6, 7):
        for ref in (q3, k3, v3):
            ref[pl.ds(j, ROWS, stride=8), :] = zrow
    xbuf[0] = hid[...]

    def layer_step(layer, carry):
        wslot = layer % 2
        wcopy(layer)[0].wait()
        normed = rms(xbuf[layer], ga[pl.ds(layer, 1), :])
        qkv = jnp.dot(normed, qkvw[wslot], preferred_element_type=F32).astype(BF16).astype(F32)
        for j in range(HEADS):
            dst = pl.ds(j, ROWS, stride=8)
            kv = j * 2 // HEADS
            q3[dst, :] = qkv[:, j * HD:(j + 1) * HD]
            k3[dst, :] = qkv[:, (HEADS + kv) * HD:(HEADS + kv + 1) * HD]
            v3[dst, :] = qkv[:, (HEADS + 2 + kv) * HD:(HEADS + 3 + kv) * HD]

        def chunk_step(part, carry):
            c = layer * CHUNKS + part
            slot = c % SLOTS
            base = pl.multiple_of(part * (CHUNK * 8), CHUNK * 8)
            rows = pl.ds(base, CHUNK * 8)
            qc = q3[rows, :]
            s_self = jnp.sum(qc * k3[rows, :], axis=-1, keepdims=True) * (HD ** -0.5)
            kcopy(c)[0].wait()
            zero = jnp.zeros((8, HD), F32)
            scores = []
            for i in range(CHUNK // 2):
                qa = qc[16 * i:16 * i + 8]
                qb = qc[16 * i + 8:16 * i + 16]
                lhs = jnp.concatenate([jnp.concatenate([qa, zero], 1), jnp.concatenate([zero, qb], 1)], 0).astype(BF16)
                keys = jnp.concatenate([kbuf[slot, 2 * i], kbuf[slot, 2 * i + 1]], 1)
                scores.append(lax.dot_general(lhs, keys, NT, preferred_element_type=F32))
            s = jnp.concatenate(scores, 0) * (HD ** -0.5)
            col = lax.broadcasted_iota(jnp.int32, s.shape, 1)
            head = lax.broadcasted_iota(jnp.int32, s.shape, 0) % 8
            lim = len3[rows, :]
            lim = jnp.concatenate([lim] * (2 * CACHE // HD), 1)
            good = (col % 2 == head // 3) & (col.astype(F32) < lim)
            s = jnp.where(good, s, -1e30)
            top = jnp.maximum(jnp.max(s, axis=-1, keepdims=True), s_self)
            e = jnp.exp(s - top)
            e_self = jnp.exp(s_self - top)
            inv = 1.0 / (jnp.sum(e, axis=-1, keepdims=True) + e_self)
            p = (e * inv).astype(BF16)
            self_out = (e_self * inv).astype(BF16).astype(F32) * v3[rows, :]
            kcopy(c)[1].wait()
            outs = []
            for i in range(CHUNK // 2):
                vals = jnp.concatenate([vbuf[slot, 2 * i], vbuf[slot, 2 * i + 1]], 1)
                o = jnp.dot(p[16 * i:16 * i + 16], vals, preferred_element_type=F32)
                outs += [o[0:8, 0:HD], o[8:16, HD:2 * HD]]
            o3[rows, :] = jnp.concatenate(outs, 0) + self_out

            @pl.when(c + SLOTS < LAYERS * CHUNKS)
            def _():
                for cp in kcopy(c + SLOTS):
                    cp.start()
            return carry

        lax.fori_loop(0, CHUNKS, chunk_step, 0)
        attn = jnp.concatenate([o3[pl.ds(j, ROWS, stride=8), :] for j in range(HEADS)], 1).astype(BF16)
        wcopy(layer)[1].wait()
        proj = jnp.dot(attn, outw[wslot], preferred_element_type=F32)
        mid = (xbuf[layer].astype(F32) + proj).astype(BF16)

        @pl.when(me != layer)
        def _():
            hbuf[layer] = mid
            send_h(layer).start()

        @pl.when(layer + 1 < LAYERS)
        def _():
            for cp in wcopy(layer + 1):
                cp.start()

        @pl.when(me == layer)
        def _():
            hg[me] = mid
            gain = gf[pl.ds(layer, 1), :]

            @pl.when(layer == layer)
            def _():
                for cp in fcopy():
                    cp.wait()

            def half_step(turn, carry):
                half = (me // 2 + turn) % 2
                for k in range(2):
                    src = half * 2 + k

                    @pl.when(src != me)
                    def _():
                        recv_h(src).wait_recv()
                two = pl.ds(half * 2, 2)
                rows_h = hg[two].reshape(2 * ROWS, D)
                n2 = rms(rows_h, gain)
                for b in range(FFN // FBLK):
                    cols = slice(b * FBLK, (b + 1) * FBLK)
                    a = jnp.dot(n2, fg[:, cols], preferred_element_type=F32)
                    u = jnp.dot(n2, fu[:, cols], preferred_element_type=F32)
                    zbuf[:, cols] = (a * jax.nn.sigmoid(a) * u).astype(BF16)
                down = jnp.dot(zbuf[...], fd[...], preferred_element_type=F32)
                xg[two] = (rows_h.astype(F32) + down).astype(BF16).reshape(2, ROWS, D)
                for k in range(2):
                    dst = half * 2 + k

                    @pl.when(dst != me)
                    def _():
                        send_x(layer, dst).start()
                return carry

            lax.fori_loop(0, 2, half_step, 0)
            xbuf[layer + 1] = xg[me]

        @pl.when(me != layer)
        def _():
            send_h(layer).wait_send()
            send_x(layer, me).wait_recv()
        return carry

    lax.fori_loop(0, LAYERS, layer_step, 0)
    for step in range(1, 4):
        send_x(0, (me + step) % 4).wait_send()
    out[...] = xbuf[LAYERS]


def solution(mesh):
    row_spec = P(('grp', 'data'), None)
    rep_spec = P()
    cache_spec = P(None, ('grp', 'data'))
    len_spec = P(('grp', 'data'))
    owned_spec = P('data')

    def per_device(hidden, w_qkv, w_out, norm_attn, norm_ffn, k_cache, v_cache, seq_lens, w_gate, w_up, w_down):
        kc = k_cache.reshape(LAYERS, ROWS, 2 * CACHE, HD)
        vc = v_cache.reshape(LAYERS, ROWS, 2 * CACHE, HD)
        vm = pl.BlockSpec(memory_space=pltpu.VMEM)
        anys = pl.BlockSpec(memory_space=pl.ANY)
        dma = pltpu.SemaphoreType.DMA
        return pl.pallas_call(
            kernel,
            out_shape=jax.ShapeDtypeStruct((ROWS, D), BF16),
            in_specs=[vm] * 4 + [anys] * 7,
            out_specs=vm,
            scratch_shapes=[
                pltpu.VMEM((SLOTS, CHUNK, 2 * CACHE, HD), BF16),
                pltpu.VMEM((SLOTS, CHUNK, 2 * CACHE, HD), BF16),
                pltpu.VMEM((2, D, QKV), BF16),
                pltpu.VMEM((2, D, D), BF16),
                pltpu.VMEM((D, FFN), BF16),
                pltpu.VMEM((D, FFN), BF16),
                pltpu.VMEM((FFN, D), BF16),
                pltpu.VMEM((ROWS * 8, HD), F32),
                pltpu.VMEM((ROWS * 8, HD), F32),
                pltpu.VMEM((ROWS * 8, HD), F32),
                pltpu.VMEM((ROWS * 8, HD), F32),
                pltpu.VMEM((ROWS * 8, HD), F32),
                pltpu.VMEM((LAYERS + 1, ROWS, D), BF16),
                pltpu.VMEM((LAYERS, ROWS, D), BF16),
                pltpu.VMEM((4, ROWS, D), BF16),
                pltpu.VMEM((4, ROWS, D), BF16),
                pltpu.VMEM((2 * ROWS, FFN), BF16),
                dma((SLOTS,)), dma((SLOTS,)), dma((2, 2)), dma((3,)),
                dma((LAYERS,)), dma((4,)), dma((4,)), dma((LAYERS,)),
            ],
            compiler_params=pltpu.CompilerParams(collective_id=0, has_side_effects=True, vmem_limit_bytes=67043328),
        )(hidden, norm_attn, norm_ffn, seq_lens.reshape(1, ROWS), w_qkv, w_out, kc, vc, w_gate, w_up, w_down)

    return jax.shard_map(per_device, mesh=mesh, in_specs=(row_spec, rep_spec, rep_spec, rep_spec, rep_spec, cache_spec, cache_spec, len_spec, owned_spec, owned_spec, owned_spec), out_specs=row_spec, check_vma=False)
```

```python
import jax
import jax.numpy as jnp
from jax import lax
from jax.experimental import pallas as pl
from jax.experimental.pallas import tpu as pltpu
from jax.sharding import PartitionSpec as P

NORM_EPS = 1e-5
F32 = jnp.float32
BF16 = jnp.bfloat16
LAYERS = 4
ROWS = 64
D = 768
HD = 128
HEADS = 6
CACHE = 256
QKV = 1280
FFN = 2048
CHUNK = 16
CHUNKS = ROWS // CHUNK
SLOTS = 6
HALF = ROWS // 2
FBLK = 512
NT = (((1,), (1,)), ((), ()))


def rms(rows_bf16, gain):
    vals = rows_bf16.astype(F32)
    inv = lax.rsqrt(jnp.mean(vals * vals, axis=-1, keepdims=True) + NORM_EPS)
    return (vals * inv * gain).astype(BF16)


def kernel(hid, ga, gf, lens, wqkv, wout, kc, vc, wg, wu, wd, out,
           kbuf, vbuf, qkvw, outw, fg, fu, fd, q3, k3, v3, o3, len3, xbuf, hbuf, hin, xo, zbuf,
           ksem, vsem, wsem, fsem, fs_sem, fr_sem, hs_sem, hr_sem, xs_sem, xr_sem):
    me = lax.axis_index("data")
    chip, core = me // 2, me % 2
    mate, peer = chip * 2 + (1 - core), (me + 2) % 4
    mesh_id = pl.DeviceIdType.MESH

    def kcopy(c, which):
        layer, part, slot = c // CHUNKS, c % CHUNKS, c % SLOTS
        src = pl.ds(pl.multiple_of(part * CHUNK, CHUNK), CHUNK)
        if which == 0:
            return pltpu.make_async_copy(kc.at[layer, src], kbuf.at[slot], ksem.at[slot])
        return pltpu.make_async_copy(vc.at[layer, src], vbuf.at[slot], vsem.at[slot])

    def wcopy(layer, which):
        slot = layer % 2
        if which == 0:
            return pltpu.make_async_copy(wqkv.at[layer], qkvw.at[slot], wsem.at[slot, 0])
        return pltpu.make_async_copy(wout.at[layer], outw.at[slot], wsem.at[slot, 1])

    ffn_parts = ((wg, fg), (wu, fu), (wd, fd))

    def fcopy(k):
        return pltpu.make_async_copy(ffn_parts[k][0].at[0], ffn_parts[k][1].at[core], fsem.at[k])

    def fsend(k, idx):
        return pltpu.make_async_remote_copy(
            src_ref=ffn_parts[k][0].at[0], dst_ref=ffn_parts[k][1].at[idx], send_sem=fs_sem.at[k], recv_sem=fr_sem.at[k],
            device_id={"data": mate}, device_id_type=mesh_id)

    def send_h(layer, half, dst, slot, pos):
        rows = pl.ds(pl.multiple_of(half * HALF, HALF), HALF)
        return pltpu.make_async_remote_copy(
            src_ref=hbuf.at[layer, rows], dst_ref=hin.at[slot, pos, rows],
            send_sem=hs_sem.at[layer, half], recv_sem=hr_sem.at[slot, pos, half],
            device_id={"data": dst}, device_id_type=mesh_id)

    def send_x(layer, dst, slot, pos):
        return pltpu.make_async_remote_copy(
            src_ref=xo.at[slot, pos], dst_ref=xbuf.at[layer + 1], send_sem=xs_sem.at[slot, pos], recv_sem=xr_sem.at[layer],
            device_id={"data": dst}, device_id_type=mesh_id)

    wcopy(0, 0).start()
    for c in range(CHUNKS):
        for which in range(2):
            kcopy(c, which).start()
    wcopy(0, 1).start()
    for k in range(3):
        fcopy(k).start()
    for c in range(CHUNKS, SLOTS):
        for which in range(2):
            kcopy(c, which).start()

    barrier = pltpu.get_barrier_semaphore()
    for step in range(1, 4):
        pl.semaphore_signal(barrier, inc=1, device_id={"data": (me + step) % 4}, device_id_type=mesh_id)
    pl.semaphore_wait(barrier, 3)

    @pl.when(me != 0)
    def _():
        for k in range(3):
            fsend(k, core).start()

    pick = (lax.broadcasted_iota(jnp.int32, (ROWS * 8, ROWS), 0) // 8 == lax.broadcasted_iota(jnp.int32, (ROWS * 8, ROWS), 1))
    lrow = jnp.broadcast_to(lens[...].astype(F32), (HD, ROWS)).astype(BF16)
    len3[...] = 2.0 * lax.dot_general(pick.astype(F32).astype(BF16), lrow, NT, preferred_element_type=F32)
    zrow = jnp.zeros((ROWS, HD), F32)
    for j in (6, 7):
        for ref in (q3, k3, v3):
            ref[pl.ds(j, ROWS, stride=8), :] = zrow
    xbuf[0] = hid[...]

    def is_local(layer):
        return (chip == layer // 2) & ((layer > 0) | (me == 0))

    def layer_step(layer, carry):
        wslot = layer % 2
        local = is_local(layer)
        dst = jnp.where(layer == 0, 0, peer)
        slot = jnp.where((layer == 0) & (me == 1), 0, 2 * (layer % 2) + 1)
        pos = jnp.where(layer == 0, core, 0)
        wcopy(layer, 0).wait()

        @pl.when((layer > 0) & jnp.logical_not(is_local(layer - 1)))
        def _():
            send_x(layer - 1, me, 0, 0).wait_recv()

        normed = rms(xbuf[layer], ga[pl.ds(layer, 1), :])
        qkv = jnp.dot(normed, qkvw[wslot], preferred_element_type=F32).astype(BF16).astype(F32)
        for j in range(HEADS):
            rows8 = pl.ds(j, ROWS, stride=8)
            kv = j * 2 // HEADS
            q3[rows8, :] = qkv[:, j * HD:(j + 1) * HD]
            k3[rows8, :] = qkv[:, (HEADS + kv) * HD:(HEADS + kv + 1) * HD]
            v3[rows8, :] = qkv[:, (HEADS + 2 + kv) * HD:(HEADS + 3 + kv) * HD]

        def chunk_step(part, carry):
            c = layer * CHUNKS + part
            cslot = c % SLOTS
            base = pl.multiple_of(part * (CHUNK * 8), CHUNK * 8)
            rows = pl.ds(base, CHUNK * 8)
            qc = q3[rows, :]
            s_self = jnp.sum(qc * k3[rows, :], axis=-1, keepdims=True) * (HD ** -0.5)
            kcopy(c, 0).wait()
            zero = jnp.zeros((8, HD), F32)
            scores = []
            for i in range(CHUNK // 2):
                qa = qc[16 * i:16 * i + 8]
                qb = qc[16 * i + 8:16 * i + 16]
                lhs = jnp.concatenate([jnp.concatenate([qa, zero], 1), jnp.concatenate([zero, qb], 1)], 0).astype(BF16)
                keys = jnp.concatenate([kbuf[cslot, 2 * i], kbuf[cslot, 2 * i + 1]], 1)
                scores.append(lax.dot_general(lhs, keys, NT, preferred_element_type=F32))
            s = jnp.concatenate(scores, 0) * (HD ** -0.5)
            col = lax.broadcasted_iota(jnp.int32, s.shape, 1)
            head = lax.broadcasted_iota(jnp.int32, s.shape, 0) % 8
            lim = len3[rows, :]
            lim = jnp.concatenate([lim] * (2 * CACHE // HD), 1)
            good = (col % 2 == head // 3) & (col.astype(F32) < lim)
            s = jnp.where(good, s, -1e30)
            top = jnp.maximum(jnp.max(s, axis=-1, keepdims=True), s_self)
            e = jnp.exp(s - top)
            e_self = jnp.exp(s_self - top)
            inv = 1.0 / (jnp.sum(e, axis=-1, keepdims=True) + e_self)
            p = (e * inv).astype(BF16)
            self_out = (e_self * inv).astype(BF16).astype(F32) * v3[rows, :]
            kcopy(c, 1).wait()
            outs = []
            for i in range(CHUNK // 2):
                vals = jnp.concatenate([vbuf[cslot, 2 * i], vbuf[cslot, 2 * i + 1]], 1)
                o = jnp.dot(p[16 * i:16 * i + 16], vals, preferred_element_type=F32)
                outs += [o[0:8, 0:HD], o[8:16, HD:2 * HD]]
            o3[rows, :] = jnp.concatenate(outs, 0) + self_out

            @pl.when(c + SLOTS < LAYERS * CHUNKS)
            def _():
                for which in range(2):
                    kcopy(c + SLOTS, which).start()
            return carry

        def half_att(half, carry):
            lax.fori_loop(half * (CHUNKS // 2), (half + 1) * (CHUNKS // 2), chunk_step, 0)

            @pl.when(half == 0)
            def _():
                wcopy(layer, 1).wait()

            base = half * (HALF * 8)
            attn = jnp.concatenate([o3[pl.ds(base + j, HALF, stride=8), :] for j in range(HEADS)], 1).astype(BF16)
            proj = jnp.dot(attn, outw[wslot], preferred_element_type=F32)
            rows = pl.ds(pl.multiple_of(half * HALF, HALF), HALF)
            mid = (xbuf[layer, rows].astype(F32) + proj).astype(BF16)

            @pl.when(local)
            def _():
                hin[2 * (layer % 2), 0, rows] = mid

            @pl.when(jnp.logical_not(local))
            def _():
                hbuf[layer, rows] = mid
                send_h(layer, half, dst, slot, pos).start()
            return carry

        lax.fori_loop(0, 2, half_att, 0)

        @pl.when(layer + 1 < LAYERS)
        def _():
            for which in range(2):
                wcopy(layer + 1, which).start()

        def ffn_step(turn, carry):
            serve = chip == turn
            tl = jnp.where(serve, jnp.where(chip == 0, layer - 1, layer + 1), layer)
            todo = jnp.where(serve, (layer >= 1) & (layer <= 2), tl // 2 == chip) & ((tl > 0) | (me == 0))

            @pl.when(todo)
            def _():
                idx = tl % 2
                fslot = 2 * idx + jnp.where(serve, 1, 0)
                both = tl == 0

                @pl.when(serve)
                def _():
                    for half in range(2):
                        send_h(0, half, me, fslot, 0).wait_recv()

                @pl.when(both)
                def _():
                    for half in range(2):
                        send_h(0, half, me, fslot, 1).wait_recv()

                first = jnp.where(serve, 1, 0) == chip

                @pl.when(first & (idx == core))
                def _():
                    for k in range(3):
                        fcopy(k).wait()

                @pl.when(first & (idx != core))
                def _():
                    for k in range(3):
                        fsend(k, idx).wait_recv()

                rows_h = hin[fslot].reshape(2 * ROWS, D)
                n2 = rms(rows_h, gf[pl.ds(tl, 1), :])
                for b in range(FFN // FBLK):
                    cols = slice(b * FBLK, (b + 1) * FBLK)
                    a = jnp.dot(n2, fg[idx, :, cols], preferred_element_type=F32)
                    u = jnp.dot(n2, fu[idx, :, cols], preferred_element_type=F32)
                    zbuf[:, cols] = (a * jax.nn.sigmoid(a) * u).astype(BF16)
                down = jnp.dot(zbuf[...], fd[idx], preferred_element_type=F32)
                xo[fslot] = (rows_h.astype(F32) + down).astype(BF16).reshape(2, ROWS, D)

                @pl.when(serve)
                def _():
                    send_x(tl, peer, fslot, 0).start()

                @pl.when(jnp.logical_not(serve))
                def _():
                    xbuf[tl + 1] = xo[fslot, 0]

                @pl.when(both)
                def _():
                    send_x(tl, jnp.where(serve, 3, 1), fslot, 1).start()
            return carry

        lax.fori_loop(0, 2, ffn_step, 0)
        return carry

    lax.fori_loop(0, LAYERS, layer_step, 0)

    @pl.when(chip == 0)
    def _():
        send_x(LAYERS - 1, me, 0, 0).wait_recv()

    out[...] = xbuf[LAYERS]

    for layer in range(LAYERS):
        @pl.when(jnp.logical_not(is_local(layer)))
        def _():
            for half in range(2):
                send_h(layer, half, 0, 0, 0).wait_send()

    @pl.when(me != 0)
    def _():
        send_x(0, me, 3, 0).wait_send()
        for k in range(3):
            fsend(k, core).wait_send()

    @pl.when(chip == 1)
    def _():
        send_x(0, me, 1, 0).wait_send()

    @pl.when(me == 0)
    def _():
        for slot, pos in ((0, 1), (1, 0), (1, 1), (3, 0)):
            send_x(0, me, slot, pos).wait_send()


def solution(mesh):
    row_spec = P(('grp', 'data'), None)
    rep_spec = P()
    cache_spec = P(None, ('grp', 'data'))
    len_spec = P(('grp', 'data'))
    owned_spec = P('data')

    def per_device(hidden, w_qkv, w_out, norm_attn, norm_ffn, k_cache, v_cache, seq_lens, w_gate, w_up, w_down):
        kc = k_cache.reshape(LAYERS, ROWS, 2 * CACHE, HD)
        vc = v_cache.reshape(LAYERS, ROWS, 2 * CACHE, HD)
        vm = pl.BlockSpec(memory_space=pltpu.VMEM)
        anys = pl.BlockSpec(memory_space=pl.ANY)
        dma = pltpu.SemaphoreType.DMA
        return pl.pallas_call(
            kernel,
            out_shape=jax.ShapeDtypeStruct((ROWS, D), BF16),
            in_specs=[vm] * 4 + [anys] * 7,
            out_specs=vm,
            scratch_shapes=[
                pltpu.VMEM((SLOTS, CHUNK, 2 * CACHE, HD), BF16),
                pltpu.VMEM((SLOTS, CHUNK, 2 * CACHE, HD), BF16),
                pltpu.VMEM((2, D, QKV), BF16),
                pltpu.VMEM((2, D, D), BF16),
                pltpu.VMEM((2, D, FFN), BF16),
                pltpu.VMEM((2, D, FFN), BF16),
                pltpu.VMEM((2, FFN, D), BF16),
                pltpu.VMEM((ROWS * 8, HD), F32),
                pltpu.VMEM((ROWS * 8, HD), F32),
                pltpu.VMEM((ROWS * 8, HD), F32),
                pltpu.VMEM((ROWS * 8, HD), F32),
                pltpu.VMEM((ROWS * 8, HD), F32),
                pltpu.VMEM((LAYERS + 1, ROWS, D), BF16),
                pltpu.VMEM((LAYERS, ROWS, D), BF16),
                pltpu.VMEM((4, 2, ROWS, D), BF16),
                pltpu.VMEM((4, 2, ROWS, D), BF16),
                pltpu.VMEM((2 * ROWS, FFN), BF16),
                dma((SLOTS,)), dma((SLOTS,)), dma((2, 2)), dma((3,)), dma((3,)), dma((3,)),
                dma((LAYERS, 2)), dma((4, 2, 2)), dma((4, 2)), dma((LAYERS,)),
            ],
            compiler_params=pltpu.CompilerParams(collective_id=0, has_side_effects=True, vmem_limit_bytes=67043328),
        )(hidden, norm_attn, norm_ffn, seq_lens.reshape(1, ROWS), w_qkv, w_out, kc, vc, w_gate, w_up, w_down)

    return jax.shard_map(per_device, mesh=mesh, in_specs=(row_spec, rep_spec, rep_spec, rep_spec, rep_spec, cache_spec, cache_spec, len_spec, owned_spec, owned_spec, owned_spec), out_specs=row_spec, check_vma=False)
```

```python
import jax
import jax.numpy as jnp
from jax import lax
from jax.experimental import pallas as pl
from jax.experimental.pallas import tpu as pltpu
from jax.sharding import PartitionSpec as P

NORM_EPS = 1e-5
F32 = jnp.float32
BF16 = jnp.bfloat16
LAYERS = 4
ROWS = 64
D = 768
HD = 128
HEADS = 6
CACHE = 256
QKV = 1280
FFN = 2048
CHUNK = 16
CHUNKS = ROWS // CHUNK
SLOTS = 6
HALF = ROWS // 2
FBLK = 512
NT = (((1,), (1,)), ((), ()))


def rms(rows_bf16, gain):
    vals = rows_bf16.astype(F32)
    inv = lax.rsqrt(jnp.mean(vals * vals, axis=-1, keepdims=True) + NORM_EPS)
    return (vals * inv * gain).astype(BF16)


def kernel(hid_in, ga_in, gf_in, lens_in, wqkv, wout, kc, vc, wg, wu, wd, out,
           kbuf, vbuf, qkvw, outw, fg, fu, fd, q3, k3, v3, o3, len3, xbuf, hbuf, hin, xo, zbuf,
           ksem, vsem, wsem, fsem, fs_sem, fr_sem, hs_sem, hr_sem, xs_sem, xr_sem, ga, gf, lens, isem):
    me = lax.axis_index("data")
    chip, core = me // 2, me % 2
    mate, peer = chip * 2 + (1 - core), (me + 2) % 4
    mesh_id = pl.DeviceIdType.MESH

    def kcopy(c, which):
        layer, part, slot = c // CHUNKS, c % CHUNKS, c % SLOTS
        src = pl.ds(pl.multiple_of(part * CHUNK, CHUNK), CHUNK)
        if which == 0:
            return pltpu.make_async_copy(kc.at[layer, src], kbuf.at[slot], ksem.at[slot])
        return pltpu.make_async_copy(vc.at[layer, src], vbuf.at[slot], vsem.at[slot])

    def wcopy(layer, which):
        slot = layer % 2
        if which == 0:
            return pltpu.make_async_copy(wqkv.at[layer], qkvw.at[slot], wsem.at[slot, 0])
        return pltpu.make_async_copy(wout.at[layer], outw.at[slot], wsem.at[slot, 1])

    ffn_parts = ((wg, fg), (wu, fu), (wd, fd))

    def fcopy(k):
        return pltpu.make_async_copy(ffn_parts[k][0].at[0], ffn_parts[k][1].at[core], fsem.at[k])

    def fsend(k, idx):
        return pltpu.make_async_remote_copy(
            src_ref=ffn_parts[k][0].at[0], dst_ref=ffn_parts[k][1].at[idx], send_sem=fs_sem.at[k], recv_sem=fr_sem.at[k],
            device_id={"data": mate}, device_id_type=mesh_id)

    def send_h(layer, half, dst, slot, pos):
        rows = pl.ds(pl.multiple_of(half * HALF, HALF), HALF)
        return pltpu.make_async_remote_copy(
            src_ref=hbuf.at[layer, rows], dst_ref=hin.at[slot, pos, rows],
            send_sem=hs_sem.at[layer, half], recv_sem=hr_sem.at[slot, pos, half],
            device_id={"data": dst}, device_id_type=mesh_id)

    def send_x(layer, dst, slot, pos):
        return pltpu.make_async_remote_copy(
            src_ref=xo.at[slot, pos], dst_ref=xbuf.at[layer + 1], send_sem=xs_sem.at[slot, pos], recv_sem=xr_sem.at[layer],
            device_id={"data": dst}, device_id_type=mesh_id)

    small = [pltpu.make_async_copy(src, dst, isem.at[k]) for k, (src, dst) in enumerate(
        ((hid_in, xbuf.at[0]), (ga_in, ga), (gf_in, gf), (lens_in, lens)))]
    for cp in small:
        cp.start()
    wcopy(0, 0).start()
    for c in range(3):
        for which in range(2):
            kcopy(c, which).start()

    barrier = pltpu.get_barrier_semaphore()
    for step in range(1, 4):
        pl.semaphore_signal(barrier, inc=1, device_id={"data": (me + step) % 4}, device_id_type=mesh_id)
    for cp in small:
        cp.wait()

    pick = (lax.broadcasted_iota(jnp.int32, (ROWS * 8, ROWS), 0) // 8 == lax.broadcasted_iota(jnp.int32, (ROWS * 8, ROWS), 1))
    lrow = jnp.broadcast_to(lens[...].astype(F32), (HD, ROWS)).astype(BF16)
    len3[...] = 2.0 * lax.dot_general(pick.astype(F32).astype(BF16), lrow, NT, preferred_element_type=F32)
    zrow = jnp.zeros((ROWS, HD), F32)
    for j in (6, 7):
        for ref in (q3, k3, v3):
            ref[pl.ds(j, ROWS, stride=8), :] = zrow
    pl.semaphore_wait(barrier, 3)

    def is_local(layer):
        return (chip == layer // 2) & ((layer > 0) | (me == 0))

    def layer_step(layer, carry):
        wslot = layer % 2
        local = is_local(layer)
        dst = jnp.where(layer == 0, 0, peer)
        slot = jnp.where((layer == 0) & (me == 1), 0, 2 * (layer % 2) + 1)
        pos = jnp.where(layer == 0, core, 0)
        wcopy(layer, 0).wait()

        @pl.when((layer > 0) & jnp.logical_not(is_local(layer - 1)))
        def _():
            send_x(layer - 1, me, 0, 0).wait_recv()

        normed = rms(xbuf[layer], ga[pl.ds(layer, 1), :])
        qkv = jnp.dot(normed, qkvw[wslot], preferred_element_type=F32).astype(BF16).astype(F32)
        for j in range(HEADS):
            rows8 = pl.ds(j, ROWS, stride=8)
            kv = j * 2 // HEADS
            q3[rows8, :] = qkv[:, j * HD:(j + 1) * HD]
            k3[rows8, :] = qkv[:, (HEADS + kv) * HD:(HEADS + kv + 1) * HD]
            v3[rows8, :] = qkv[:, (HEADS + 2 + kv) * HD:(HEADS + 3 + kv) * HD]

        def chunk_step(part, carry):
            c = layer * CHUNKS + part
            cslot = c % SLOTS
            base = pl.multiple_of(part * (CHUNK * 8), CHUNK * 8)
            rows = pl.ds(base, CHUNK * 8)

            @pl.when((layer > 0) & (c + SLOTS - 1 < LAYERS * CHUNKS))
            def _():
                for which in range(2):
                    kcopy(c + SLOTS - 1, which).start()

            @pl.when(c == 0)
            def _():
                for which in range(2):
                    kcopy(3, which).start()
                wcopy(0, 1).start()

            @pl.when(c == jnp.where(chip == 0, 1, CHUNKS + 1))
            def _():
                for k in range(3):
                    fcopy(k).start()

            @pl.when(c == 3)
            def _():
                for which in range(2):
                    kcopy(4, which).start()

            qc = q3[rows, :]
            s_self = jnp.sum(qc * k3[rows, :], axis=-1, keepdims=True) * (HD ** -0.5)
            kcopy(c, 0).wait()
            zero = jnp.zeros((8, HD), F32)
            scores = []
            for i in range(CHUNK // 2):
                qa = qc[16 * i:16 * i + 8]
                qb = qc[16 * i + 8:16 * i + 16]
                lhs = jnp.concatenate([jnp.concatenate([qa, zero], 1), jnp.concatenate([zero, qb], 1)], 0).astype(BF16)
                keys = jnp.concatenate([kbuf[cslot, 2 * i], kbuf[cslot, 2 * i + 1]], 1)
                scores.append(lax.dot_general(lhs, keys, NT, preferred_element_type=F32))
            s = jnp.concatenate(scores, 0) * (HD ** -0.5)
            col = lax.broadcasted_iota(jnp.int32, s.shape, 1)
            head = lax.broadcasted_iota(jnp.int32, s.shape, 0) % 8
            lim = len3[rows, :]
            lim = jnp.concatenate([lim] * (2 * CACHE // HD), 1)
            good = (col % 2 == head // 3) & (col.astype(F32) < lim)
            s = jnp.where(good, s, -1e30)
            top = jnp.maximum(jnp.max(s, axis=-1, keepdims=True), s_self)
            e = jnp.exp(s - top)
            e_self = jnp.exp(s_self - top)
            inv = 1.0 / (jnp.sum(e, axis=-1, keepdims=True) + e_self)
            p = (e * inv).astype(BF16)
            self_out = (e_self * inv).astype(BF16).astype(F32) * v3[rows, :]
            kcopy(c, 1).wait()
            outs = []
            for i in range(CHUNK // 2):
                vals = jnp.concatenate([vbuf[cslot, 2 * i], vbuf[cslot, 2 * i + 1]], 1)
                o = jnp.dot(p[16 * i:16 * i + 16], vals, preferred_element_type=F32)
                outs += [o[0:8, 0:HD], o[8:16, HD:2 * HD]]
            o3[rows, :] = jnp.concatenate(outs, 0) + self_out
            return carry

        def half_att(half, carry):
            lax.fori_loop(half * (CHUNKS // 2), (half + 1) * (CHUNKS // 2), chunk_step, 0)

            @pl.when(half == 0)
            def _():
                wcopy(layer, 1).wait()

            base = half * (HALF * 8)
            attn = jnp.concatenate([o3[pl.ds(base + j, HALF, stride=8), :] for j in range(HEADS)], 1).astype(BF16)
            proj = jnp.dot(attn, outw[wslot], preferred_element_type=F32)
            rows = pl.ds(pl.multiple_of(half * HALF, HALF), HALF)
            mid = (xbuf[layer, rows].astype(F32) + proj).astype(BF16)

            @pl.when(local)
            def _():
                hin[2 * (layer % 2), 0, rows] = mid

            @pl.when(jnp.logical_not(local))
            def _():
                hbuf[layer, rows] = mid
                send_h(layer, half, dst, slot, pos).start()
            return carry

        lax.fori_loop(0, 2, half_att, 0)

        @pl.when(layer + 1 < LAYERS)
        def _():
            for which in range(2):
                wcopy(layer + 1, which).start()

        @pl.when(layer == 0)
        def _():
            for c in range(CHUNKS + 1, CHUNKS + SLOTS - 1):
                for which in range(2):
                    kcopy(c, which).start()

        @pl.when((layer == 0) & (me != 0))
        def _():
            for k in range(3):
                fsend(k, core).start()

        def ffn_step(turn, carry):
            serve0 = (layer == 2) | (turn == 1)
            serve1 = (layer != 2) & (turn == 0)
            serve = jnp.where(chip == 0, serve0, serve1)
            tl = jnp.where(chip == 0, jnp.where(layer == 2, 1, layer), jnp.where(layer == 1, 2, layer))
            todo0 = jnp.where(turn == 0, layer < 3, layer == 0) & ((layer > 0) | (me == 0))
            todo1 = jnp.where(turn == 0, layer > 0, layer == 3)
            todo = jnp.where(chip == 0, todo0, todo1)

            @pl.when(todo)
            def _():
                idx = tl % 2
                fslot = 2 * idx + jnp.where(serve, 1, 0)
                both = tl == 0

                @pl.when(serve)
                def _():
                    for half in range(2):
                        send_h(0, half, me, fslot, 0).wait_recv()

                @pl.when(both)
                def _():
                    for half in range(2):
                        send_h(0, half, me, fslot, 1).wait_recv()

                first = jnp.where(serve, 1, 0) == chip

                @pl.when(first & (idx == core))
                def _():
                    for k in range(3):
                        fcopy(k).wait()

                @pl.when(first & (idx != core))
                def _():
                    for k in range(3):
                        fsend(k, idx).wait_recv()

                rows_h = hin[fslot].reshape(2 * ROWS, D)
                n2 = rms(rows_h, gf[pl.ds(tl, 1), :])
                for b in range(FFN // FBLK):
                    cols = slice(b * FBLK, (b + 1) * FBLK)
                    a = jnp.dot(n2, fg[idx, :, cols], preferred_element_type=F32)
                    u = jnp.dot(n2, fu[idx, :, cols], preferred_element_type=F32)
                    zbuf[:, cols] = (a * jax.nn.sigmoid(a) * u).astype(BF16)
                down = jnp.dot(zbuf[...], fd[idx], preferred_element_type=F32)
                xo[fslot] = (rows_h.astype(F32) + down).astype(BF16).reshape(2, ROWS, D)

                @pl.when(serve)
                def _():
                    send_x(tl, peer, fslot, 0).start()

                @pl.when(jnp.logical_not(serve))
                def _():
                    xbuf[tl + 1] = xo[fslot, 0]

                @pl.when(both)
                def _():
                    send_x(tl, jnp.where(serve, 3, 1), fslot, 1).start()
            return carry

        lax.fori_loop(0, 2, ffn_step, 0)
        return carry

    lax.fori_loop(0, LAYERS, layer_step, 0)

    @pl.when(chip == 0)
    def _():
        send_x(LAYERS - 1, me, 0, 0).wait_recv()

    out[...] = xbuf[LAYERS]

    for layer in range(LAYERS):
        @pl.when(jnp.logical_not(is_local(layer)))
        def _():
            for half in range(2):
                send_h(layer, half, 0, 0, 0).wait_send()

    @pl.when(me != 0)
    def _():
        send_x(0, me, 3, 0).wait_send()
        for k in range(3):
            fsend(k, core).wait_send()

    @pl.when(chip == 1)
    def _():
        send_x(0, me, 1, 0).wait_send()

    @pl.when(me == 0)
    def _():
        for slot, pos in ((0, 1), (1, 0), (1, 1), (3, 0)):
            send_x(0, me, slot, pos).wait_send()


def solution(mesh):
    row_spec = P(('grp', 'data'), None)
    rep_spec = P()
    cache_spec = P(None, ('grp', 'data'))
    len_spec = P(('grp', 'data'))
    owned_spec = P('data')

    def per_device(hidden, w_qkv, w_out, norm_attn, norm_ffn, k_cache, v_cache, seq_lens, w_gate, w_up, w_down):
        kc = k_cache.reshape(LAYERS, ROWS, 2 * CACHE, HD)
        vc = v_cache.reshape(LAYERS, ROWS, 2 * CACHE, HD)
        vm = pl.BlockSpec(memory_space=pltpu.VMEM)
        anys = pl.BlockSpec(memory_space=pl.ANY)
        dma = pltpu.SemaphoreType.DMA
        return pl.pallas_call(
            kernel,
            out_shape=jax.ShapeDtypeStruct((ROWS, D), BF16),
            in_specs=[anys] * 11,
            out_specs=vm,
            scratch_shapes=[
                pltpu.VMEM((SLOTS, CHUNK, 2 * CACHE, HD), BF16),
                pltpu.VMEM((SLOTS, CHUNK, 2 * CACHE, HD), BF16),
                pltpu.VMEM((2, D, QKV), BF16),
                pltpu.VMEM((2, D, D), BF16),
                pltpu.VMEM((2, D, FFN), BF16),
                pltpu.VMEM((2, D, FFN), BF16),
                pltpu.VMEM((2, FFN, D), BF16),
                pltpu.VMEM((ROWS * 8, HD), F32),
                pltpu.VMEM((ROWS * 8, HD), F32),
                pltpu.VMEM((ROWS * 8, HD), F32),
                pltpu.VMEM((ROWS * 8, HD), F32),
                pltpu.VMEM((ROWS * 8, HD), F32),
                pltpu.VMEM((LAYERS + 1, ROWS, D), BF16),
                pltpu.VMEM((LAYERS, ROWS, D), BF16),
                pltpu.VMEM((4, 2, ROWS, D), BF16),
                pltpu.VMEM((4, 2, ROWS, D), BF16),
                pltpu.VMEM((2 * ROWS, FFN), BF16),
                dma((SLOTS,)), dma((SLOTS,)), dma((2, 2)), dma((3,)), dma((3,)), dma((3,)),
                dma((LAYERS, 2)), dma((4, 2, 2)), dma((4, 2)), dma((LAYERS,)),
                pltpu.VMEM((LAYERS, D), F32), pltpu.VMEM((LAYERS, D), F32), pltpu.VMEM((1, ROWS), jnp.int32), dma((4,)),
            ],
            compiler_params=pltpu.CompilerParams(collective_id=0, has_side_effects=True, vmem_limit_bytes=67043328),
        )(hidden, norm_attn, norm_ffn, seq_lens.reshape(1, ROWS), w_qkv, w_out, kc, vc, w_gate, w_up, w_down)

    return jax.shard_map(per_device, mesh=mesh, in_specs=(row_spec, rep_spec, rep_spec, rep_spec, rep_spec, cache_spec, cache_spec, len_spec, owned_spec, owned_spec, owned_spec), out_specs=row_spec, check_vma=False)
```

```python
import jax
import jax.numpy as jnp
from jax import lax
from jax.experimental import pallas as pl
from jax.experimental.pallas import tpu as pltpu
from jax.sharding import PartitionSpec as P

NORM_EPS = 1e-5
F32 = jnp.float32
BF16 = jnp.bfloat16
LAYERS = 4
ROWS = 64
D = 768
HD = 128
HEADS = 6
CACHE = 256
QKV = 1280
FFN = 2048
CHUNK = 16
CHUNKS = ROWS // CHUNK
SLOTS = 6
HALF = ROWS // 2
FBLK = 512
NT = (((1,), (1,)), ((), ()))


def rms(rows_bf16, gain):
    vals = rows_bf16.astype(F32)
    inv = lax.rsqrt(jnp.mean(vals * vals, axis=-1, keepdims=True) + NORM_EPS)
    return (vals * inv * gain).astype(BF16)


def kernel(hid_in, ga_in, gf_in, lens_in, wqkv, wout, kc, vc, wg, wu, wd, out,
           kbuf, vbuf, qkvw, outw, fg, fu, fd, q3, k3, v3, o3, len3, xbuf, hbuf, hin, xo, zbuf,
           ksem, vsem, wsem, fsem, fs_sem, fr_sem, hs_sem, hr_sem, xs_sem, xr_sem, ga, gf, lens, isem):
    me = lax.axis_index("data")
    chip, core = me // 2, me % 2
    mate, peer = chip * 2 + (1 - core), (me + 2) % 4
    mesh_id = pl.DeviceIdType.MESH

    def kcopy(c, which):
        layer, part, slot = c // CHUNKS, c % CHUNKS, c % SLOTS
        src = pl.ds(pl.multiple_of(part * CHUNK, CHUNK), CHUNK)
        if which == 0:
            return pltpu.make_async_copy(kc.at[layer, src], kbuf.at[slot], ksem.at[slot])
        return pltpu.make_async_copy(vc.at[layer, src], vbuf.at[slot], vsem.at[slot])

    def wcopy(layer, which):
        slot = layer % 2
        if which == 0:
            return pltpu.make_async_copy(wqkv.at[layer], qkvw.at[slot], wsem.at[slot, 0])
        return pltpu.make_async_copy(wout.at[layer], outw.at[slot], wsem.at[slot, 1])

    ffn_parts = ((wg, fg), (wu, fu), (wd, fd))

    def fcopy(k):
        return pltpu.make_async_copy(ffn_parts[k][0].at[0], ffn_parts[k][1].at[core], fsem.at[k])

    def fsend(k, idx):
        return pltpu.make_async_remote_copy(
            src_ref=ffn_parts[k][0].at[0], dst_ref=ffn_parts[k][1].at[idx], send_sem=fs_sem.at[k], recv_sem=fr_sem.at[k],
            device_id={"data": mate}, device_id_type=mesh_id)

    def send_h(layer, half, dst, slot, pos):
        rows = pl.ds(pl.multiple_of(half * HALF, HALF), HALF)
        return pltpu.make_async_remote_copy(
            src_ref=hbuf.at[layer, rows], dst_ref=hin.at[slot, pos, rows],
            send_sem=hs_sem.at[layer, half], recv_sem=hr_sem.at[slot, pos, half],
            device_id={"data": dst}, device_id_type=mesh_id)

    def send_x(layer, dst, slot, pos):
        return pltpu.make_async_remote_copy(
            src_ref=xo.at[slot, pos], dst_ref=xbuf.at[layer + 1], send_sem=xs_sem.at[slot, pos], recv_sem=xr_sem.at[layer],
            device_id={"data": dst}, device_id_type=mesh_id)

    small = [pltpu.make_async_copy(src, dst, isem.at[k]) for k, (src, dst) in enumerate(
        ((hid_in, xbuf.at[0]), (ga_in, ga), (gf_in, gf), (lens_in, lens)))]
    for cp in small:
        cp.start()
    wcopy(0, 0).start()
    for c in range(3):
        for which in range(2):
            kcopy(c, which).start()

    barrier = pltpu.get_barrier_semaphore()
    for step in range(1, 4):
        pl.semaphore_signal(barrier, inc=1, device_id={"data": (me + step) % 4}, device_id_type=mesh_id)
    for cp in small:
        cp.wait()

    pick = (lax.broadcasted_iota(jnp.int32, (ROWS * 8, ROWS), 0) // 8 == lax.broadcasted_iota(jnp.int32, (ROWS * 8, ROWS), 1))
    lrow = jnp.broadcast_to(lens[...].astype(F32), (HD, ROWS)).astype(BF16)
    len3[...] = 2.0 * lax.dot_general(pick.astype(F32).astype(BF16), lrow, NT, preferred_element_type=F32)
    zrow = jnp.zeros((ROWS, HD), F32)
    for j in (6, 7):
        for ref in (q3, k3, v3):
            ref[pl.ds(j, ROWS, stride=8), :] = zrow
    pl.semaphore_wait(barrier, 3)

    def is_local(layer):
        return (chip == layer // 2) & ((layer > 0) | (me == 0))

    def layer_step(layer, carry):
        wslot = layer % 2
        local = is_local(layer)
        dst = jnp.where(layer == 0, 0, peer)
        slot = jnp.where((layer == 0) & (me == 1), 0, 2 * (layer % 2) + 1)
        pos = jnp.where(layer == 0, core, 0)
        wcopy(layer, 0).wait()

        @pl.when((layer > 0) & jnp.logical_not(is_local(layer - 1)))
        def _():
            send_x(layer - 1, me, 0, 0).wait_recv()

        normed = rms(xbuf[layer], ga[pl.ds(layer, 1), :])
        qkv = jnp.dot(normed, qkvw[wslot], preferred_element_type=F32).astype(BF16).astype(F32)
        for j in range(HEADS):
            rows8 = pl.ds(j, ROWS, stride=8)
            kv = j * 2 // HEADS
            q3[rows8, :] = qkv[:, j * HD:(j + 1) * HD]
            k3[rows8, :] = qkv[:, (HEADS + kv) * HD:(HEADS + kv + 1) * HD]
            v3[rows8, :] = qkv[:, (HEADS + 2 + kv) * HD:(HEADS + 3 + kv) * HD]

        def issue_start(c):
            @pl.when(c == 0)
            def _():
                for which in range(2):
                    kcopy(3, which).start()
                wcopy(0, 1).start()

            @pl.when((c == 0) & (me == 1))
            def _():
                for k in range(3):
                    fsend(k, core).start()

            @pl.when((c == jnp.where(chip == 0, 0, CHUNKS)) & (me != 1))
            def _():
                for k in range(3):
                    fcopy(k).start()

        def issue_end(c):
            @pl.when(c == 0)
            def _():
                for early in range(4, SLOTS):
                    for which in range(2):
                        kcopy(early, which).start()

            @pl.when(c + SLOTS < LAYERS * CHUNKS)
            def _():
                for k in range(2):
                    for which in range(2):
                        kcopy(c + k + SLOTS, which).start()

        def chunk_math(part):
            cslot = (layer * CHUNKS + part) % SLOTS
            rows = pl.ds(pl.multiple_of(part * (CHUNK * 8), CHUNK * 8), CHUNK * 8)
            qc = q3[rows, :]
            s_self = jnp.sum(qc * k3[rows, :], axis=-1, keepdims=True) * (HD ** -0.5)
            zero = jnp.zeros((8, HD), F32)
            scores = []
            for i in range(CHUNK // 2):
                qa = qc[16 * i:16 * i + 8]
                qb = qc[16 * i + 8:16 * i + 16]
                lhs = jnp.concatenate([jnp.concatenate([qa, zero], 1), jnp.concatenate([zero, qb], 1)], 0).astype(BF16)
                keys = jnp.concatenate([kbuf[cslot, 2 * i], kbuf[cslot, 2 * i + 1]], 1)
                scores.append(lax.dot_general(lhs, keys, NT, preferred_element_type=F32))
            s = jnp.concatenate(scores, 0) * (HD ** -0.5)
            col = lax.broadcasted_iota(jnp.int32, s.shape, 1)
            head = lax.broadcasted_iota(jnp.int32, s.shape, 0) % 8
            lim = len3[rows, :]
            lim = jnp.concatenate([lim] * (2 * CACHE // HD), 1)
            good = (col % 2 == head // 3) & (col.astype(F32) < lim)
            s = jnp.where(good, s, -1e30)
            top = jnp.maximum(jnp.max(s, axis=-1, keepdims=True), s_self)
            e = jnp.exp(s - top)
            e_self = jnp.exp(s_self - top)
            inv = 1.0 / (jnp.sum(e, axis=-1, keepdims=True) + e_self)
            p = (e * inv).astype(BF16)
            self_out = (e_self * inv).astype(BF16).astype(F32) * v3[rows, :]
            outs = []
            for i in range(CHUNK // 2):
                vals = jnp.concatenate([vbuf[cslot, 2 * i], vbuf[cslot, 2 * i + 1]], 1)
                o = jnp.dot(p[16 * i:16 * i + 16], vals, preferred_element_type=F32)
                outs += [o[0:8, 0:HD], o[8:16, HD:2 * HD]]
            o3[rows, :] = jnp.concatenate(outs, 0) + self_out

        def chunk_pair(part):
            issue_start(layer * CHUNKS + part)
            for k in range(2):
                for which in range(2):
                    kcopy(layer * CHUNKS + part + k, which).wait()
            for k in range(2):
                chunk_math(part + k)
            issue_end(layer * CHUNKS + part)

        def half_att(half, carry):
            chunk_pair(half * (CHUNKS // 2))

            @pl.when(half == 0)
            def _():
                wcopy(layer, 1).wait()

            base = half * (HALF * 8)
            attn = jnp.concatenate([o3[pl.ds(base + j, HALF, stride=8), :] for j in range(HEADS)], 1).astype(BF16)
            proj = jnp.dot(attn, outw[wslot], preferred_element_type=F32)
            rows = pl.ds(pl.multiple_of(half * HALF, HALF), HALF)
            mid = (xbuf[layer, rows].astype(F32) + proj).astype(BF16)

            @pl.when(local)
            def _():
                hin[2 * (layer % 2), 0, rows] = mid

            @pl.when(jnp.logical_not(local))
            def _():
                hbuf[layer, rows] = mid
                send_h(layer, half, dst, slot, pos).start()
            return carry

        lax.fori_loop(0, 2, half_att, 0)

        @pl.when(layer + 1 < LAYERS)
        def _():
            for which in range(2):
                wcopy(layer + 1, which).start()

        @pl.when((layer == 0) & (me != 0))
        def _():
            @pl.when(me == 1)
            def _():
                for k in range(3):
                    fcopy(k).start()

            @pl.when(me != 1)
            def _():
                for k in range(3):
                    fsend(k, core).start()

        def ffn_step(turn, carry):
            serve0 = (layer == 2) | (turn == 1)
            serve1 = (layer != 2) & (turn == 0)
            serve = jnp.where(chip == 0, serve0, serve1)
            tl = jnp.where(chip == 0, jnp.where(layer == 2, 1, layer), jnp.where(layer == 1, 2, layer))
            todo0 = jnp.where(turn == 0, layer < 3, layer == 0) & ((layer > 0) | (me == 0))
            todo1 = jnp.where(turn == 0, layer > 0, layer == 3)
            todo = jnp.where(chip == 0, todo0, todo1)

            @pl.when(todo)
            def _():
                idx = tl % 2
                fslot = 2 * idx + jnp.where(serve, 1, 0)
                both = tl == 0

                @pl.when(serve)
                def _():
                    for half in range(2):
                        send_h(0, half, me, fslot, 0).wait_recv()

                @pl.when(both)
                def _():
                    for half in range(2):
                        send_h(0, half, me, fslot, 1).wait_recv()

                first = jnp.where(serve, 1, 0) == chip

                @pl.when(first & (idx == core))
                def _():
                    for k in range(3):
                        fcopy(k).wait()

                @pl.when(first & (idx != core))
                def _():
                    for k in range(3):
                        fsend(k, idx).wait_recv()

                def ffn(count):
                    rows_h = hin[fslot, 0:count].reshape(count * ROWS, D)
                    n2 = rms(rows_h, gf[pl.ds(tl, 1), :])
                    zrows = slice(0, count * ROWS)
                    for b in range(FFN // FBLK):
                        cols = slice(b * FBLK, (b + 1) * FBLK)
                        a = jnp.dot(n2, fg[idx, :, cols], preferred_element_type=F32)
                        u = jnp.dot(n2, fu[idx, :, cols], preferred_element_type=F32)
                        zbuf[zrows, cols] = (a * jax.nn.sigmoid(a) * u).astype(BF16)
                    down = jnp.dot(zbuf[zrows, :], fd[idx], preferred_element_type=F32)
                    xo[fslot, 0:count] = (rows_h.astype(F32) + down).astype(BF16).reshape(count, ROWS, D)

                @pl.when(both)
                def _():
                    ffn(2)

                @pl.when(jnp.logical_not(both))
                def _():
                    ffn(1)

                @pl.when(serve)
                def _():
                    send_x(tl, peer, fslot, 0).start()

                @pl.when(jnp.logical_not(serve))
                def _():
                    xbuf[tl + 1] = xo[fslot, 0]

                @pl.when(both)
                def _():
                    send_x(tl, jnp.where(serve, 3, 1), fslot, 1).start()
            return carry

        lax.fori_loop(0, 2, ffn_step, 0)
        return carry

    lax.fori_loop(0, LAYERS, layer_step, 0)

    @pl.when(chip == 0)
    def _():
        send_x(LAYERS - 1, me, 0, 0).wait_recv()

    out[...] = xbuf[LAYERS]

    for layer in range(LAYERS):
        @pl.when(jnp.logical_not(is_local(layer)))
        def _():
            for half in range(2):
                send_h(layer, half, 0, 0, 0).wait_send()

    @pl.when(me != 0)
    def _():
        send_x(0, me, 3, 0).wait_send()
        for k in range(3):
            fsend(k, core).wait_send()

    @pl.when(chip == 1)
    def _():
        send_x(0, me, 1, 0).wait_send()

    @pl.when(me == 0)
    def _():
        for slot, pos in ((0, 1), (1, 0), (1, 1), (3, 0)):
            send_x(0, me, slot, pos).wait_send()


def solution(mesh):
    row_spec = P(('grp', 'data'), None)
    rep_spec = P()
    cache_spec = P(None, ('grp', 'data'))
    len_spec = P(('grp', 'data'))
    owned_spec = P('data')

    def per_device(hidden, w_qkv, w_out, norm_attn, norm_ffn, k_cache, v_cache, seq_lens, w_gate, w_up, w_down):
        kc = k_cache.reshape(LAYERS, ROWS, 2 * CACHE, HD)
        vc = v_cache.reshape(LAYERS, ROWS, 2 * CACHE, HD)
        vm = pl.BlockSpec(memory_space=pltpu.VMEM)
        anys = pl.BlockSpec(memory_space=pl.ANY)
        dma = pltpu.SemaphoreType.DMA
        return pl.pallas_call(
            kernel,
            out_shape=jax.ShapeDtypeStruct((ROWS, D), BF16),
            in_specs=[anys] * 11,
            out_specs=vm,
            scratch_shapes=[
                pltpu.VMEM((SLOTS, CHUNK, 2 * CACHE, HD), BF16),
                pltpu.VMEM((SLOTS, CHUNK, 2 * CACHE, HD), BF16),
                pltpu.VMEM((2, D, QKV), BF16),
                pltpu.VMEM((2, D, D), BF16),
                pltpu.VMEM((2, D, FFN), BF16),
                pltpu.VMEM((2, D, FFN), BF16),
                pltpu.VMEM((2, FFN, D), BF16),
                pltpu.VMEM((ROWS * 8, HD), F32),
                pltpu.VMEM((ROWS * 8, HD), F32),
                pltpu.VMEM((ROWS * 8, HD), F32),
                pltpu.VMEM((ROWS * 8, HD), F32),
                pltpu.VMEM((ROWS * 8, HD), F32),
                pltpu.VMEM((LAYERS + 1, ROWS, D), BF16),
                pltpu.VMEM((LAYERS, ROWS, D), BF16),
                pltpu.VMEM((4, 2, ROWS, D), BF16),
                pltpu.VMEM((4, 2, ROWS, D), BF16),
                pltpu.VMEM((2 * ROWS, FFN), BF16),
                dma((SLOTS,)), dma((SLOTS,)), dma((2, 2)), dma((3,)), dma((3,)), dma((3,)),
                dma((LAYERS, 2)), dma((4, 2, 2)), dma((4, 2)), dma((LAYERS,)),
                pltpu.VMEM((LAYERS, D), F32), pltpu.VMEM((LAYERS, D), F32), pltpu.VMEM((1, ROWS), jnp.int32), dma((4,)),
            ],
            compiler_params=pltpu.CompilerParams(collective_id=0, has_side_effects=True, vmem_limit_bytes=67043328),
        )(hidden, norm_attn, norm_ffn, seq_lens.reshape(1, ROWS), w_qkv, w_out, kc, vc, w_gate, w_up, w_down)

    return jax.shard_map(per_device, mesh=mesh, in_specs=(row_spec, rep_spec, rep_spec, rep_spec, rep_spec, cache_spec, cache_spec, len_spec, owned_spec, owned_spec, owned_spec), out_specs=row_spec, check_vma=False)
```

```python
import jax
import jax.numpy as jnp
from jax import lax
from jax.experimental import pallas as pl
from jax.experimental.pallas import tpu as pltpu
from jax.sharding import PartitionSpec as P

NORM_EPS = 1e-5
EXP_SCALE = 1.4426950408889634 * 128 ** -0.5
F32 = jnp.float32
BF16 = jnp.bfloat16
LAYERS = 4
ROWS = 64
D = 768
HD = 128
HEADS = 6
CACHE = 256
QKV = 1280
FFN = 2048
CHUNK = 16
CHUNKS = ROWS // CHUNK
SLOTS = 6
HALF = ROWS // 2
FBLK = 512
NT = (((1,), (1,)), ((), ()))


def rms(rows_bf16, gain):
    vals = rows_bf16.astype(F32)
    inv = lax.rsqrt(jnp.mean(vals * vals, axis=-1, keepdims=True) + NORM_EPS)
    return (vals * inv * gain).astype(BF16)


def kernel(hid_in, ga_in, gf_in, lens_in, wqkv, wout, kc, vc, wg, wu, wd, out,
           kbuf, vbuf, qkvw, outw, fg, fu, fd, q3, k3, v3, o3, len3, xbuf, hbuf, hin, xo, zbuf,
           ksem, vsem, wsem, fsem, fs_sem, fr_sem, hs_sem, hr_sem, xs_sem, xr_sem, ga, gf, lens, isem):
    me = lax.axis_index("data")
    chip, core = lax.shift_right_logical(me, 1), lax.rem(me, 2)
    mate, peer = chip * 2 + (1 - core), lax.rem(me + 2, 4)
    mesh_id = pl.DeviceIdType.MESH

    def kcopy(c, which):
        layer, part, slot = lax.shift_right_logical(jnp.int32(c), 2), lax.rem(jnp.int32(c), CHUNKS), lax.rem(jnp.int32(c), SLOTS)
        src = pl.ds(pl.multiple_of(part * CHUNK, CHUNK), CHUNK)
        if which == 0:
            return pltpu.make_async_copy(kc.at[layer, src], kbuf.at[slot], ksem.at[slot])
        return pltpu.make_async_copy(vc.at[layer, src], vbuf.at[slot], vsem.at[slot])

    def wcopy(layer, which):
        slot = lax.rem(jnp.int32(layer), 2)
        if which == 0:
            return pltpu.make_async_copy(wqkv.at[layer], qkvw.at[slot], wsem.at[slot, 0])
        return pltpu.make_async_copy(wout.at[layer], outw.at[slot], wsem.at[slot, 1])

    ffn_parts = ((wg, fg), (wu, fu), (wd, fd))

    def fcopy(k):
        return pltpu.make_async_copy(ffn_parts[k][0].at[0], ffn_parts[k][1].at[core], fsem.at[k])

    def fsend(k, idx):
        return pltpu.make_async_remote_copy(
            src_ref=ffn_parts[k][0].at[0], dst_ref=ffn_parts[k][1].at[idx], send_sem=fs_sem.at[k], recv_sem=fr_sem.at[k],
            device_id={"data": mate}, device_id_type=mesh_id)

    def send_h(layer, half, dst, slot, pos):
        rows = pl.ds(pl.multiple_of(half * HALF, HALF), HALF)
        return pltpu.make_async_remote_copy(
            src_ref=hbuf.at[layer, rows], dst_ref=hin.at[slot, pos, rows],
            send_sem=hs_sem.at[layer, half], recv_sem=hr_sem.at[slot, pos, half],
            device_id={"data": dst}, device_id_type=mesh_id)

    def send_x(layer, dst, slot, pos):
        return pltpu.make_async_remote_copy(
            src_ref=xo.at[slot, pos], dst_ref=xbuf.at[layer + 1], send_sem=xs_sem.at[slot, pos], recv_sem=xr_sem.at[layer],
            device_id={"data": dst}, device_id_type=mesh_id)

    small = [pltpu.make_async_copy(src, dst, isem.at[k]) for k, (src, dst) in enumerate(
        ((hid_in, xbuf.at[0]), (ga_in, ga), (gf_in, gf), (lens_in, lens)))]
    for cp in small:
        cp.start()
    wcopy(0, 0).start()
    for c in range(3):
        for which in range(2):
            kcopy(c, which).start()

    barrier = pltpu.get_barrier_semaphore()
    for step in range(1, 4):
        pl.semaphore_signal(barrier, inc=1, device_id={"data": lax.rem(me + step, 4)}, device_id_type=mesh_id)
    for cp in small:
        cp.wait()

    pick = (lax.broadcasted_iota(jnp.int32, (ROWS * 8, ROWS), 0) // 8 == lax.broadcasted_iota(jnp.int32, (ROWS * 8, ROWS), 1))
    lrow = jnp.broadcast_to(lens[...].astype(F32), (HD, ROWS)).astype(BF16)
    len3[...] = 2.0 * lax.dot_general(pick.astype(F32).astype(BF16), lrow, NT, preferred_element_type=F32)
    zrow = jnp.zeros((ROWS, HD), F32)
    for j in (6, 7):
        for ref in (q3, k3, v3):
            ref[pl.ds(j, ROWS, stride=8), :] = zrow
    pl.semaphore_wait(barrier, 3)

    @pl.when(me != 0)
    def _():
        fsend(0, core).start()

    def is_local(layer):
        return (chip == layer // 2) & ((layer > 0) | (me == 0))

    def layer_step(layer, carry):
        wslot = lax.rem(jnp.int32(layer), 2)
        local = is_local(layer)
        dst = jnp.where(layer == 0, 0, peer)
        slot = jnp.where((layer == 0) & (me == 1), 0, 2 * wslot + 1)
        pos = jnp.where(layer == 0, core, 0)
        wcopy(layer, 0).wait()

        @pl.when((layer > 0) & jnp.logical_not(is_local(layer - 1)))
        def _():
            send_x(layer - 1, me, 0, 0).wait_recv()

        normed = rms(xbuf[layer], ga[pl.ds(layer, 1), :])
        qkv = jnp.dot(normed, qkvw[wslot], preferred_element_type=F32).astype(BF16).astype(F32)
        for j in range(HEADS):
            rows8 = pl.ds(j, ROWS, stride=8)
            kv = j * 2 // HEADS
            q3[rows8, :] = qkv[:, j * HD:(j + 1) * HD]
            k3[rows8, :] = qkv[:, (HEADS + kv) * HD:(HEADS + kv + 1) * HD]
            v3[rows8, :] = qkv[:, (HEADS + 2 + kv) * HD:(HEADS + 3 + kv) * HD]

        def refill(c, ok=True):
            @pl.when((c < LAYERS * CHUNKS) & ok)
            def _():
                for which in range(2):
                    kcopy(c, which).start()

        col8 = lax.broadcasted_iota(jnp.int32, (8, 2 * CACHE), 1)
        kv8 = jnp.where(lax.broadcasted_iota(jnp.int32, (8, 2 * CACHE), 0) < HEADS // 2, 0, 1)
        cols8 = jnp.where((col8 & 1) == kv8, col8.astype(F32), 4.0 * CACHE)[None]

        def chunk_math(part):
            cslot = lax.rem(layer * CHUNKS + part, SLOTS)
            rows = pl.ds(pl.multiple_of(part * (CHUNK * 8), CHUNK * 8), CHUNK * 8)
            qc = q3[rows, :]
            s_self = jnp.sum(qc * k3[rows, :], axis=-1, keepdims=True).reshape(CHUNK, 8, 1)
            zero = jnp.zeros((8, HD), F32)
            scores = []
            for i in range(CHUNK // 2):
                qa = qc[16 * i:16 * i + 8]
                qb = qc[16 * i + 8:16 * i + 16]
                lhs = jnp.concatenate([jnp.concatenate([qa, zero], 1), jnp.concatenate([zero, qb], 1)], 0).astype(BF16)
                keys = jnp.concatenate([kbuf[cslot, 2 * i], kbuf[cslot, 2 * i + 1]], 1)
                scores.append(lax.dot_general(lhs, keys, NT, preferred_element_type=F32))
            s = jnp.concatenate(scores, 0).reshape(CHUNK, 8, 2 * CACHE)
            lim = jnp.concatenate([len3[rows, :].reshape(CHUNK, 8, HD)] * (2 * CACHE // HD), 2)
            s = jnp.where(cols8 < lim, s, -1e30 * HD ** 0.5)
            top = jnp.maximum(jnp.max(s, axis=-1, keepdims=True), s_self)
            e = jnp.exp2((s - top) * EXP_SCALE)
            e_self = jnp.exp2((s_self - top) * EXP_SCALE)
            inv = 1.0 / (jnp.sum(e, axis=-1, keepdims=True) + e_self)
            p = (e * inv).reshape(CHUNK * 8, 2 * CACHE).astype(BF16)
            self_out = (e_self * inv).astype(BF16).astype(F32).reshape(CHUNK * 8, 1) * v3[rows, :]
            outs = []
            for i in range(CHUNK // 2):
                vals = jnp.concatenate([vbuf[cslot, 2 * i], vbuf[cslot, 2 * i + 1]], 1)
                o = jnp.dot(p[16 * i:16 * i + 16], vals, preferred_element_type=F32)
                outs += [o[0:8, 0:HD], o[8:16, HD:2 * HD]]
            o3[rows, :] = jnp.concatenate(outs, 0) + self_out

        def chunk_pair(part):
            for k in range(2):
                for which in range(2):
                    kcopy(layer * CHUNKS + part + k, which).wait()
            for k in range(2):
                chunk_math(part + k)

        def half_att(half, carry):
            @pl.when(half == 0)
            def _():
                @pl.when(layer == 0)
                def _():
                    for which in range(2):
                        kcopy(3, which).start()
                    wcopy(0, 1).start()

                @pl.when(jnp.where(me == 0, layer == 0, (chip == 1) & (layer == 1)))
                def _():
                    for k in range(3):
                        fcopy(k).start()

            @pl.when(half == 1)
            def _():
                @pl.when(layer == 0)
                def _():
                    for c in (4, 5):
                        for which in range(2):
                            kcopy(c, which).start()

                refill(layer * CHUNKS + 6)

            chunk_pair(half * (CHUNKS // 2))

            @pl.when(half == 0)
            def _():
                wcopy(layer, 1).wait()

            base = half * (HALF * 8)
            attn = jnp.concatenate([o3[pl.ds(base + j, HALF, stride=8), :] for j in range(HEADS)], 1).astype(BF16)
            proj = jnp.dot(attn, outw[wslot], preferred_element_type=F32)
            rows = pl.ds(pl.multiple_of(half * HALF, HALF), HALF)
            mid = (xbuf[layer, rows].astype(F32) + proj).astype(BF16)

            @pl.when(local)
            def _():
                hin[2 * wslot, 0, rows] = mid

            @pl.when(jnp.logical_not(local))
            def _():
                hbuf[layer, rows] = mid
                send_h(layer, half, dst, slot, pos).start()
            return carry

        lax.fori_loop(0, 2, half_att, 0)

        @pl.when(layer + 1 < LAYERS)
        def _():
            for which in range(2):
                wcopy(layer + 1, which).start()

        @pl.when((layer == 0) & (me != 0))
        def _():
            for k in range(1, 3):
                fsend(k, core).start()

        @pl.when((layer == 0) & (me == 1))
        def _():
            for k in range(3):
                fcopy(k).start()

        refill(layer * CHUNKS + 7)

        def ffn_step(turn, carry):
            serve0 = (layer == 2) | (turn == 1)
            serve1 = (layer != 2) & (turn == 0)
            serve = jnp.where(chip == 0, serve0, serve1)
            tl = jnp.where(chip == 0, jnp.where(layer == 2, 1, layer), jnp.where(layer == 1, 2, layer))
            todo0 = jnp.where(turn == 0, layer < 3, layer == 0) & ((layer > 0) | (me == 0))
            todo1 = jnp.where(turn == 0, layer > 0, layer == 3)
            todo = jnp.where(chip == 0, todo0, todo1)

            @pl.when(todo)
            def _():
                idx = lax.rem(tl, 2)
                fslot = 2 * idx + jnp.where(serve, 1, 0)
                both = tl == 0

                @pl.when(serve)
                def _():
                    for half in range(2):
                        send_h(0, half, me, fslot, 0).wait_recv()

                @pl.when(both)
                def _():
                    for half in range(2):
                        send_h(0, half, me, fslot, 1).wait_recv()

                first = jnp.where(serve, 1, 0) == chip

                @pl.when(first & (idx == core))
                def _():
                    for k in range(3):
                        fcopy(k).wait()

                @pl.when(first & (idx != core))
                def _():
                    for k in range(3):
                        fsend(k, idx).wait_recv()

                def ffn(count):
                    rows_h = hin[fslot, 0:count].reshape(count * ROWS, D)
                    n2 = rms(rows_h, gf[pl.ds(tl, 1), :])
                    zrows = slice(0, count * ROWS)
                    for b in range(FFN // FBLK):
                        cols = slice(b * FBLK, (b + 1) * FBLK)
                        a = jnp.dot(n2, fg[idx, :, cols], preferred_element_type=F32)
                        u = jnp.dot(n2, fu[idx, :, cols], preferred_element_type=F32)
                        zbuf[zrows, cols] = (a * jax.nn.sigmoid(a) * u).astype(BF16)
                    down = jnp.dot(zbuf[zrows, :], fd[idx], preferred_element_type=F32)
                    xo[fslot, 0:count] = (rows_h.astype(F32) + down).astype(BF16).reshape(count, ROWS, D)

                @pl.when(both)
                def _():
                    ffn(2)

                @pl.when(jnp.logical_not(both))
                def _():
                    ffn(1)

                @pl.when(serve)
                def _():
                    send_x(tl, peer, fslot, 0).start()

                @pl.when(jnp.logical_not(serve))
                def _():
                    xbuf[tl + 1] = xo[fslot, 0]

                @pl.when(both)
                def _():
                    send_x(tl, jnp.where(serve, 3, 1), fslot, 1).start()
            return carry

        refill(layer * CHUNKS + 8)
        lax.fori_loop(0, 2, ffn_step, 0)
        refill(layer * CHUNKS + 9)
        return carry

    lax.fori_loop(0, LAYERS, layer_step, 0)

    @pl.when(chip == 0)
    def _():
        send_x(LAYERS - 1, me, 0, 0).wait_recv()

    out[...] = xbuf[LAYERS]

    for layer in range(LAYERS):
        @pl.when(jnp.logical_not(is_local(layer)))
        def _():
            for half in range(2):
                send_h(layer, half, 0, 0, 0).wait_send()

    @pl.when(me != 0)
    def _():
        send_x(0, me, 3, 0).wait_send()
        for k in range(3):
            fsend(k, core).wait_send()

    @pl.when(chip == 1)
    def _():
        send_x(0, me, 1, 0).wait_send()

    @pl.when(me == 0)
    def _():
        for slot, pos in ((0, 1), (1, 0), (1, 1), (3, 0)):
            send_x(0, me, slot, pos).wait_send()


def solution(mesh):
    row_spec = P(('grp', 'data'), None)
    rep_spec = P()
    cache_spec = P(None, ('grp', 'data'))
    len_spec = P(('grp', 'data'))
    owned_spec = P('data')

    def per_device(hidden, w_qkv, w_out, norm_attn, norm_ffn, k_cache, v_cache, seq_lens, w_gate, w_up, w_down):
        kc = k_cache.reshape(LAYERS, ROWS, 2 * CACHE, HD)
        vc = v_cache.reshape(LAYERS, ROWS, 2 * CACHE, HD)
        vm = pl.BlockSpec(memory_space=pltpu.VMEM)
        anys = pl.BlockSpec(memory_space=pl.ANY)
        dma = pltpu.SemaphoreType.DMA
        return pl.pallas_call(
            kernel,
            out_shape=jax.ShapeDtypeStruct((ROWS, D), BF16),
            in_specs=[anys] * 11,
            out_specs=vm,
            scratch_shapes=[
                pltpu.VMEM((SLOTS, CHUNK, 2 * CACHE, HD), BF16),
                pltpu.VMEM((SLOTS, CHUNK, 2 * CACHE, HD), BF16),
                pltpu.VMEM((2, D, QKV), BF16),
                pltpu.VMEM((2, D, D), BF16),
                pltpu.VMEM((2, D, FFN), BF16),
                pltpu.VMEM((2, D, FFN), BF16),
                pltpu.VMEM((2, FFN, D), BF16),
                pltpu.VMEM((ROWS * 8, HD), F32),
                pltpu.VMEM((ROWS * 8, HD), F32),
                pltpu.VMEM((ROWS * 8, HD), F32),
                pltpu.VMEM((ROWS * 8, HD), F32),
                pltpu.VMEM((ROWS * 8, HD), F32),
                pltpu.VMEM((LAYERS + 1, ROWS, D), BF16),
                pltpu.VMEM((LAYERS, ROWS, D), BF16),
                pltpu.VMEM((4, 2, ROWS, D), BF16),
                pltpu.VMEM((4, 2, ROWS, D), BF16),
                pltpu.VMEM((2 * ROWS, FFN), BF16),
                dma((SLOTS,)), dma((SLOTS,)), dma((2, 2)), dma((3,)), dma((3,)), dma((3,)),
                dma((LAYERS, 2)), dma((4, 2, 2)), dma((4, 2)), dma((LAYERS,)),
                pltpu.VMEM((LAYERS, D), F32), pltpu.VMEM((LAYERS, D), F32), pltpu.VMEM((1, ROWS), jnp.int32), dma((4,)),
            ],
            compiler_params=pltpu.CompilerParams(collective_id=0, has_side_effects=True, vmem_limit_bytes=67043328),
        )(hidden, norm_attn, norm_ffn, seq_lens.reshape(1, ROWS), w_qkv, w_out, kc, vc, w_gate, w_up, w_down)

    return jax.shard_map(per_device, mesh=mesh, in_specs=(row_spec, rep_spec, rep_spec, rep_spec, rep_spec, cache_spec, cache_spec, len_spec, owned_spec, owned_spec, owned_spec), out_specs=row_spec, check_vma=False)
```

```python
import jax
import jax.numpy as jnp
from jax import lax
from jax.experimental import pallas as pl
from jax.experimental.pallas import tpu as pltpu
from jax.sharding import PartitionSpec as P

NORM_EPS = 1e-5
EXP_SCALE = 1.4426950408889634 * 128 ** -0.5
F32 = jnp.float32
BF16 = jnp.bfloat16
LAYERS = 4
ROWS = 64
D = 768
HD = 128
HEADS = 6
CACHE = 256
QKV = 1280
FFN = 2048
CHUNK = 16
CHUNKS = ROWS // CHUNK
SLOTS = 6
HALF = ROWS // 2
FBLK = 512
NT = (((1,), (1,)), ((), ()))


def rms(rows_bf16, gain):
    vals = rows_bf16.astype(F32)
    inv = lax.rsqrt(jnp.mean(vals * vals, axis=-1, keepdims=True) + NORM_EPS)
    return (vals * inv * gain).astype(BF16)


def kernel(hid_in, ga_in, gf_in, lens_in, wqkv, wout, kc, vc, wg, wu, wd, out,
           kbuf, vbuf, qkvw, outw, fg, fu, fd, q3, k3, v3, o3, len3, xbuf, hbuf, hin, xo, zbuf,
           ksem, vsem, wsem, fsem, fs_sem, fr_sem, hs_sem, hr_sem, xs_sem, xr_sem, ga, gf, lens, isem):
    me = lax.axis_index("data")
    chip, core = lax.shift_right_logical(me, 1), lax.rem(me, 2)
    mate, peer = chip * 2 + (1 - core), lax.rem(me + 2, 4)
    mesh_id = pl.DeviceIdType.MESH

    def kcopy(c, which):
        layer, part, slot = lax.shift_right_logical(jnp.int32(c), 2), lax.rem(jnp.int32(c), CHUNKS), lax.rem(jnp.int32(c), SLOTS)
        src = pl.ds(pl.multiple_of(part * CHUNK, CHUNK), CHUNK)
        if which == 0:
            return pltpu.make_async_copy(kc.at[layer, src], kbuf.at[slot], ksem.at[slot])
        return pltpu.make_async_copy(vc.at[layer, src], vbuf.at[slot], vsem.at[slot])

    def wcopy(layer, which):
        slot = lax.rem(jnp.int32(layer), 2)
        if which == 0:
            return pltpu.make_async_copy(wqkv.at[layer], qkvw.at[slot], wsem.at[slot, 0])
        return pltpu.make_async_copy(wout.at[layer], outw.at[slot], wsem.at[slot, 1])

    ffn_parts = ((wg, fg), (wu, fu), (wd, fd))

    def fcopy(k):
        return pltpu.make_async_copy(ffn_parts[k][0].at[0], ffn_parts[k][1].at[core], fsem.at[k])

    def fsend(k, idx):
        return pltpu.make_async_remote_copy(
            src_ref=ffn_parts[k][0].at[0], dst_ref=ffn_parts[k][1].at[idx], send_sem=fs_sem.at[k], recv_sem=fr_sem.at[k],
            device_id={"data": mate}, device_id_type=mesh_id)

    def send_h(layer, half, dst, slot, pos):
        rows = pl.ds(pl.multiple_of(half * HALF, HALF), HALF)
        return pltpu.make_async_remote_copy(
            src_ref=hbuf.at[layer, rows], dst_ref=hin.at[slot, pos, rows],
            send_sem=hs_sem.at[layer, half], recv_sem=hr_sem.at[slot, pos, half],
            device_id={"data": dst}, device_id_type=mesh_id)

    def send_x(layer, dst, slot, pos):
        return pltpu.make_async_remote_copy(
            src_ref=xo.at[slot, pos], dst_ref=xbuf.at[layer + 1], send_sem=xs_sem.at[slot, pos], recv_sem=xr_sem.at[layer],
            device_id={"data": dst}, device_id_type=mesh_id)

    small = [pltpu.make_async_copy(src, dst, isem.at[k]) for k, (src, dst) in enumerate(
        ((hid_in, xbuf.at[0]), (ga_in, ga), (gf_in, gf), (lens_in, lens)))]
    for cp in small:
        cp.start()
    wcopy(0, 0).start()
    for c in range(3):
        for which in range(2):
            kcopy(c, which).start()

    barrier = pltpu.get_barrier_semaphore()
    for step in range(1, 4):
        pl.semaphore_signal(barrier, inc=1, device_id={"data": lax.rem(me + step, 4)}, device_id_type=mesh_id)
    for cp in small:
        cp.wait()

    pick = (lax.broadcasted_iota(jnp.int32, (ROWS * 8, ROWS), 0) // 8 == lax.broadcasted_iota(jnp.int32, (ROWS * 8, ROWS), 1))
    lrow = jnp.broadcast_to(lens[...].astype(F32), (HD, ROWS)).astype(BF16)
    len3[...] = 2.0 * lax.dot_general(pick.astype(F32).astype(BF16), lrow, NT, preferred_element_type=F32)
    zrow = jnp.zeros((ROWS, HD), F32)
    for j in (6, 7):
        for ref in (q3, k3, v3):
            ref[pl.ds(j, ROWS, stride=8), :] = zrow
    pl.semaphore_wait(barrier, 3)

    @pl.when(me == 1)
    def _():
        fsend(0, core).start()

    def is_local(layer):
        return (chip == layer // 2) & ((layer > 0) | (me == 0))

    def layer_step(layer, carry):
        wslot = lax.rem(jnp.int32(layer), 2)
        local = is_local(layer)
        dst = jnp.where(layer == 0, 0, peer)
        slot = jnp.where((layer == 0) & (me == 1), 0, 2 * wslot + 1)
        pos = jnp.where(layer == 0, core, 0)
        wcopy(layer, 0).wait()

        @pl.when((layer > 0) & jnp.logical_not(is_local(layer - 1)))
        def _():
            send_x(layer - 1, me, 0, 0).wait_recv()

        normed = rms(xbuf[layer], ga[pl.ds(layer, 1), :])
        qkv = jnp.dot(normed, qkvw[wslot], preferred_element_type=F32).astype(BF16).astype(F32)
        for j in range(HEADS):
            rows8 = pl.ds(j, ROWS, stride=8)
            kv = j * 2 // HEADS
            q3[rows8, :] = qkv[:, j * HD:(j + 1) * HD]
            k3[rows8, :] = qkv[:, (HEADS + kv) * HD:(HEADS + kv + 1) * HD]
            v3[rows8, :] = qkv[:, (HEADS + 2 + kv) * HD:(HEADS + 3 + kv) * HD]

        def refill(c, ok=True):
            @pl.when((c < LAYERS * CHUNKS) & ok)
            def _():
                for which in range(2):
                    kcopy(c, which).start()

        col8 = lax.broadcasted_iota(jnp.int32, (8, 2 * CACHE), 1)
        kv8 = jnp.where(lax.broadcasted_iota(jnp.int32, (8, 2 * CACHE), 0) < HEADS // 2, 0, 1)
        cols8 = jnp.where((col8 & 1) == kv8, col8.astype(F32), 4.0 * CACHE)[None]

        def chunk_math(part):
            cslot = lax.rem(layer * CHUNKS + part, SLOTS)
            rows = pl.ds(pl.multiple_of(part * (CHUNK * 8), CHUNK * 8), CHUNK * 8)
            qc = q3[rows, :]
            s_self = jnp.sum(qc * k3[rows, :], axis=-1, keepdims=True).reshape(CHUNK, 8, 1)
            zero = jnp.zeros((8, HD), F32)
            scores = []
            for i in range(CHUNK // 2):
                qa = qc[16 * i:16 * i + 8]
                qb = qc[16 * i + 8:16 * i + 16]
                lhs = jnp.concatenate([jnp.concatenate([qa, zero], 1), jnp.concatenate([zero, qb], 1)], 0).astype(BF16)
                keys = jnp.concatenate([kbuf[cslot, 2 * i], kbuf[cslot, 2 * i + 1]], 1)
                scores.append(lax.dot_general(lhs, keys, NT, preferred_element_type=F32))
            s = jnp.concatenate(scores, 0).reshape(CHUNK, 8, 2 * CACHE)
            lim = jnp.concatenate([len3[rows, :].reshape(CHUNK, 8, HD)] * (2 * CACHE // HD), 2)
            s = jnp.where(cols8 < lim, s, -1e30 * HD ** 0.5)
            top = jnp.maximum(jnp.max(s, axis=-1, keepdims=True), s_self)
            e = jnp.exp2((s - top) * EXP_SCALE)
            e_self = jnp.exp2((s_self - top) * EXP_SCALE)
            inv = 1.0 / (jnp.sum(e, axis=-1, keepdims=True) + e_self)
            p = (e * inv).reshape(CHUNK * 8, 2 * CACHE).astype(BF16)
            self_out = (e_self * inv).astype(BF16).astype(F32).reshape(CHUNK * 8, 1) * v3[rows, :]
            outs = []
            for i in range(CHUNK // 2):
                vals = jnp.concatenate([vbuf[cslot, 2 * i], vbuf[cslot, 2 * i + 1]], 1)
                o = jnp.dot(p[16 * i:16 * i + 16], vals, preferred_element_type=F32)
                outs += [o[0:8, 0:HD], o[8:16, HD:2 * HD]]
            o3[rows, :] = jnp.concatenate(outs, 0) + self_out

        def chunk_pair(part):
            for k in range(2):
                for which in range(2):
                    kcopy(layer * CHUNKS + part + k, which).wait()
            for k in range(2):
                chunk_math(part + k)

        def half_att(half, carry):
            @pl.when(half == 0)
            def _():
                @pl.when(layer == 0)
                def _():
                    for which in range(2):
                        kcopy(3, which).start()
                    wcopy(0, 1).start()

                @pl.when(jnp.where(me == 0, layer == 0, (chip == 1) & (layer == 1)))
                def _():
                    for k in range(3):
                        fcopy(k).start()

            @pl.when(half == 1)
            def _():
                @pl.when(layer == 0)
                def _():
                    for c in (4, 5):
                        for which in range(2):
                            kcopy(c, which).start()

                refill(layer * CHUNKS + 6)

            chunk_pair(half * (CHUNKS // 2))

            @pl.when(half == 0)
            def _():
                wcopy(layer, 1).wait()

            base = half * (HALF * 8)
            attn = jnp.concatenate([o3[pl.ds(base + j, HALF, stride=8), :] for j in range(HEADS)], 1).astype(BF16)
            proj = jnp.dot(attn, outw[wslot], preferred_element_type=F32)
            rows = pl.ds(pl.multiple_of(half * HALF, HALF), HALF)
            mid = (xbuf[layer, rows].astype(F32) + proj).astype(BF16)

            @pl.when(local)
            def _():
                hin[2 * wslot, 0, rows] = mid

            @pl.when(jnp.logical_not(local))
            def _():
                hbuf[layer, rows] = mid
                send_h(layer, half, dst, slot, pos).start()
            return carry

        lax.fori_loop(0, 2, half_att, 0)

        @pl.when(layer + 1 < LAYERS)
        def _():
            for which in range(2):
                wcopy(layer + 1, which).start()

        @pl.when((layer == 0) & (chip == 1))
        def _():
            fsend(0, core).start()

        @pl.when((layer == 0) & (me != 0))
        def _():
            fsend(1, core).start()

        @pl.when(jnp.where(chip == 0, (layer == 0) & (me == 1), layer == 1))
        def _():
            fsend(2, core).start()

        @pl.when((layer == 0) & (me == 1))
        def _():
            for k in range(3):
                fcopy(k).start()

        refill(layer * CHUNKS + 7)

        def ffn_step(turn, carry):
            serve0 = (layer == 2) | (turn == 1)
            serve1 = (layer != 2) & (turn == 0)
            serve = jnp.where(chip == 0, serve0, serve1)
            tl = jnp.where(chip == 0, jnp.where(layer == 2, 1, layer), jnp.where(layer == 1, 2, layer))
            todo0 = jnp.where(turn == 0, layer < 3, layer == 0) & ((layer > 0) | (me == 0))
            todo1 = jnp.where(turn == 0, layer > 0, layer == 3)
            todo = jnp.where(chip == 0, todo0, todo1)

            @pl.when(todo)
            def _():
                idx = lax.rem(tl, 2)
                fslot = 2 * idx + jnp.where(serve, 1, 0)
                both = tl == 0

                @pl.when(serve)
                def _():
                    for half in range(2):
                        send_h(0, half, me, fslot, 0).wait_recv()

                @pl.when(both)
                def _():
                    for half in range(2):
                        send_h(0, half, me, fslot, 1).wait_recv()

                first = jnp.where(serve, 1, 0) == chip

                @pl.when(first & (idx == core))
                def _():
                    for k in range(3):
                        fcopy(k).wait()

                @pl.when(first & (idx != core))
                def _():
                    for k in range(3):
                        fsend(k, idx).wait_recv()

                def ffn(count):
                    rows_h = hin[fslot, 0:count].reshape(count * ROWS, D)
                    n2 = rms(rows_h, gf[pl.ds(tl, 1), :])
                    zrows = slice(0, count * ROWS)
                    for b in range(FFN // FBLK):
                        cols = slice(b * FBLK, (b + 1) * FBLK)
                        a = jnp.dot(n2, fg[idx, :, cols], preferred_element_type=F32)
                        u = jnp.dot(n2, fu[idx, :, cols], preferred_element_type=F32)
                        zbuf[zrows, cols] = (a * jax.nn.sigmoid(a) * u).astype(BF16)
                    down = jnp.dot(zbuf[zrows, :], fd[idx], preferred_element_type=F32)
                    xo[fslot, 0:count] = (rows_h.astype(F32) + down).astype(BF16).reshape(count, ROWS, D)

                @pl.when(both)
                def _():
                    ffn(2)

                @pl.when(jnp.logical_not(both))
                def _():
                    ffn(1)

                @pl.when(serve)
                def _():
                    send_x(tl, peer, fslot, 0).start()

                @pl.when(jnp.logical_not(serve))
                def _():
                    xbuf[tl + 1] = xo[fslot, 0]

                @pl.when(both)
                def _():
                    send_x(tl, jnp.where(serve, 3, 1), fslot, 1).start()
            return carry

        refill(layer * CHUNKS + 8)
        lax.fori_loop(0, 2, ffn_step, 0)
        refill(layer * CHUNKS + 9)
        return carry

    lax.fori_loop(0, LAYERS, layer_step, 0)

    @pl.when(chip == 0)
    def _():
        send_x(LAYERS - 1, me, 0, 0).wait_recv()

    out[...] = xbuf[LAYERS]

    for layer in range(LAYERS):
        @pl.when(jnp.logical_not(is_local(layer)))
        def _():
            for half in range(2):
                send_h(layer, half, 0, 0, 0).wait_send()

    @pl.when(me != 0)
    def _():
        send_x(0, me, 3, 0).wait_send()
        for k in range(3):
            fsend(k, core).wait_send()

    @pl.when(chip == 1)
    def _():
        send_x(0, me, 1, 0).wait_send()

    @pl.when(me == 0)
    def _():
        for slot, pos in ((0, 1), (1, 0), (1, 1), (3, 0)):
            send_x(0, me, slot, pos).wait_send()


def solution(mesh):
    row_spec = P(('grp', 'data'), None)
    rep_spec = P()
    cache_spec = P(None, ('grp', 'data'))
    len_spec = P(('grp', 'data'))
    owned_spec = P('data')

    def per_device(hidden, w_qkv, w_out, norm_attn, norm_ffn, k_cache, v_cache, seq_lens, w_gate, w_up, w_down):
        kc = k_cache.reshape(LAYERS, ROWS, 2 * CACHE, HD)
        vc = v_cache.reshape(LAYERS, ROWS, 2 * CACHE, HD)
        vm = pl.BlockSpec(memory_space=pltpu.VMEM)
        anys = pl.BlockSpec(memory_space=pl.ANY)
        dma = pltpu.SemaphoreType.DMA
        return pl.pallas_call(
            kernel,
            out_shape=pltpu.VMEM((ROWS, D), BF16),
            in_specs=[anys] * 11,
            out_specs=vm,
            scratch_shapes=[
                pltpu.VMEM((SLOTS, CHUNK, 2 * CACHE, HD), BF16),
                pltpu.VMEM((SLOTS, CHUNK, 2 * CACHE, HD), BF16),
                pltpu.VMEM((2, D, QKV), BF16),
                pltpu.VMEM((2, D, D), BF16),
                pltpu.VMEM((2, D, FFN), BF16),
                pltpu.VMEM((2, D, FFN), BF16),
                pltpu.VMEM((2, FFN, D), BF16),
                pltpu.VMEM((ROWS * 8, HD), F32),
                pltpu.VMEM((ROWS * 8, HD), F32),
                pltpu.VMEM((ROWS * 8, HD), F32),
                pltpu.VMEM((ROWS * 8, HD), F32),
                pltpu.VMEM((ROWS * 8, HD), F32),
                pltpu.VMEM((LAYERS + 1, ROWS, D), BF16),
                pltpu.VMEM((LAYERS, ROWS, D), BF16),
                pltpu.VMEM((4, 2, ROWS, D), BF16),
                pltpu.VMEM((4, 2, ROWS, D), BF16),
                pltpu.VMEM((2 * ROWS, FFN), BF16),
                dma((SLOTS,)), dma((SLOTS,)), dma((2, 2)), dma((3,)), dma((3,)), dma((3,)),
                dma((LAYERS, 2)), dma((4, 2, 2)), dma((4, 2)), dma((LAYERS,)),
                pltpu.VMEM((LAYERS, D), F32), pltpu.VMEM((LAYERS, D), F32), pltpu.VMEM((1, ROWS), jnp.int32), dma((4,)),
            ],
            compiler_params=pltpu.CompilerParams(collective_id=0, has_side_effects=True, vmem_limit_bytes=64000000),
        )(hidden, norm_attn, norm_ffn, seq_lens.reshape(1, ROWS), w_qkv, w_out, kc, vc, w_gate, w_up, w_down)

    return jax.shard_map(per_device, mesh=mesh, in_specs=(row_spec, rep_spec, rep_spec, rep_spec, rep_spec, cache_spec, cache_spec, len_spec, owned_spec, owned_spec, owned_spec), out_specs=row_spec, check_vma=False)
```

```python
import jax
import jax.numpy as jnp
from jax import lax
from jax.experimental import pallas as pl
from jax.experimental.pallas import tpu as pltpu
from jax.sharding import PartitionSpec as P

NORM_EPS = 1e-5
EXP_SCALE = 1.4426950408889634 * 128 ** -0.5
F32 = jnp.float32
BF16 = jnp.bfloat16
LAYERS = 4
ROWS = 64
D = 768
HD = 128
HEADS = 6
CACHE = 256
QKV = 1280
FFN = 2048
CHUNK = 16
CHUNKS = ROWS // CHUNK
SLOTS = 6
HALF = ROWS // 2
FBLK = 512
NT = (((1,), (1,)), ((), ()))


def rms(rows_bf16, gain):
    vals = rows_bf16.astype(F32)
    inv = lax.rsqrt(jnp.mean(vals * vals, axis=-1, keepdims=True) + NORM_EPS)
    return (vals * inv * gain).astype(BF16)


def kernel(hid_in, ga_in, gf_in, lens_in, wqkv, wout, kc, vc, wg, wu, wd, out,
           kbuf, vbuf, qkvw, outw, fg, fu, fd, q3, k3, v3, o3, len3, xbuf, hbuf, hin, xo, zbuf,
           ksem, vsem, wsem, fsem, fs_sem, fr_sem, hs_sem, hr_sem, xs_sem, xr_sem, ga, gf, lens, isem):
    me = lax.axis_index("data")
    chip, core = lax.shift_right_logical(me, 1), lax.rem(me, 2)
    mate, peer = chip * 2 + (1 - core), lax.rem(me + 2, 4)
    mesh_id = pl.DeviceIdType.MESH

    def kcopy(c, which):
        layer, part, slot = lax.shift_right_logical(jnp.int32(c), 2), lax.rem(jnp.int32(c), CHUNKS), lax.rem(jnp.int32(c), SLOTS)
        src = pl.ds(pl.multiple_of(part * CHUNK, CHUNK), CHUNK)
        if which == 0:
            return pltpu.make_async_copy(kc.at[layer, src], kbuf.at[slot], ksem.at[slot])
        return pltpu.make_async_copy(vc.at[layer, src], vbuf.at[slot], vsem.at[slot])

    def wcopy(layer, which):
        slot = lax.rem(jnp.int32(layer), 2)
        if which == 0:
            return pltpu.make_async_copy(wqkv.at[layer], qkvw.at[slot], wsem.at[slot, 0])
        return pltpu.make_async_copy(wout.at[layer], outw.at[slot], wsem.at[slot, 1])

    ffn_parts = ((wg, fg), (wu, fu), (wd, fd))

    def fcopy(k):
        return pltpu.make_async_copy(ffn_parts[k][0].at[0], ffn_parts[k][1].at[core], fsem.at[k])

    def fsend(k, idx):
        return pltpu.make_async_remote_copy(
            src_ref=ffn_parts[k][0].at[0], dst_ref=ffn_parts[k][1].at[idx], send_sem=fs_sem.at[k], recv_sem=fr_sem.at[k],
            device_id={"data": mate}, device_id_type=mesh_id)

    def send_h(layer, half, dst, slot, pos):
        rows = pl.ds(pl.multiple_of(half * HALF, HALF), HALF)
        return pltpu.make_async_remote_copy(
            src_ref=hbuf.at[layer, rows], dst_ref=hin.at[slot, pos, rows],
            send_sem=hs_sem.at[layer, half], recv_sem=hr_sem.at[slot, pos, half],
            device_id={"data": dst}, device_id_type=mesh_id)

    def send_x(layer, dst, slot, pos, half):
        rows = pl.ds(pl.multiple_of(half * HALF, HALF), HALF)
        return pltpu.make_async_remote_copy(
            src_ref=xo.at[slot, pos, rows], dst_ref=xbuf.at[layer + 1, rows],
            send_sem=xs_sem.at[slot, pos, half], recv_sem=xr_sem.at[layer, half],
            device_id={"data": dst}, device_id_type=mesh_id)

    small = [pltpu.make_async_copy(src, dst, isem.at[k]) for k, (src, dst) in enumerate(
        ((hid_in, xbuf.at[0]), (ga_in, ga), (gf_in, gf), (lens_in, lens)))]
    for cp in small:
        cp.start()
    wcopy(0, 0).start()
    for c in range(3):
        for which in range(2):
            kcopy(c, which).start()

    barrier = pltpu.get_barrier_semaphore()
    for step in range(1, 4):
        pl.semaphore_signal(barrier, inc=1, device_id={"data": lax.rem(me + step, 4)}, device_id_type=mesh_id)
    for cp in small:
        cp.wait()

    pick = (lax.broadcasted_iota(jnp.int32, (ROWS * 8, ROWS), 0) // 8 == lax.broadcasted_iota(jnp.int32, (ROWS * 8, ROWS), 1))
    lrow = jnp.broadcast_to(lens[...].astype(F32), (HD, ROWS)).astype(BF16)
    len3[...] = 2.0 * lax.dot_general(pick.astype(F32).astype(BF16), lrow, NT, preferred_element_type=F32)
    zrow = jnp.zeros((ROWS, HD), F32)
    for j in (6, 7):
        for ref in (q3, k3, v3):
            ref[pl.ds(j, ROWS, stride=8), :] = zrow
    pl.semaphore_wait(barrier, 3)

    @pl.when(me == 1)
    def _():
        fsend(0, core).start()

    def is_local(layer):
        return (chip == layer // 2) & ((layer > 0) | (me == 0))

    def layer_step(layer, carry):
        wslot = lax.rem(jnp.int32(layer), 2)
        local = is_local(layer)
        dst = jnp.where(layer == 0, 0, peer)
        slot = jnp.where((layer == 0) & (me == 1), 0, 2 * wslot + 1)
        pos = jnp.where(layer == 0, core, 0)
        wcopy(layer, 0).wait()
        fetched = (layer > 0) & jnp.logical_not(is_local(layer - 1))

        def project(half):
            @pl.when(fetched)
            def _():
                send_x(layer - 1, me, 0, 0, half).wait_recv()

            normed = rms(xbuf[layer, pl.ds(pl.multiple_of(half * HALF, HALF), HALF)], ga[pl.ds(layer, 1), :])
            qkv = jnp.dot(normed, qkvw[wslot], preferred_element_type=F32).astype(BF16).astype(F32)
            for j in range(HEADS):
                rows8 = pl.ds(half * (HALF * 8) + j, HALF, stride=8)
                kv = j * 2 // HEADS
                q3[rows8, :] = qkv[:, j * HD:(j + 1) * HD]
                k3[rows8, :] = qkv[:, (HEADS + kv) * HD:(HEADS + kv + 1) * HD]
                v3[rows8, :] = qkv[:, (HEADS + 2 + kv) * HD:(HEADS + 3 + kv) * HD]

        def refill(c, ok=True):
            @pl.when((c < LAYERS * CHUNKS) & ok)
            def _():
                for which in range(2):
                    kcopy(c, which).start()

        col8 = lax.broadcasted_iota(jnp.int32, (8, 2 * CACHE), 1)
        kv8 = jnp.where(lax.broadcasted_iota(jnp.int32, (8, 2 * CACHE), 0) < HEADS // 2, 0, 1)
        cols8 = jnp.where((col8 & 1) == kv8, col8.astype(F32), 4.0 * CACHE)[None]

        def chunk_math(part):
            cslot = lax.rem(layer * CHUNKS + part, SLOTS)
            rows = pl.ds(pl.multiple_of(part * (CHUNK * 8), CHUNK * 8), CHUNK * 8)
            qc = q3[rows, :]
            s_self = jnp.sum(qc * k3[rows, :], axis=-1, keepdims=True).reshape(CHUNK, 8, 1)
            zero = jnp.zeros((8, HD), F32)
            scores = []
            for i in range(CHUNK // 2):
                qa = qc[16 * i:16 * i + 8]
                qb = qc[16 * i + 8:16 * i + 16]
                lhs = jnp.concatenate([jnp.concatenate([qa, zero], 1), jnp.concatenate([zero, qb], 1)], 0).astype(BF16)
                keys = jnp.concatenate([kbuf[cslot, 2 * i], kbuf[cslot, 2 * i + 1]], 1)
                scores.append(lax.dot_general(lhs, keys, NT, preferred_element_type=F32))
            s = jnp.concatenate(scores, 0).reshape(CHUNK, 8, 2 * CACHE)
            lim = jnp.concatenate([len3[rows, :].reshape(CHUNK, 8, HD)] * (2 * CACHE // HD), 2)
            s = jnp.where(cols8 < lim, s, -1e30 * HD ** 0.5)
            top = jnp.maximum(jnp.max(s, axis=-1, keepdims=True), s_self)
            e = jnp.exp2((s - top) * EXP_SCALE)
            e_self = jnp.exp2((s_self - top) * EXP_SCALE)
            inv = 1.0 / (jnp.sum(e, axis=-1, keepdims=True) + e_self)
            p = (e * inv).reshape(CHUNK * 8, 2 * CACHE).astype(BF16)
            self_out = (e_self * inv).astype(BF16).astype(F32).reshape(CHUNK * 8, 1) * v3[rows, :]
            outs = []
            for i in range(CHUNK // 2):
                vals = jnp.concatenate([vbuf[cslot, 2 * i], vbuf[cslot, 2 * i + 1]], 1)
                o = jnp.dot(p[16 * i:16 * i + 16], vals, preferred_element_type=F32)
                outs += [o[0:8, 0:HD], o[8:16, HD:2 * HD]]
            o3[rows, :] = jnp.concatenate(outs, 0) + self_out

        def chunk_pair(part):
            for k in range(2):
                for which in range(2):
                    kcopy(layer * CHUNKS + part + k, which).wait()
            for k in range(2):
                chunk_math(part + k)

        def wait_weights(idx):
            @pl.when(idx == core)
            def _():
                for k in range(3):
                    fcopy(k).wait()

            @pl.when(idx != core)
            def _():
                for k in range(3):
                    fsend(k, idx).wait_recv()

        def ffn(rows_h, tl, idx):
            n2 = rms(rows_h, gf[pl.ds(tl, 1), :])
            zrows = slice(0, rows_h.shape[0])
            for b in range(FFN // FBLK):
                cols = slice(b * FBLK, (b + 1) * FBLK)
                a = jnp.dot(n2, fg[idx, :, cols], preferred_element_type=F32)
                u = jnp.dot(n2, fu[idx, :, cols], preferred_element_type=F32)
                zbuf[zrows, cols] = (a * jax.nn.sigmoid(a) * u).astype(BF16)
            down = jnp.dot(zbuf[zrows, :], fd[idx], preferred_element_type=F32)
            return (rows_h.astype(F32) + down).astype(BF16)

        def half_att(half, carry):
            @pl.when(half == 0)
            def _():
                @pl.when(layer == 0)
                def _():
                    for which in range(2):
                        kcopy(3, which).start()
                    wcopy(0, 1).start()

                @pl.when(jnp.where(me == 0, layer == 0, (chip == 1) & (layer == 1)))
                def _():
                    for k in range(3):
                        fcopy(k).start()

            @pl.when(half == 1)
            def _():
                @pl.when(layer == 0)
                def _():
                    for c in (4, 5):
                        for which in range(2):
                            kcopy(c, which).start()

                refill(layer * CHUNKS + 6)

            project(half)
            chunk_pair(half * (CHUNKS // 2))

            @pl.when(half == 0)
            def _():
                wcopy(layer, 1).wait()

            base = half * (HALF * 8)
            attn = jnp.concatenate([o3[pl.ds(base + j, HALF, stride=8), :] for j in range(HEADS)], 1).astype(BF16)
            proj = jnp.dot(attn, outw[wslot], preferred_element_type=F32)
            rows = pl.ds(pl.multiple_of(half * HALF, HALF), HALF)
            mid = (xbuf[layer, rows].astype(F32) + proj).astype(BF16)

            @pl.when(local)
            def _():
                hin[2 * wslot, 0, rows] = mid

            @pl.when(jnp.logical_not(local))
            def _():
                hbuf[layer, rows] = mid
                send_h(layer, half, dst, slot, pos).start()

            @pl.when(jnp.where(chip == 0, layer == 2, (layer + half == 2) & (layer > 0)))
            def _():
                tl = jnp.where(chip == 0, 1, 2)
                th = jnp.where(chip == 0, half, 1 - half)
                idx = 1 - chip
                fslot = 2 * idx + 1
                send_h(0, th, me, fslot, 0).wait_recv()

                @pl.when((chip == 1) & (th == 0))
                def _():
                    wait_weights(idx)

                rows = pl.ds(pl.multiple_of(th * HALF, HALF), HALF)
                xo[fslot, 0, rows] = ffn(hin[fslot, 0, rows], tl, idx)
                send_x(tl, peer, fslot, 0, th).start()
            return carry

        lax.fori_loop(0, 2, half_att, 0)

        @pl.when(layer + 1 < LAYERS)
        def _():
            for which in range(2):
                wcopy(layer + 1, which).start()

        @pl.when((layer == 0) & (chip == 1))
        def _():
            fsend(0, core).start()

        @pl.when((layer == 0) & (me != 0))
        def _():
            fsend(1, core).start()

        @pl.when(jnp.where(chip == 0, (layer == 0) & (me == 1), layer == 1))
        def _():
            fsend(2, core).start()

        @pl.when((layer == 0) & (me == 1))
        def _():
            for k in range(3):
                fcopy(k).start()

        refill(layer * CHUNKS + 7)

        def ffn_step(turn, carry):
            serve = jnp.where(chip == 0, turn == 1, (layer == 3) & (turn == 0))
            todo0 = jnp.where(turn == 0, layer < 2, layer == 0) & ((layer > 0) | (me == 0))
            todo1 = jnp.where(turn == 0, layer > 1, layer == 3)

            @pl.when(jnp.where(chip == 0, todo0, todo1))
            def _():
                idx = wslot
                fslot = 2 * idx + jnp.where(serve, 1, 0)
                both = layer == 0

                @pl.when(serve)
                def _():
                    for half in range(2):
                        send_h(0, half, me, fslot, 0).wait_recv()

                @pl.when(both)
                def _():
                    for half in range(2):
                        send_h(0, half, me, fslot, 1).wait_recv()

                @pl.when(jnp.where(chip == 0, turn == 0, serve))
                def _():
                    wait_weights(idx)

                @pl.when(both)
                def _():
                    xo[fslot] = ffn(hin[fslot].reshape(2 * ROWS, D), layer, idx).reshape(2, ROWS, D)

                @pl.when(jnp.logical_not(both))
                def _():
                    xo[fslot, 0] = ffn(hin[fslot, 0], layer, idx)

                @pl.when(serve)
                def _():
                    for half in range(2):
                        send_x(layer, peer, fslot, 0, half).start()

                @pl.when(jnp.logical_not(serve))
                def _():
                    xbuf[layer + 1] = xo[fslot, 0]

                @pl.when(both)
                def _():
                    for half in range(2):
                        send_x(layer, jnp.where(serve, 3, 1), fslot, 1, half).start()
            return carry

        refill(layer * CHUNKS + 8)
        lax.fori_loop(0, 2, ffn_step, 0)
        refill(layer * CHUNKS + 9)
        return carry

    lax.fori_loop(0, LAYERS, layer_step, 0)

    @pl.when(chip == 0)
    def _():
        for half in range(2):
            send_x(LAYERS - 1, me, 0, 0, half).wait_recv()

    out[...] = xbuf[LAYERS]

    for half in range(2):
        for layer in range(LAYERS):
            @pl.when(jnp.logical_not(is_local(layer)))
            def _():
                send_h(layer, half, 0, 0, 0).wait_send()

        @pl.when(me != 0)
        def _():
            send_x(0, me, 3, 0, half).wait_send()

        @pl.when(chip == 1)
        def _():
            send_x(0, me, 1, 0, half).wait_send()

        @pl.when(me == 0)
        def _():
            for slot, pos in ((0, 1), (1, 0), (1, 1), (3, 0)):
                send_x(0, me, slot, pos, half).wait_send()

    @pl.when(me != 0)
    def _():
        for k in range(3):
            fsend(k, core).wait_send()


def solution(mesh):
    row_spec = P(('grp', 'data'), None)
    rep_spec = P()
    cache_spec = P(None, ('grp', 'data'))
    len_spec = P(('grp', 'data'))
    owned_spec = P('data')

    def per_device(hidden, w_qkv, w_out, norm_attn, norm_ffn, k_cache, v_cache, seq_lens, w_gate, w_up, w_down):
        kc = k_cache.reshape(LAYERS, ROWS, 2 * CACHE, HD)
        vc = v_cache.reshape(LAYERS, ROWS, 2 * CACHE, HD)
        vm = pl.BlockSpec(memory_space=pltpu.VMEM)
        anys = pl.BlockSpec(memory_space=pl.ANY)
        dma = pltpu.SemaphoreType.DMA
        return pl.pallas_call(
            kernel,
            out_shape=pltpu.VMEM((ROWS, D), BF16),
            in_specs=[anys] * 11,
            out_specs=vm,
            scratch_shapes=[
                pltpu.VMEM((SLOTS, CHUNK, 2 * CACHE, HD), BF16),
                pltpu.VMEM((SLOTS, CHUNK, 2 * CACHE, HD), BF16),
                pltpu.VMEM((2, D, QKV), BF16),
                pltpu.VMEM((2, D, D), BF16),
                pltpu.VMEM((2, D, FFN), BF16),
                pltpu.VMEM((2, D, FFN), BF16),
                pltpu.VMEM((2, FFN, D), BF16),
                pltpu.VMEM((ROWS * 8, HD), F32),
                pltpu.VMEM((ROWS * 8, HD), F32),
                pltpu.VMEM((ROWS * 8, HD), F32),
                pltpu.VMEM((ROWS * 8, HD), F32),
                pltpu.VMEM((ROWS * 8, HD), F32),
                pltpu.VMEM((LAYERS + 1, ROWS, D), BF16),
                pltpu.VMEM((LAYERS, ROWS, D), BF16),
                pltpu.VMEM((4, 2, ROWS, D), BF16),
                pltpu.VMEM((4, 2, ROWS, D), BF16),
                pltpu.VMEM((2 * ROWS, FFN), BF16),
                dma((SLOTS,)), dma((SLOTS,)), dma((2, 2)), dma((3,)), dma((3,)), dma((3,)),
                dma((LAYERS, 2)), dma((4, 2, 2)), dma((4, 2, 2)), dma((LAYERS, 2)),
                pltpu.VMEM((LAYERS, D), F32), pltpu.VMEM((LAYERS, D), F32), pltpu.VMEM((1, ROWS), jnp.int32), dma((4,)),
            ],
            compiler_params=pltpu.CompilerParams(collective_id=0, has_side_effects=True, vmem_limit_bytes=64000000),
        )(hidden, norm_attn, norm_ffn, seq_lens.reshape(1, ROWS), w_qkv, w_out, kc, vc, w_gate, w_up, w_down)

    return jax.shard_map(per_device, mesh=mesh, in_specs=(row_spec, rep_spec, rep_spec, rep_spec, rep_spec, cache_spec, cache_spec, len_spec, owned_spec, owned_spec, owned_spec), out_specs=row_spec, check_vma=False)
```

```python
import jax
import jax.numpy as jnp
from jax import lax
from jax.experimental import pallas as pl
from jax.experimental.pallas import tpu as pltpu
from jax.sharding import PartitionSpec as P

NORM_EPS = 1e-5
EXP_SCALE = 1.4426950408889634 * 128 ** -0.5
F32 = jnp.float32
BF16 = jnp.bfloat16
LAYERS = 4
ROWS = 64
D = 768
HD = 128
HEADS = 6
CACHE = 256
QKV = 1280
FFN = 2048
CHUNK = 16
CHUNKS = ROWS // CHUNK
SLOTS = 6
HALF = ROWS // 2
FBLK = 512
NT = (((1,), (1,)), ((), ()))


def rms(rows_bf16, gain):
    vals = rows_bf16.astype(F32)
    inv = lax.rsqrt(jnp.mean(vals * vals, axis=-1, keepdims=True) + NORM_EPS)
    return (vals * inv * gain).astype(BF16)


def kernel(hid_in, ga_in, gf_in, lens_in, wqkv, wout, kc, vc, wg, wu, wd, out,
           kbuf, vbuf, qkvw, outw, fg, fu, fd, q3, k3, v3, o3, len3, xbuf, hbuf, hin, xo, zbuf,
           ksem, vsem, wsem, fsem, fs_sem, fr_sem, hs_sem, hr_sem, xs_sem, xr_sem, ga, gf, lens, isem):
    me = lax.axis_index("data")
    chip, core = lax.shift_right_logical(me, 1), lax.rem(me, 2)
    mate, peer = chip * 2 + (1 - core), lax.rem(me + 2, 4)
    mesh_id = pl.DeviceIdType.MESH

    def kcopy(c, which):
        layer, part, slot = lax.shift_right_logical(jnp.int32(c), 2), lax.rem(jnp.int32(c), CHUNKS), lax.rem(jnp.int32(c), SLOTS)
        src = pl.ds(pl.multiple_of(part * CHUNK, CHUNK), CHUNK)
        if which == 0:
            return pltpu.make_async_copy(kc.at[layer, src], kbuf.at[slot], ksem.at[slot])
        return pltpu.make_async_copy(vc.at[layer, src], vbuf.at[slot], vsem.at[slot])

    def wcopy(layer, which):
        slot = lax.rem(jnp.int32(layer), 2)
        if which == 0:
            return pltpu.make_async_copy(wqkv.at[layer], qkvw.at[slot], wsem.at[slot, 0])
        return pltpu.make_async_copy(wout.at[layer], outw.at[slot], wsem.at[slot, 1])

    ffn_parts = ((wg, fg), (wu, fu), (wd, fd))

    def fcopy(k):
        return pltpu.make_async_copy(ffn_parts[k][0].at[0], ffn_parts[k][1].at[core], fsem.at[k])

    def fsend(k, idx):
        return pltpu.make_async_remote_copy(
            src_ref=ffn_parts[k][0].at[0], dst_ref=ffn_parts[k][1].at[idx], send_sem=fs_sem.at[k], recv_sem=fr_sem.at[k],
            device_id={"data": mate}, device_id_type=mesh_id)

    def send_h(layer, half, dst, slot, pos):
        rows = pl.ds(pl.multiple_of(half * HALF, HALF), HALF)
        return pltpu.make_async_remote_copy(
            src_ref=hbuf.at[layer, rows], dst_ref=hin.at[slot, pos, rows],
            send_sem=hs_sem.at[layer, half], recv_sem=hr_sem.at[slot, pos, half],
            device_id={"data": dst}, device_id_type=mesh_id)

    def send_x(layer, dst, slot, pos, half):
        rows = pl.ds(pl.multiple_of(half * HALF, HALF), HALF)
        return pltpu.make_async_remote_copy(
            src_ref=xo.at[slot, pos, rows], dst_ref=xbuf.at[layer + 1, rows],
            send_sem=xs_sem.at[slot, pos, half], recv_sem=xr_sem.at[layer, half],
            device_id={"data": dst}, device_id_type=mesh_id)

    small = [pltpu.make_async_copy(src, dst, isem.at[k]) for k, (src, dst) in enumerate(
        ((hid_in, xbuf.at[0]), (ga_in, ga), (gf_in, gf), (lens_in, lens)))]
    for cp in small:
        cp.start()
    wcopy(0, 0).start()
    for c in range(3):
        for which in range(2):
            kcopy(c, which).start()

    barrier = pltpu.get_barrier_semaphore()
    for step in range(1, 4):
        pl.semaphore_signal(barrier, inc=1, device_id={"data": lax.rem(me + step, 4)}, device_id_type=mesh_id)
    for cp in small:
        cp.wait()

    pick = (lax.broadcasted_iota(jnp.int32, (ROWS * 8, ROWS), 0) // 8 == lax.broadcasted_iota(jnp.int32, (ROWS * 8, ROWS), 1))
    lrow = jnp.broadcast_to(lens[...].astype(F32), (HD, ROWS)).astype(BF16)
    len3[...] = 2.0 * lax.dot_general(pick.astype(F32).astype(BF16), lrow, NT, preferred_element_type=F32)
    zrow = jnp.zeros((ROWS, HD), F32)
    for j in (6, 7):
        for ref in (q3, k3, v3):
            ref[pl.ds(j, ROWS, stride=8), :] = zrow
    pl.semaphore_wait(barrier, 3)

    @pl.when(me == 1)
    def _():
        fsend(0, core).start()

    def is_local(layer):
        return (chip == layer // 2) & ((layer > 0) | (me == 0))

    def layer_step(layer, carry):
        wslot = lax.rem(jnp.int32(layer), 2)
        local = is_local(layer)
        dst = jnp.where(layer == 0, 0, peer)
        slot = jnp.where((layer == 0) & (me == 1), 0, 2 * wslot + 1)
        pos = jnp.where(layer == 0, core, 0)
        wcopy(layer, 0).wait()
        fetched = (layer > 0) & jnp.logical_not(is_local(layer - 1))

        def project(half):
            @pl.when(fetched)
            def _():
                send_x(layer - 1, me, 0, 0, half).wait_recv()

            normed = rms(xbuf[layer, pl.ds(pl.multiple_of(half * HALF, HALF), HALF)], ga[pl.ds(layer, 1), :])
            qkv = jnp.dot(normed, qkvw[wslot], preferred_element_type=F32).astype(BF16).astype(F32)
            for j in range(HEADS):
                rows8 = pl.ds(half * (HALF * 8) + j, HALF, stride=8)
                kv = j * 2 // HEADS
                q3[rows8, :] = qkv[:, j * HD:(j + 1) * HD]
                k3[rows8, :] = qkv[:, (HEADS + kv) * HD:(HEADS + kv + 1) * HD]
                v3[rows8, :] = qkv[:, (HEADS + 2 + kv) * HD:(HEADS + 3 + kv) * HD]

        def refill(c, ok=True):
            @pl.when((c < LAYERS * CHUNKS) & ok)
            def _():
                for which in range(2):
                    kcopy(c, which).start()

        col8 = lax.broadcasted_iota(jnp.int32, (8, 2 * CACHE), 1)
        kv8 = jnp.where(lax.broadcasted_iota(jnp.int32, (8, 2 * CACHE), 0) < HEADS // 2, 0, 1)
        cols8 = jnp.where((col8 & 1) == kv8, col8.astype(F32), 4.0 * CACHE)[None]

        def chunk_math(part):
            cslot = lax.rem(layer * CHUNKS + part, SLOTS)
            rows = pl.ds(pl.multiple_of(part * (CHUNK * 8), CHUNK * 8), CHUNK * 8)
            qc = q3[rows, :]
            s_self = jnp.sum(qc * k3[rows, :], axis=-1, keepdims=True).reshape(CHUNK, 8, 1)
            zero = jnp.zeros((8, HD), F32)
            scores = []
            for i in range(CHUNK // 2):
                qa = qc[16 * i:16 * i + 8]
                qb = qc[16 * i + 8:16 * i + 16]
                lhs = jnp.concatenate([jnp.concatenate([qa, zero], 1), jnp.concatenate([zero, qb], 1)], 0).astype(BF16)
                keys = jnp.concatenate([kbuf[cslot, 2 * i], kbuf[cslot, 2 * i + 1]], 1)
                scores.append(lax.dot_general(lhs, keys, NT, preferred_element_type=F32))
            s = jnp.concatenate(scores, 0).reshape(CHUNK, 8, 2 * CACHE)
            lim = jnp.concatenate([len3[rows, :].reshape(CHUNK, 8, HD)] * (2 * CACHE // HD), 2)
            s = jnp.where(cols8 < lim, s, -1e30 * HD ** 0.5)
            top = jnp.maximum(jnp.max(s, axis=-1, keepdims=True), s_self)
            e = jnp.exp2((s - top) * EXP_SCALE)
            e_self = jnp.exp2((s_self - top) * EXP_SCALE)
            inv = 1.0 / (jnp.sum(e, axis=-1, keepdims=True) + e_self)
            p = (e * inv).reshape(CHUNK * 8, 2 * CACHE).astype(BF16)
            self_out = (e_self * inv).astype(BF16).astype(F32).reshape(CHUNK * 8, 1) * v3[rows, :]
            outs = []
            for i in range(CHUNK // 2):
                vals = jnp.concatenate([vbuf[cslot, 2 * i], vbuf[cslot, 2 * i + 1]], 1)
                o = jnp.dot(p[16 * i:16 * i + 16], vals, preferred_element_type=F32)
                outs += [o[0:8, 0:HD], o[8:16, HD:2 * HD]]
            o3[rows, :] = jnp.concatenate(outs, 0) + self_out

        def chunk_pair(part):
            for k in range(2):
                for which in range(2):
                    kcopy(layer * CHUNKS + part + k, which).wait()
            for k in range(2):
                chunk_math(part + k)

        def wait_weights(idx):
            @pl.when(idx == core)
            def _():
                for k in range(3):
                    fcopy(k).wait()

            @pl.when(idx != core)
            def _():
                for k in range(3):
                    fsend(k, idx).wait_recv()

        def ffn(rows_h, tl, idx):
            n2 = rms(rows_h, gf[pl.ds(tl, 1), :])
            zrows = slice(0, rows_h.shape[0])
            for b in range(FFN // FBLK):
                cols = slice(b * FBLK, (b + 1) * FBLK)
                a = jnp.dot(n2, fg[idx, :, cols], preferred_element_type=F32)
                u = jnp.dot(n2, fu[idx, :, cols], preferred_element_type=F32)
                zbuf[zrows, cols] = (a * jax.nn.sigmoid(a) * u).astype(BF16)
            down = jnp.dot(zbuf[zrows, :], fd[idx], preferred_element_type=F32)
            return (rows_h.astype(F32) + down).astype(BF16)

        def half_att(half, carry):
            @pl.when(half == 0)
            def _():
                @pl.when(layer == 0)
                def _():
                    for which in range(2):
                        kcopy(3, which).start()
                    wcopy(0, 1).start()

                @pl.when(jnp.where(me == 0, layer == 0, (chip == 1) & (layer == 1)))
                def _():
                    for k in range(3):
                        fcopy(k).start()

            @pl.when(half == 1)
            def _():
                @pl.when(layer == 0)
                def _():
                    for c in (4, 5):
                        for which in range(2):
                            kcopy(c, which).start()

                refill(layer * CHUNKS + 6)

            project(half)
            chunk_pair(half * (CHUNKS // 2))

            @pl.when(half == 0)
            def _():
                wcopy(layer, 1).wait()

            base = half * (HALF * 8)
            attn = jnp.concatenate([o3[pl.ds(base + j, HALF, stride=8), :] for j in range(HEADS)], 1).astype(BF16)
            proj = jnp.dot(attn, outw[wslot], preferred_element_type=F32)
            rows = pl.ds(pl.multiple_of(half * HALF, HALF), HALF)
            mid = (xbuf[layer, rows].astype(F32) + proj).astype(BF16)

            @pl.when(local)
            def _():
                hin[2 * wslot, 0, rows] = mid

            @pl.when(jnp.logical_not(local))
            def _():
                hbuf[layer, rows] = mid
                send_h(layer, half, dst, slot, pos).start()

            @pl.when(half == 1)
            def _():
                @pl.when(layer + 1 < LAYERS)
                def _():
                    for which in range(2):
                        wcopy(layer + 1, which).start()

                @pl.when((layer == 0) & (chip == 1))
                def _():
                    fsend(0, core).start()

                @pl.when((layer == 0) & (me != 0))
                def _():
                    fsend(1, core).start()

                @pl.when(jnp.where(chip == 0, (layer == 0) & (me == 1), layer == 1))
                def _():
                    fsend(2, core).start()

                @pl.when((layer == 0) & (me == 1))
                def _():
                    for k in range(3):
                        fcopy(k).start()

                refill(layer * CHUNKS + 7)
                refill(layer * CHUNKS + 8)

            @pl.when(jnp.where(chip == 0, layer == 2, (layer + half == 2) & (layer > 0)))
            def _():
                tl = jnp.where(chip == 0, 1, 2)
                th = jnp.where(chip == 0, half, 1 - half)
                idx = 1 - chip
                fslot = 2 * idx + 1
                send_h(0, th, me, fslot, 0).wait_recv()

                @pl.when((chip == 1) & (th == 0))
                def _():
                    wait_weights(idx)

                rows = pl.ds(pl.multiple_of(th * HALF, HALF), HALF)
                xo[fslot, 0, rows] = ffn(hin[fslot, 0, rows], tl, idx)
                send_x(tl, peer, fslot, 0, th).start()
            return carry

        lax.fori_loop(0, 2, half_att, 0)

        def ffn_step(turn, carry):
            serve = jnp.where(chip == 0, turn == 1, (layer == 3) & (turn == 0))
            todo0 = jnp.where(turn == 0, layer < 2, layer == 0) & ((layer > 0) | (me == 0))
            todo1 = jnp.where(turn == 0, layer > 1, layer == 3)

            @pl.when(jnp.where(chip == 0, todo0, todo1))
            def _():
                idx = wslot
                fslot = 2 * idx + jnp.where(serve, 1, 0)
                both = layer == 0

                @pl.when(serve)
                def _():
                    for half in range(2):
                        send_h(0, half, me, fslot, 0).wait_recv()

                @pl.when(both)
                def _():
                    for half in range(2):
                        send_h(0, half, me, fslot, 1).wait_recv()

                @pl.when(jnp.where(chip == 0, turn == 0, serve))
                def _():
                    wait_weights(idx)

                @pl.when(both)
                def _():
                    xo[fslot] = ffn(hin[fslot].reshape(2 * ROWS, D), layer, idx).reshape(2, ROWS, D)

                @pl.when(jnp.logical_not(both))
                def _():
                    xo[fslot, 0] = ffn(hin[fslot, 0], layer, idx)

                @pl.when(serve)
                def _():
                    for half in range(2):
                        send_x(layer, peer, fslot, 0, half).start()

                @pl.when(jnp.logical_not(serve))
                def _():
                    xbuf[layer + 1] = xo[fslot, 0]

                @pl.when(both)
                def _():
                    for half in range(2):
                        send_x(layer, jnp.where(serve, 3, 1), fslot, 1, half).start()
            return carry

        lax.fori_loop(0, 2, ffn_step, 0)
        refill(layer * CHUNKS + 9)
        return carry

    lax.fori_loop(0, LAYERS, layer_step, 0)

    @pl.when(chip == 0)
    def _():
        for half in range(2):
            send_x(LAYERS - 1, me, 0, 0, half).wait_recv()

    out[...] = xbuf[LAYERS]

    for half in range(2):
        for layer in range(LAYERS):
            @pl.when(jnp.logical_not(is_local(layer)))
            def _():
                send_h(layer, half, 0, 0, 0).wait_send()

        @pl.when(me != 0)
        def _():
            send_x(0, me, 3, 0, half).wait_send()

        @pl.when(chip == 1)
        def _():
            send_x(0, me, 1, 0, half).wait_send()

        @pl.when(me == 0)
        def _():
            for slot, pos in ((0, 1), (1, 0), (1, 1), (3, 0)):
                send_x(0, me, slot, pos, half).wait_send()

    @pl.when(me != 0)
    def _():
        for k in range(3):
            fsend(k, core).wait_send()


def solution(mesh):
    row_spec = P(('grp', 'data'), None)
    rep_spec = P()
    cache_spec = P(None, ('grp', 'data'))
    len_spec = P(('grp', 'data'))
    owned_spec = P('data')

    def per_device(hidden, w_qkv, w_out, norm_attn, norm_ffn, k_cache, v_cache, seq_lens, w_gate, w_up, w_down):
        kc = k_cache.reshape(LAYERS, ROWS, 2 * CACHE, HD)
        vc = v_cache.reshape(LAYERS, ROWS, 2 * CACHE, HD)
        vm = pl.BlockSpec(memory_space=pltpu.VMEM)
        anys = pl.BlockSpec(memory_space=pl.ANY)
        dma = pltpu.SemaphoreType.DMA
        return pl.pallas_call(
            kernel,
            out_shape=pltpu.VMEM((ROWS, D), BF16),
            in_specs=[anys] * 11,
            out_specs=vm,
            scratch_shapes=[
                pltpu.VMEM((SLOTS, CHUNK, 2 * CACHE, HD), BF16),
                pltpu.VMEM((SLOTS, CHUNK, 2 * CACHE, HD), BF16),
                pltpu.VMEM((2, D, QKV), BF16),
                pltpu.VMEM((2, D, D), BF16),
                pltpu.VMEM((2, D, FFN), BF16),
                pltpu.VMEM((2, D, FFN), BF16),
                pltpu.VMEM((2, FFN, D), BF16),
                pltpu.VMEM((ROWS * 8, HD), F32),
                pltpu.VMEM((ROWS * 8, HD), F32),
                pltpu.VMEM((ROWS * 8, HD), F32),
                pltpu.VMEM((ROWS * 8, HD), F32),
                pltpu.VMEM((ROWS * 8, HD), F32),
                pltpu.VMEM((LAYERS + 1, ROWS, D), BF16),
                pltpu.VMEM((LAYERS, ROWS, D), BF16),
                pltpu.VMEM((4, 2, ROWS, D), BF16),
                pltpu.VMEM((4, 2, ROWS, D), BF16),
                pltpu.VMEM((2 * ROWS, FFN), BF16),
                dma((SLOTS,)), dma((SLOTS,)), dma((2, 2)), dma((3,)), dma((3,)), dma((3,)),
                dma((LAYERS, 2)), dma((4, 2, 2)), dma((4, 2, 2)), dma((LAYERS, 2)),
                pltpu.VMEM((LAYERS, D), F32), pltpu.VMEM((LAYERS, D), F32), pltpu.VMEM((1, ROWS), jnp.int32), dma((4,)),
            ],
            compiler_params=pltpu.CompilerParams(collective_id=0, has_side_effects=True, vmem_limit_bytes=64000000),
        )(hidden, norm_attn, norm_ffn, seq_lens.reshape(1, ROWS), w_qkv, w_out, kc, vc, w_gate, w_up, w_down)

    return jax.shard_map(per_device, mesh=mesh, in_specs=(row_spec, rep_spec, rep_spec, rep_spec, rep_spec, cache_spec, cache_spec, len_spec, owned_spec, owned_spec, owned_spec), out_specs=row_spec, check_vma=False)
```

```python
import jax
import jax.numpy as jnp
from jax import lax
from jax.experimental import pallas as pl
from jax.experimental.pallas import tpu as pltpu
from jax.sharding import PartitionSpec as P

NORM_EPS = 1e-5
EXP_SCALE = 1.4426950408889634 * 128 ** -0.5
F32 = jnp.float32
BF16 = jnp.bfloat16
LAYERS = 4
ROWS = 64
D = 768
HD = 128
HEADS = 6
CACHE = 256
QKV = 1280
FFN = 2048
CHUNK = 16
CHUNKS = ROWS // CHUNK
SLOTS = 6
HALF = ROWS // 2
FBLK = 512
NT = (((1,), (1,)), ((), ()))


def rms(rows_bf16, gain):
    vals = rows_bf16.astype(F32)
    inv = lax.rsqrt(jnp.mean(vals * vals, axis=-1, keepdims=True) + NORM_EPS)
    return (vals * inv * gain).astype(BF16)


def kernel(hid_in, ga_in, gf_in, lens_in, wqkv, wout, kc, vc, wg, wu, wd, out,
           kbuf, vbuf, qkvw, outw, fg, fu, fd, q3, k3, v3, o3, len3, xbuf, hbuf, hin, xo, zbuf,
           ksem, vsem, wsem, fsem, fs_sem, fr_sem, hs_sem, hr_sem, xs_sem, xr_sem, ga, gf, lens, isem):
    me = lax.axis_index("data")
    chip, core = lax.shift_right_logical(me, 1), lax.rem(me, 2)
    mate, peer = chip * 2 + (1 - core), lax.rem(me + 2, 4)
    mesh_id = pl.DeviceIdType.MESH

    def kcopy(c, which):
        layer, part, slot = lax.shift_right_logical(jnp.int32(c), 2), lax.rem(jnp.int32(c), CHUNKS), lax.rem(jnp.int32(c), SLOTS)
        src = pl.ds(pl.multiple_of(part * CHUNK, CHUNK), CHUNK)
        if which == 0:
            return pltpu.make_async_copy(kc.at[layer, src], kbuf.at[slot], ksem.at[slot])
        return pltpu.make_async_copy(vc.at[layer, src], vbuf.at[slot], vsem.at[slot])

    def wcopy(layer, which):
        slot = lax.rem(jnp.int32(layer), 2)
        if which == 0:
            return pltpu.make_async_copy(wqkv.at[layer], qkvw.at[slot], wsem.at[slot, 0])
        return pltpu.make_async_copy(wout.at[layer], outw.at[slot], wsem.at[slot, 1])

    ffn_parts = ((wg, fg), (wu, fu), (wd, fd))

    def fcopy(k):
        return pltpu.make_async_copy(ffn_parts[k][0].at[0], ffn_parts[k][1].at[core], fsem.at[k])

    def fsend(k, idx):
        return pltpu.make_async_remote_copy(
            src_ref=ffn_parts[k][0].at[0], dst_ref=ffn_parts[k][1].at[idx], send_sem=fs_sem.at[k], recv_sem=fr_sem.at[k],
            device_id={"data": mate}, device_id_type=mesh_id)

    def send_h(layer, half, dst, slot, pos):
        rows = pl.ds(pl.multiple_of(half * HALF, HALF), HALF)
        return pltpu.make_async_remote_copy(
            src_ref=hbuf.at[layer, rows], dst_ref=hin.at[slot, pos, rows],
            send_sem=hs_sem.at[layer, half], recv_sem=hr_sem.at[slot, pos, half],
            device_id={"data": dst}, device_id_type=mesh_id)

    def send_x(layer, dst, slot, pos):
        return pltpu.make_async_remote_copy(
            src_ref=xo.at[slot, pos], dst_ref=xbuf.at[layer + 1], send_sem=xs_sem.at[slot, pos], recv_sem=xr_sem.at[layer],
            device_id={"data": dst}, device_id_type=mesh_id)

    small = [pltpu.make_async_copy(src, dst, isem.at[k]) for k, (src, dst) in enumerate(
        ((hid_in, xbuf.at[0]), (ga_in, ga), (gf_in, gf), (lens_in, lens)))]
    for cp in small:
        cp.start()
    wcopy(0, 0).start()
    for c in range(3):
        for which in range(2):
            kcopy(c, which).start()

    barrier = pltpu.get_barrier_semaphore()
    for step in range(1, 4):
        pl.semaphore_signal(barrier, inc=1, device_id={"data": lax.rem(me + step, 4)}, device_id_type=mesh_id)
    for cp in small:
        cp.wait()

    pick = (lax.broadcasted_iota(jnp.int32, (ROWS * 8, ROWS), 0) // 8 == lax.broadcasted_iota(jnp.int32, (ROWS * 8, ROWS), 1))
    lrow = jnp.broadcast_to(lens[...].astype(F32), (HD, ROWS)).astype(BF16)
    len3[...] = 2.0 * lax.dot_general(pick.astype(F32).astype(BF16), lrow, NT, preferred_element_type=F32)
    zrow = jnp.zeros((ROWS, HD), F32)
    for j in (6, 7):
        for ref in (q3, k3, v3):
            ref[pl.ds(j, ROWS, stride=8), :] = zrow
    pl.semaphore_wait(barrier, 3)

    @pl.when(me == 1)
    def _():
        fsend(0, core).start()

    def is_local(layer):
        return (chip == layer // 2) & ((layer > 0) | (me == 0))

    def layer_step(layer, carry):
        wslot = lax.rem(jnp.int32(layer), 2)
        local = is_local(layer)
        dst = jnp.where(layer == 0, 0, peer)
        slot = jnp.where((layer == 0) & (me == 1), 0, 2 * wslot + 1)
        pos = jnp.where(layer == 0, core, 0)
        wcopy(layer, 0).wait()

        @pl.when((layer > 0) & jnp.logical_not(is_local(layer - 1)))
        def _():
            send_x(layer - 1, me, 0, 0).wait_recv()

        normed = rms(xbuf[layer], ga[pl.ds(layer, 1), :])
        qkv = jnp.dot(normed, qkvw[wslot], preferred_element_type=F32).astype(BF16).astype(F32)
        for j in range(HEADS):
            rows8 = pl.ds(j, ROWS, stride=8)
            kv = j * 2 // HEADS
            q3[rows8, :] = qkv[:, j * HD:(j + 1) * HD]
            k3[rows8, :] = qkv[:, (HEADS + kv) * HD:(HEADS + kv + 1) * HD]
            v3[rows8, :] = qkv[:, (HEADS + 2 + kv) * HD:(HEADS + 3 + kv) * HD]

        def refill(c, ok=True):
            @pl.when((c < LAYERS * CHUNKS) & ok)
            def _():
                for which in range(2):
                    kcopy(c, which).start()

        col8 = lax.broadcasted_iota(jnp.int32, (8, 2 * CACHE), 1)
        kv8 = jnp.where(lax.broadcasted_iota(jnp.int32, (8, 2 * CACHE), 0) < HEADS // 2, 0, 1)
        cols8 = jnp.where((col8 & 1) == kv8, col8.astype(F32), 4.0 * CACHE)[None]

        def chunk_math(part):
            cslot = lax.rem(layer * CHUNKS + part, SLOTS)
            rows = pl.ds(pl.multiple_of(part * (CHUNK * 8), CHUNK * 8), CHUNK * 8)
            qc = q3[rows, :]
            s_self = jnp.sum(qc * k3[rows, :], axis=-1, keepdims=True).reshape(CHUNK, 8, 1)
            zero = jnp.zeros((8, HD), F32)
            scores = []
            for i in range(CHUNK // 2):
                qa = qc[16 * i:16 * i + 8]
                qb = qc[16 * i + 8:16 * i + 16]
                lhs = jnp.concatenate([jnp.concatenate([qa, zero], 1), jnp.concatenate([zero, qb], 1)], 0).astype(BF16)
                keys = jnp.concatenate([kbuf[cslot, 2 * i], kbuf[cslot, 2 * i + 1]], 1)
                scores.append(lax.dot_general(lhs, keys, NT, preferred_element_type=F32))
            s = jnp.concatenate(scores, 0).reshape(CHUNK, 8, 2 * CACHE)
            lim = jnp.concatenate([len3[rows, :].reshape(CHUNK, 8, HD)] * (2 * CACHE // HD), 2)
            s = jnp.where(cols8 < lim, s, -1e30 * HD ** 0.5)
            top = jnp.maximum(jnp.max(s, axis=-1, keepdims=True), s_self)
            e = jnp.exp2((s - top) * EXP_SCALE)
            e_self = jnp.exp2((s_self - top) * EXP_SCALE)
            inv = 1.0 / (jnp.sum(e, axis=-1, keepdims=True) + e_self)
            p = (e * inv).reshape(CHUNK * 8, 2 * CACHE).astype(BF16)
            self_out = (e_self * inv).astype(BF16).astype(F32).reshape(CHUNK * 8, 1) * v3[rows, :]
            outs = []
            for i in range(CHUNK // 2):
                vals = jnp.concatenate([vbuf[cslot, 2 * i], vbuf[cslot, 2 * i + 1]], 1)
                o = jnp.dot(p[16 * i:16 * i + 16], vals, preferred_element_type=F32)
                outs += [o[0:8, 0:HD], o[8:16, HD:2 * HD]]
            o3[rows, :] = jnp.concatenate(outs, 0) + self_out

        def chunk_pair(part):
            @pl.when(layer == 0)
            def _():
                def one(k, carry):
                    for which in range(2):
                        kcopy(part + k, which).wait()
                    chunk_math(part + k)
                    return carry

                lax.fori_loop(0, 2, one, 0)

            @pl.when(layer > 0)
            def _():
                for k in range(2):
                    for which in range(2):
                        kcopy(layer * CHUNKS + part + k, which).wait()
                for k in range(2):
                    chunk_math(part + k)

        def half_att(half, carry):
            @pl.when(half == 0)
            def _():
                @pl.when(layer == 0)
                def _():
                    for which in range(2):
                        kcopy(3, which).start()
                    wcopy(0, 1).start()

                @pl.when(jnp.where(me == 0, layer == 0, (chip == 1) & (layer == 1)))
                def _():
                    for k in range(3):
                        fcopy(k).start()

            @pl.when(half == 1)
            def _():
                @pl.when(layer == 0)
                def _():
                    for c in (4, 5):
                        for which in range(2):
                            kcopy(c, which).start()

                refill(layer * CHUNKS + 6)

            chunk_pair(half * (CHUNKS // 2))

            @pl.when(half == 0)
            def _():
                wcopy(layer, 1).wait()

            base = half * (HALF * 8)
            attn = jnp.concatenate([o3[pl.ds(base + j, HALF, stride=8), :] for j in range(HEADS)], 1).astype(BF16)
            proj = jnp.dot(attn, outw[wslot], preferred_element_type=F32)
            rows = pl.ds(pl.multiple_of(half * HALF, HALF), HALF)
            mid = (xbuf[layer, rows].astype(F32) + proj).astype(BF16)

            @pl.when(local)
            def _():
                hin[2 * wslot, 0, rows] = mid

            @pl.when(jnp.logical_not(local))
            def _():
                hbuf[layer, rows] = mid
                send_h(layer, half, dst, slot, pos).start()
            return carry

        lax.fori_loop(0, 2, half_att, 0)

        @pl.when(layer + 1 < LAYERS)
        def _():
            for which in range(2):
                wcopy(layer + 1, which).start()

        @pl.when((layer == 0) & (chip == 1))
        def _():
            fsend(0, core).start()

        @pl.when((layer == 0) & (me != 0))
        def _():
            fsend(1, core).start()

        @pl.when(jnp.where(chip == 0, (layer == 0) & (me == 1), layer == 1))
        def _():
            fsend(2, core).start()

        @pl.when((layer == 0) & (me == 1))
        def _():
            for k in range(3):
                fcopy(k).start()

        refill(layer * CHUNKS + 7)

        def ffn_step(turn, carry):
            serve0 = (layer == 2) | (turn == 1)
            serve1 = (layer != 2) & (turn == 0)
            serve = jnp.where(chip == 0, serve0, serve1)
            tl = jnp.where(chip == 0, jnp.where(layer == 2, 1, layer), jnp.where(layer == 1, 2, layer))
            todo0 = jnp.where(turn == 0, layer < 3, layer == 0) & ((layer > 0) | (me == 0))
            todo1 = jnp.where(turn == 0, layer > 0, layer == 3)
            todo = jnp.where(chip == 0, todo0, todo1)

            @pl.when(todo)
            def _():
                idx = lax.rem(tl, 2)
                fslot = 2 * idx + jnp.where(serve, 1, 0)
                both = tl == 0

                @pl.when(serve)
                def _():
                    for half in range(2):
                        send_h(0, half, me, fslot, 0).wait_recv()

                @pl.when(both)
                def _():
                    for half in range(2):
                        send_h(0, half, me, fslot, 1).wait_recv()

                first = jnp.where(serve, 1, 0) == chip

                @pl.when(first & (idx == core))
                def _():
                    for k in range(3):
                        fcopy(k).wait()

                @pl.when(first & (idx != core))
                def _():
                    for k in range(3):
                        fsend(k, idx).wait_recv()

                def ffn(count):
                    rows_h = hin[fslot, 0:count].reshape(count * ROWS, D)
                    n2 = rms(rows_h, gf[pl.ds(tl, 1), :])
                    zrows = slice(0, count * ROWS)
                    for b in range(FFN // FBLK):
                        cols = slice(b * FBLK, (b + 1) * FBLK)
                        a = jnp.dot(n2, fg[idx, :, cols], preferred_element_type=F32)
                        u = jnp.dot(n2, fu[idx, :, cols], preferred_element_type=F32)
                        zbuf[zrows, cols] = (a * jax.nn.sigmoid(a) * u).astype(BF16)
                    down = jnp.dot(zbuf[zrows, :], fd[idx], preferred_element_type=F32)
                    xo[fslot, 0:count] = (rows_h.astype(F32) + down).astype(BF16).reshape(count, ROWS, D)

                @pl.when(both)
                def _():
                    ffn(2)

                @pl.when(jnp.logical_not(both))
                def _():
                    ffn(1)

                @pl.when(serve)
                def _():
                    send_x(tl, peer, fslot, 0).start()

                @pl.when(jnp.logical_not(serve))
                def _():
                    xbuf[tl + 1] = xo[fslot, 0]

                @pl.when(both)
                def _():
                    send_x(tl, jnp.where(serve, 3, 1), fslot, 1).start()
            return carry

        refill(layer * CHUNKS + 8)
        lax.fori_loop(0, 2, ffn_step, 0)
        refill(layer * CHUNKS + 9)
        return carry

    lax.fori_loop(0, LAYERS, layer_step, 0)

    @pl.when(chip == 0)
    def _():
        send_x(LAYERS - 1, me, 0, 0).wait_recv()

    out[...] = xbuf[LAYERS]

    for layer in range(LAYERS):
        @pl.when(jnp.logical_not(is_local(layer)))
        def _():
            for half in range(2):
                send_h(layer, half, 0, 0, 0).wait_send()

    @pl.when(me != 0)
    def _():
        send_x(0, me, 3, 0).wait_send()
        for k in range(3):
            fsend(k, core).wait_send()

    @pl.when(chip == 1)
    def _():
        send_x(0, me, 1, 0).wait_send()

    @pl.when(me == 0)
    def _():
        for slot, pos in ((0, 1), (1, 0), (1, 1), (3, 0)):
            send_x(0, me, slot, pos).wait_send()


def solution(mesh):
    row_spec = P(('grp', 'data'), None)
    rep_spec = P()
    cache_spec = P(None, ('grp', 'data'))
    len_spec = P(('grp', 'data'))
    owned_spec = P('data')

    def per_device(hidden, w_qkv, w_out, norm_attn, norm_ffn, k_cache, v_cache, seq_lens, w_gate, w_up, w_down):
        kc = k_cache.reshape(LAYERS, ROWS, 2 * CACHE, HD)
        vc = v_cache.reshape(LAYERS, ROWS, 2 * CACHE, HD)
        vm = pl.BlockSpec(memory_space=pltpu.VMEM)
        anys = pl.BlockSpec(memory_space=pl.ANY)
        dma = pltpu.SemaphoreType.DMA
        return pl.pallas_call(
            kernel,
            out_shape=pltpu.VMEM((ROWS, D), BF16),
            in_specs=[anys] * 11,
            out_specs=vm,
            scratch_shapes=[
                pltpu.VMEM((SLOTS, CHUNK, 2 * CACHE, HD), BF16),
                pltpu.VMEM((SLOTS, CHUNK, 2 * CACHE, HD), BF16),
                pltpu.VMEM((2, D, QKV), BF16),
                pltpu.VMEM((2, D, D), BF16),
                pltpu.VMEM((2, D, FFN), BF16),
                pltpu.VMEM((2, D, FFN), BF16),
                pltpu.VMEM((2, FFN, D), BF16),
                pltpu.VMEM((ROWS * 8, HD), F32),
                pltpu.VMEM((ROWS * 8, HD), F32),
                pltpu.VMEM((ROWS * 8, HD), F32),
                pltpu.VMEM((ROWS * 8, HD), F32),
                pltpu.VMEM((ROWS * 8, HD), F32),
                pltpu.VMEM((LAYERS + 1, ROWS, D), BF16),
                pltpu.VMEM((LAYERS, ROWS, D), BF16),
                pltpu.VMEM((4, 2, ROWS, D), BF16),
                pltpu.VMEM((4, 2, ROWS, D), BF16),
                pltpu.VMEM((2 * ROWS, FFN), BF16),
                dma((SLOTS,)), dma((SLOTS,)), dma((2, 2)), dma((3,)), dma((3,)), dma((3,)),
                dma((LAYERS, 2)), dma((4, 2, 2)), dma((4, 2)), dma((LAYERS,)),
                pltpu.VMEM((LAYERS, D), F32), pltpu.VMEM((LAYERS, D), F32), pltpu.VMEM((1, ROWS), jnp.int32), dma((4,)),
            ],
            compiler_params=pltpu.CompilerParams(collective_id=0, has_side_effects=True, vmem_limit_bytes=64000000),
        )(hidden, norm_attn, norm_ffn, seq_lens.reshape(1, ROWS), w_qkv, w_out, kc, vc, w_gate, w_up, w_down)

    return jax.shard_map(per_device, mesh=mesh, in_specs=(row_spec, rep_spec, rep_spec, rep_spec, rep_spec, cache_spec, cache_spec, len_spec, owned_spec, owned_spec, owned_spec), out_specs=row_spec, check_vma=False)
```

```python
import jax
import jax.numpy as jnp
from jax import lax
from jax.experimental import pallas as pl
from jax.experimental.pallas import tpu as pltpu
from jax.sharding import PartitionSpec as P

NORM_EPS = 1e-5
EXP_SCALE = 1.4426950408889634 * 128 ** -0.5
F32 = jnp.float32
BF16 = jnp.bfloat16
LAYERS = 4
ROWS = 64
D = 768
HD = 128
HEADS = 6
CACHE = 256
QKV = 1280
FFN = 2048
CHUNK = 16
CHUNKS = ROWS // CHUNK
SLOTS = 6
HALF = ROWS // 2
FBLK = 512
NT = (((1,), (1,)), ((), ()))


def rms(rows_bf16, gain):
    vals = rows_bf16.astype(F32)
    inv = lax.rsqrt(jnp.mean(vals * vals, axis=-1, keepdims=True) + NORM_EPS)
    return (vals * inv * gain).astype(BF16)


def kernel(hid_in, ga_in, gf_in, lens_in, wqkv, wout, kc, vc, wg, wu, wd, out,
           kbuf, vbuf, qkvw, outw, fg, fu, fd, q3, k3, v3, o3, len3, xbuf, hbuf, hin, xo, zbuf,
           ksem, vsem, wsem, fsem, fs_sem, fr_sem, hs_sem, hr_sem, xs_sem, xr_sem, ga, gf, lens, isem):
    me = lax.axis_index("data")
    chip, core = lax.shift_right_logical(me, 1), lax.rem(me, 2)
    mate, peer = chip * 2 + (1 - core), lax.rem(me + 2, 4)
    mesh_id = pl.DeviceIdType.MESH

    def kcopy(c, which):
        layer, part, slot = lax.shift_right_logical(jnp.int32(c), 2), lax.rem(jnp.int32(c), CHUNKS), lax.rem(jnp.int32(c), SLOTS)
        src = pl.ds(pl.multiple_of(part * CHUNK, CHUNK), CHUNK)
        if which == 0:
            return pltpu.make_async_copy(kc.at[layer, src], kbuf.at[slot], ksem.at[slot])
        return pltpu.make_async_copy(vc.at[layer, src], vbuf.at[slot], vsem.at[slot])

    def wcopy(layer, which):
        slot = lax.rem(jnp.int32(layer), 2)
        if which == 0:
            return pltpu.make_async_copy(wqkv.at[layer], qkvw.at[slot], wsem.at[slot, 0])
        return pltpu.make_async_copy(wout.at[layer], outw.at[slot], wsem.at[slot, 1])

    ffn_parts = ((wg, fg), (wu, fu), (wd, fd))

    def fcopy(k):
        return pltpu.make_async_copy(ffn_parts[k][0].at[0], ffn_parts[k][1].at[core], fsem.at[k])

    def fsend(k, idx):
        return pltpu.make_async_remote_copy(
            src_ref=ffn_parts[k][0].at[0], dst_ref=ffn_parts[k][1].at[idx], send_sem=fs_sem.at[k], recv_sem=fr_sem.at[k],
            device_id={"data": mate}, device_id_type=mesh_id)

    def send_h(layer, half, dst, slot, pos):
        rows = pl.ds(pl.multiple_of(half * HALF, HALF), HALF)
        return pltpu.make_async_remote_copy(
            src_ref=hbuf.at[layer, rows], dst_ref=hin.at[slot, pos, rows],
            send_sem=hs_sem.at[layer, half], recv_sem=hr_sem.at[slot, pos, half],
            device_id={"data": dst}, device_id_type=mesh_id)

    def send_x(layer, dst, slot, pos):
        return pltpu.make_async_remote_copy(
            src_ref=xo.at[slot, pos], dst_ref=xbuf.at[layer + 1], send_sem=xs_sem.at[slot, pos], recv_sem=xr_sem.at[layer],
            device_id={"data": dst}, device_id_type=mesh_id)

    small = [pltpu.make_async_copy(src, dst, isem.at[k]) for k, (src, dst) in enumerate(
        ((hid_in, xbuf.at[0]), (ga_in, ga), (gf_in, gf), (lens_in, lens)))]
    for cp in small:
        cp.start()
    wcopy(0, 0).start()
    for c in range(3):
        for which in range(2):
            kcopy(c, which).start()

    barrier = pltpu.get_barrier_semaphore()
    for step in range(1, 4):
        pl.semaphore_signal(barrier, inc=1, device_id={"data": lax.rem(me + step, 4)}, device_id_type=mesh_id)
    for cp in small:
        cp.wait()

    pick = (lax.broadcasted_iota(jnp.int32, (ROWS * 8, ROWS), 0) // 8 == lax.broadcasted_iota(jnp.int32, (ROWS * 8, ROWS), 1))
    lrow = jnp.broadcast_to(lens[...].astype(F32), (HD, ROWS)).astype(BF16)
    len3[...] = 2.0 * lax.dot_general(pick.astype(F32).astype(BF16), lrow, NT, preferred_element_type=F32)
    zrow = jnp.zeros((ROWS, HD), F32)
    for j in (6, 7):
        for ref in (q3, k3, v3):
            ref[pl.ds(j, ROWS, stride=8), :] = zrow
    pl.semaphore_wait(barrier, 3)

    @pl.when(me == 1)
    def _():
        fsend(0, core).start()

    def is_local(layer):
        return (chip == layer // 2) & ((layer > 0) | (me == 0))

    def layer_step(layer, carry):
        wslot = lax.rem(jnp.int32(layer), 2)
        local = is_local(layer)
        dst = jnp.where(layer == 0, 0, peer)
        slot = jnp.where((layer == 0) & (me == 1), 0, 2 * wslot + 1)
        pos = jnp.where(layer == 0, core, 0)
        wcopy(layer, 0).wait()

        @pl.when((layer > 0) & jnp.logical_not(is_local(layer - 1)))
        def _():
            send_x(layer - 1, me, 0, 0).wait_recv()

        normed = rms(xbuf[layer], ga[pl.ds(layer, 1), :])
        qkv = jnp.dot(normed, qkvw[wslot], preferred_element_type=F32).astype(BF16).astype(F32)
        for j in range(HEADS):
            rows8 = pl.ds(j, ROWS, stride=8)
            kv = j * 2 // HEADS
            q3[rows8, :] = qkv[:, j * HD:(j + 1) * HD]
            k3[rows8, :] = qkv[:, (HEADS + kv) * HD:(HEADS + kv + 1) * HD]
            v3[rows8, :] = qkv[:, (HEADS + 2 + kv) * HD:(HEADS + 3 + kv) * HD]

        def refill(c, ok=True):
            @pl.when((c < LAYERS * CHUNKS) & ok)
            def _():
                for which in range(2):
                    kcopy(c, which).start()

        col8 = lax.broadcasted_iota(jnp.int32, (8, 2 * CACHE), 1)
        kv8 = jnp.where(lax.broadcasted_iota(jnp.int32, (8, 2 * CACHE), 0) < HEADS // 2, 0, 1)
        cols8 = jnp.where((col8 & 1) == kv8, col8.astype(F32), 4.0 * CACHE)[None]

        def chunk_math(part):
            cslot = lax.rem(layer * CHUNKS + part, SLOTS)
            rows = pl.ds(pl.multiple_of(part * (CHUNK * 8), CHUNK * 8), CHUNK * 8)
            qc = q3[rows, :]
            s_self = jnp.sum(qc * k3[rows, :], axis=-1, keepdims=True).reshape(CHUNK, 8, 1)
            zero = jnp.zeros((8, HD), F32)
            scores = []
            for i in range(CHUNK // 2):
                qa = qc[16 * i:16 * i + 8]
                qb = qc[16 * i + 8:16 * i + 16]
                lhs = jnp.concatenate([jnp.concatenate([qa, zero], 1), jnp.concatenate([zero, qb], 1)], 0).astype(BF16)
                keys = jnp.concatenate([kbuf[cslot, 2 * i], kbuf[cslot, 2 * i + 1]], 1)
                scores.append(lax.dot_general(lhs, keys, NT, preferred_element_type=F32))
            s = jnp.concatenate(scores, 0).reshape(CHUNK, 8, 2 * CACHE)
            lim = jnp.concatenate([len3[rows, :].reshape(CHUNK, 8, HD)] * (2 * CACHE // HD), 2)
            s = jnp.where(cols8 < lim, s, -1e30 * HD ** 0.5)
            top = jnp.maximum(jnp.max(s, axis=-1, keepdims=True), s_self)
            e = jnp.exp2((s - top) * EXP_SCALE)
            e_self = jnp.exp2((s_self - top) * EXP_SCALE)
            inv = 1.0 / (jnp.sum(e, axis=-1, keepdims=True) + e_self)
            p = (e * inv).reshape(CHUNK * 8, 2 * CACHE).astype(BF16)
            self_out = (e_self * inv).astype(BF16).astype(F32).reshape(CHUNK * 8, 1) * v3[rows, :]
            outs = []
            for i in range(CHUNK // 2):
                vals = jnp.concatenate([vbuf[cslot, 2 * i], vbuf[cslot, 2 * i + 1]], 1)
                o = jnp.dot(p[16 * i:16 * i + 16], vals, preferred_element_type=F32)
                outs += [o[0:8, 0:HD], o[8:16, HD:2 * HD]]
            o3[rows, :] = jnp.concatenate(outs, 0) + self_out

        def chunk_pair(part):
            @pl.when(layer == 0)
            def _():
                def one(k, carry):
                    for which in range(2):
                        kcopy(part + k, which).wait()
                    chunk_math(part + k)
                    return carry

                lax.fori_loop(0, 2, one, 0)

            @pl.when(layer > 0)
            def _():
                for k in range(2):
                    for which in range(2):
                        kcopy(layer * CHUNKS + part + k, which).wait()
                for k in range(2):
                    chunk_math(part + k)

        def half_att(half, carry):
            @pl.when(half == 0)
            def _():
                @pl.when(layer == 0)
                def _():
                    for which in range(2):
                        kcopy(3, which).start()
                    wcopy(0, 1).start()

                @pl.when(jnp.where(me == 0, layer == 0, (chip == 1) & (layer == 1)))
                def _():
                    for k in range(3):
                        fcopy(k).start()

            @pl.when(half == 1)
            def _():
                refill(jnp.where(layer == 0, CHUNKS, layer * CHUNKS + 6))

            chunk_pair(half * (CHUNKS // 2))

            @pl.when(half == 0)
            def _():
                wcopy(layer, 1).wait()

            base = half * (HALF * 8)
            attn = jnp.concatenate([o3[pl.ds(base + j, HALF, stride=8), :] for j in range(HEADS)], 1).astype(BF16)
            proj = jnp.dot(attn, outw[wslot], preferred_element_type=F32)
            rows = pl.ds(pl.multiple_of(half * HALF, HALF), HALF)
            mid = (xbuf[layer, rows].astype(F32) + proj).astype(BF16)

            @pl.when(local)
            def _():
                hin[2 * wslot, 0, rows] = mid

            @pl.when(jnp.logical_not(local))
            def _():
                hbuf[layer, rows] = mid
                send_h(layer, half, dst, slot, pos).start()
            return carry

        lax.fori_loop(0, 2, half_att, 0)

        def next_weights():
            for which in range(2):
                wcopy(layer + 1, which).start()

        @pl.when((layer + 1 < LAYERS) & ((layer != 2) | (chip == 1)))
        def _():
            next_weights()

        @pl.when((layer == 0) & (chip == 1))
        def _():
            fsend(0, core).start()

        @pl.when((layer == 0) & (me != 0))
        def _():
            fsend(1, core).start()

        @pl.when(jnp.where(chip == 0, (layer == 0) & (me == 1), layer == 1))
        def _():
            fsend(2, core).start()

        @pl.when((layer == 0) & (me == 1))
        def _():
            for k in range(3):
                fcopy(k).start()

        refill(CHUNKS + 1, layer == 0)

        @pl.when(chip == 1)
        def _():
            refill(CHUNKS + 2, layer == 0)
            refill(layer * CHUNKS + 7)
            refill(layer * CHUNKS + 8)

        def ffn_step(turn, carry):
            serve0 = (layer == 2) | (turn == 1)
            serve1 = (layer != 2) & (turn == 0)
            serve = jnp.where(chip == 0, serve0, serve1)
            tl = jnp.where(chip == 0, jnp.where(layer == 2, 1, layer), jnp.where(layer == 1, 2, layer))
            todo0 = jnp.where(turn == 0, layer < 3, layer == 0) & ((layer > 0) | (me == 0))
            todo1 = jnp.where(turn == 0, layer > 0, layer == 3)
            todo = jnp.where(chip == 0, todo0, todo1)

            @pl.when(todo)
            def _():
                idx = lax.rem(tl, 2)
                fslot = 2 * idx + jnp.where(serve, 1, 0)
                both = tl == 0

                @pl.when(serve)
                def _():
                    for half in range(2):
                        send_h(0, half, me, fslot, 0).wait_recv()

                @pl.when(both)
                def _():
                    for half in range(2):
                        send_h(0, half, me, fslot, 1).wait_recv()

                first = jnp.where(serve, 1, 0) == chip

                @pl.when(first & (idx == core))
                def _():
                    for k in range(3):
                        fcopy(k).wait()

                @pl.when(first & (idx != core))
                def _():
                    for k in range(3):
                        fsend(k, idx).wait_recv()

                def ffn(count):
                    rows_h = hin[fslot, 0:count].reshape(count * ROWS, D)
                    n2 = rms(rows_h, gf[pl.ds(tl, 1), :])
                    zrows = slice(0, count * ROWS)
                    for b in range(FFN // FBLK):
                        cols = slice(b * FBLK, (b + 1) * FBLK)
                        a = jnp.dot(n2, fg[idx, :, cols], preferred_element_type=F32)
                        u = jnp.dot(n2, fu[idx, :, cols], preferred_element_type=F32)
                        zbuf[zrows, cols] = (a * jax.nn.sigmoid(a) * u).astype(BF16)
                    down = jnp.dot(zbuf[zrows, :], fd[idx], preferred_element_type=F32)
                    xo[fslot, 0:count] = (rows_h.astype(F32) + down).astype(BF16).reshape(count, ROWS, D)

                @pl.when(both)
                def _():
                    ffn(2)

                @pl.when(jnp.logical_not(both))
                def _():
                    ffn(1)

                @pl.when(serve)
                def _():
                    send_x(tl, peer, fslot, 0).start()

                @pl.when(jnp.logical_not(serve))
                def _():
                    xbuf[tl + 1] = xo[fslot, 0]

                @pl.when(both)
                def _():
                    send_x(tl, jnp.where(serve, 3, 1), fslot, 1).start()

            @pl.when(chip == 0)
            def _():
                @pl.when((layer == 2) & (turn == 0))
                def _():
                    next_weights()

                @pl.when((layer == 0) & (turn == 1))
                def _():
                    for which in range(2):
                        kcopy(CHUNKS + 3, which).start()

                refill(jnp.where((layer == 0) & (turn == 0), CHUNKS + 2, layer * CHUNKS + 7 + turn))
            return carry

        lax.fori_loop(0, 2, ffn_step, 0)
        refill(layer * CHUNKS + 9)
        return carry

    lax.fori_loop(0, LAYERS, layer_step, 0)

    @pl.when(chip == 0)
    def _():
        send_x(LAYERS - 1, me, 0, 0).wait_recv()

    out[...] = xbuf[LAYERS]

    for layer in range(LAYERS):
        @pl.when(jnp.logical_not(is_local(layer)))
        def _():
            for half in range(2):
                send_h(layer, half, 0, 0, 0).wait_send()

    @pl.when(me != 0)
    def _():
        send_x(0, me, 3, 0).wait_send()
        for k in range(3):
            fsend(k, core).wait_send()

    @pl.when(chip == 1)
    def _():
        send_x(0, me, 1, 0).wait_send()

    @pl.when(me == 0)
    def _():
        for slot, pos in ((0, 1), (1, 0), (1, 1), (3, 0)):
            send_x(0, me, slot, pos).wait_send()


def solution(mesh):
    row_spec = P(('grp', 'data'), None)
    rep_spec = P()
    cache_spec = P(None, ('grp', 'data'))
    len_spec = P(('grp', 'data'))
    owned_spec = P('data')

    def per_device(hidden, w_qkv, w_out, norm_attn, norm_ffn, k_cache, v_cache, seq_lens, w_gate, w_up, w_down):
        kc = k_cache.reshape(LAYERS, ROWS, 2 * CACHE, HD)
        vc = v_cache.reshape(LAYERS, ROWS, 2 * CACHE, HD)
        vm = pl.BlockSpec(memory_space=pltpu.VMEM)
        anys = pl.BlockSpec(memory_space=pl.ANY)
        dma = pltpu.SemaphoreType.DMA
        return pl.pallas_call(
            kernel,
            out_shape=pltpu.VMEM((ROWS, D), BF16),
            in_specs=[anys] * 11,
            out_specs=vm,
            scratch_shapes=[
                pltpu.VMEM((SLOTS, CHUNK, 2 * CACHE, HD), BF16),
                pltpu.VMEM((SLOTS, CHUNK, 2 * CACHE, HD), BF16),
                pltpu.VMEM((2, D, QKV), BF16),
                pltpu.VMEM((2, D, D), BF16),
                pltpu.VMEM((2, D, FFN), BF16),
                pltpu.VMEM((2, D, FFN), BF16),
                pltpu.VMEM((2, FFN, D), BF16),
                pltpu.VMEM((ROWS * 8, HD), F32),
                pltpu.VMEM((ROWS * 8, HD), F32),
                pltpu.VMEM((ROWS * 8, HD), F32),
                pltpu.VMEM((ROWS * 8, HD), F32),
                pltpu.VMEM((ROWS * 8, HD), F32),
                pltpu.VMEM((LAYERS + 1, ROWS, D), BF16),
                pltpu.VMEM((LAYERS, ROWS, D), BF16),
                pltpu.VMEM((4, 2, ROWS, D), BF16),
                pltpu.VMEM((4, 2, ROWS, D), BF16),
                pltpu.VMEM((2 * ROWS, FFN), BF16),
                dma((SLOTS,)), dma((SLOTS,)), dma((2, 2)), dma((3,)), dma((3,)), dma((3,)),
                dma((LAYERS, 2)), dma((4, 2, 2)), dma((4, 2)), dma((LAYERS,)),
                pltpu.VMEM((LAYERS, D), F32), pltpu.VMEM((LAYERS, D), F32), pltpu.VMEM((1, ROWS), jnp.int32), dma((4,)),
            ],
            compiler_params=pltpu.CompilerParams(collective_id=0, has_side_effects=True, vmem_limit_bytes=64000000),
        )(hidden, norm_attn, norm_ffn, seq_lens.reshape(1, ROWS), w_qkv, w_out, kc, vc, w_gate, w_up, w_down)

    return jax.shard_map(per_device, mesh=mesh, in_specs=(row_spec, rep_spec, rep_spec, rep_spec, rep_spec, cache_spec, cache_spec, len_spec, owned_spec, owned_spec, owned_spec), out_specs=row_spec, check_vma=False)
```

```python
import jax
import jax.numpy as jnp
from jax import lax
from jax.experimental import pallas as pl
from jax.experimental.pallas import tpu as pltpu
from jax.sharding import PartitionSpec as P

NORM_EPS = 1e-5
EXP_SCALE = 1.4426950408889634 * 128 ** -0.5
F32 = jnp.float32
BF16 = jnp.bfloat16
LAYERS = 4
ROWS = 64
D = 768
HD = 128
HEADS = 6
CACHE = 256
QKV = 1280
FFN = 2048
CHUNK = 16
CHUNKS = ROWS // CHUNK
SLOTS = 6
HALF = ROWS // 2
FBLK = 512
NT = (((1,), (1,)), ((), ()))


def rms(rows_bf16, gain):
    vals = rows_bf16.astype(F32)
    inv = lax.rsqrt(jnp.mean(vals * vals, axis=-1, keepdims=True) + NORM_EPS)
    return (vals * inv * gain).astype(BF16)


def kernel(hid_in, ga_in, gf_in, lens_in, wqkv, wout, kc, vc, wg, wu, wd, out,
           kbuf, vbuf, qkvw, outw, fg, fu, fd, q3, k3, v3, o3, len3, xbuf, hbuf, hin, xo, zbuf,
           ksem, vsem, wsem, fsem, fs_sem, fr_sem, hs_sem, hr_sem, xs_sem, xr_sem, ga, gf, lens, isem):
    me = lax.axis_index("data")
    chip, core = lax.shift_right_logical(me, 1), lax.rem(me, 2)
    mate, peer = chip * 2 + (1 - core), lax.rem(me + 2, 4)
    mesh_id = pl.DeviceIdType.MESH

    def kcopy(c, which):
        layer, part, slot = lax.shift_right_logical(jnp.int32(c), 2), lax.rem(jnp.int32(c), CHUNKS), lax.rem(jnp.int32(c), SLOTS)
        src = pl.ds(pl.multiple_of(part * CHUNK, CHUNK), CHUNK)
        if which == 0:
            return pltpu.make_async_copy(kc.at[layer, src], kbuf.at[slot], ksem.at[slot])
        return pltpu.make_async_copy(vc.at[layer, src], vbuf.at[slot], vsem.at[slot])

    def wcopy(layer, which):
        slot = lax.rem(jnp.int32(layer), 2)
        if which == 0:
            return pltpu.make_async_copy(wqkv.at[layer], qkvw.at[slot], wsem.at[slot, 0])
        return pltpu.make_async_copy(wout.at[layer], outw.at[slot], wsem.at[slot, 1])

    ffn_parts = ((wg, fg), (wu, fu), (wd, fd))

    def fcopy(k):
        return pltpu.make_async_copy(ffn_parts[k][0].at[0], ffn_parts[k][1].at[core], fsem.at[k])

    def fsend(k, idx):
        return pltpu.make_async_remote_copy(
            src_ref=ffn_parts[k][0].at[0], dst_ref=ffn_parts[k][1].at[idx], send_sem=fs_sem.at[k], recv_sem=fr_sem.at[k],
            device_id={"data": mate}, device_id_type=mesh_id)

    def send_h(layer, half, dst, slot, pos):
        rows = pl.ds(pl.multiple_of(half * HALF, HALF), HALF)
        return pltpu.make_async_remote_copy(
            src_ref=hbuf.at[layer, rows], dst_ref=hin.at[slot, pos, rows],
            send_sem=hs_sem.at[layer, half], recv_sem=hr_sem.at[slot, pos, half],
            device_id={"data": dst}, device_id_type=mesh_id)

    def send_x(layer, dst, slot, pos):
        return pltpu.make_async_remote_copy(
            src_ref=xo.at[slot, pos], dst_ref=xbuf.at[layer + 1], send_sem=xs_sem.at[slot, pos], recv_sem=xr_sem.at[layer],
            device_id={"data": dst}, device_id_type=mesh_id)

    small = [pltpu.make_async_copy(src, dst, isem.at[k]) for k, (src, dst) in enumerate(
        ((hid_in, xbuf.at[0]), (ga_in, ga), (gf_in, gf), (lens_in, lens)))]
    for cp in small:
        cp.start()
    wcopy(0, 0).start()
    for c in range(3):
        for which in range(2):
            kcopy(c, which).start()

    barrier = pltpu.get_barrier_semaphore()
    for step in range(1, 4):
        pl.semaphore_signal(barrier, inc=1, device_id={"data": lax.rem(me + step, 4)}, device_id_type=mesh_id)
    for cp in small:
        cp.wait()

    pick = (lax.broadcasted_iota(jnp.int32, (ROWS * 8, ROWS), 0) // 8 == lax.broadcasted_iota(jnp.int32, (ROWS * 8, ROWS), 1))
    lrow = jnp.broadcast_to(lens[...].astype(F32), (HD, ROWS)).astype(BF16)
    len3[...] = 2.0 * lax.dot_general(pick.astype(F32).astype(BF16), lrow, NT, preferred_element_type=F32)
    zrow = jnp.zeros((ROWS, HD), F32)
    for j in (6, 7):
        for ref in (q3, k3, v3):
            ref[pl.ds(j, ROWS, stride=8), :] = zrow
    pl.semaphore_wait(barrier, 3)

    @pl.when(me == 1)
    def _():
        fsend(0, core).start()

    def is_local(layer):
        return (chip == layer // 2) & ((layer > 0) | (me == 0))

    def layer_step(layer, carry):
        wslot = lax.rem(jnp.int32(layer), 2)
        local = is_local(layer)
        dst = jnp.where(layer == 0, 0, peer)
        slot = jnp.where((layer == 0) & (me == 1), 0, 2 * wslot + 1)
        pos = jnp.where(layer == 0, core, 0)
        wcopy(layer, 0).wait()

        @pl.when((layer > 0) & jnp.logical_not(is_local(layer - 1)))
        def _():
            send_x(layer - 1, me, 0, 0).wait_recv()

        normed = rms(xbuf[layer], ga[pl.ds(layer, 1), :])
        qkv = jnp.dot(normed, qkvw[wslot], preferred_element_type=F32).astype(BF16).astype(F32)
        for j in range(HEADS):
            rows8 = pl.ds(j, ROWS, stride=8)
            kv = j * 2 // HEADS
            q3[rows8, :] = qkv[:, j * HD:(j + 1) * HD]
            k3[rows8, :] = qkv[:, (HEADS + kv) * HD:(HEADS + kv + 1) * HD]
            v3[rows8, :] = qkv[:, (HEADS + 2 + kv) * HD:(HEADS + 3 + kv) * HD]

        def refill(c, ok=True):
            @pl.when((c < LAYERS * CHUNKS) & ok)
            def _():
                for which in range(2):
                    kcopy(c, which).start()

        col8 = lax.broadcasted_iota(jnp.int32, (8, 2 * CACHE), 1)
        kv8 = jnp.where(lax.broadcasted_iota(jnp.int32, (8, 2 * CACHE), 0) < HEADS // 2, 0, 1)
        cols8 = jnp.where((col8 & 1) == kv8, col8.astype(F32), 4.0 * CACHE)[None]

        def chunk_math(part):
            cslot = lax.rem(layer * CHUNKS + part, SLOTS)
            rows = pl.ds(pl.multiple_of(part * (CHUNK * 8), CHUNK * 8), CHUNK * 8)
            qc = q3[rows, :]
            s_self = jnp.sum(qc * k3[rows, :], axis=-1, keepdims=True).reshape(CHUNK, 8, 1)
            zero = jnp.zeros((8, HD), F32)
            scores = []
            for i in range(CHUNK // 2):
                qa = qc[16 * i:16 * i + 8]
                qb = qc[16 * i + 8:16 * i + 16]
                lhs = jnp.concatenate([jnp.concatenate([qa, zero], 1), jnp.concatenate([zero, qb], 1)], 0).astype(BF16)
                keys = jnp.concatenate([kbuf[cslot, 2 * i], kbuf[cslot, 2 * i + 1]], 1)
                scores.append(lax.dot_general(lhs, keys, NT, preferred_element_type=F32))
            s = jnp.concatenate(scores, 0).reshape(CHUNK, 8, 2 * CACHE)
            lim = jnp.concatenate([len3[rows, :].reshape(CHUNK, 8, HD)] * (2 * CACHE // HD), 2)
            s = jnp.where(cols8 < lim, s, -1e30 * HD ** 0.5)
            top = jnp.maximum(jnp.max(s, axis=-1, keepdims=True), s_self)
            e = jnp.exp2((s - top) * EXP_SCALE)
            e_self = jnp.exp2((s_self - top) * EXP_SCALE)
            inv = 1.0 / (jnp.sum(e, axis=-1, keepdims=True) + e_self)
            p = (e * inv).reshape(CHUNK * 8, 2 * CACHE).astype(BF16)
            self_out = (e_self * inv).astype(BF16).astype(F32).reshape(CHUNK * 8, 1) * v3[rows, :]
            outs = []
            for i in range(CHUNK // 2):
                vals = jnp.concatenate([vbuf[cslot, 2 * i], vbuf[cslot, 2 * i + 1]], 1)
                o = jnp.dot(p[16 * i:16 * i + 16], vals, preferred_element_type=F32)
                outs += [o[0:8, 0:HD], o[8:16, HD:2 * HD]]
            o3[rows, :] = jnp.concatenate(outs, 0) + self_out

        def chunk_pair(part):
            @pl.when(layer == 0)
            def _():
                def one(k, carry):
                    for which in range(2):
                        kcopy(part + k, which).wait()
                    chunk_math(part + k)
                    return carry

                lax.fori_loop(0, 2, one, 0)

            @pl.when(layer > 0)
            def _():
                for k in range(2):
                    for which in range(2):
                        kcopy(layer * CHUNKS + part + k, which).wait()
                for k in range(2):
                    chunk_math(part + k)

        def mid_rows(base, rows, count):
            attn = jnp.concatenate([o3[pl.ds(base + j, count, stride=8), :] for j in range(HEADS)], 1).astype(BF16)
            proj = jnp.dot(attn, outw[wslot], preferred_element_type=F32)
            return (xbuf[layer, rows].astype(F32) + proj).astype(BF16)

        def half_att(half, carry):
            @pl.when(half == 0)
            def _():
                @pl.when(layer == 0)
                def _():
                    for which in range(2):
                        kcopy(3, which).start()
                    wcopy(0, 1).start()

                @pl.when(jnp.where(me == 0, layer == 0, (chip == 1) & (layer == 1)))
                def _():
                    for k in range(3):
                        fcopy(k).start()

            @pl.when(half == 1)
            def _():
                @pl.when(layer == 0)
                def _():
                    for c in (4, 5):
                        for which in range(2):
                            kcopy(c, which).start()

                refill(layer * CHUNKS + 6)

            chunk_pair(half * (CHUNKS // 2))

            @pl.when(half == 0)
            def _():
                wcopy(layer, 1).wait()

            @pl.when(jnp.logical_not(local))
            def _():
                rows = pl.ds(pl.multiple_of(half * HALF, HALF), HALF)
                hbuf[layer, rows] = mid_rows(half * (HALF * 8), rows, HALF)
                send_h(layer, half, dst, slot, pos).start()
            return carry

        lax.fori_loop(0, 2, half_att, 0)

        @pl.when(local)
        def _():
            hin[2 * wslot, 0] = mid_rows(0, pl.ds(0, ROWS), ROWS)

        @pl.when(layer + 1 < LAYERS)
        def _():
            for which in range(2):
                wcopy(layer + 1, which).start()

        @pl.when((layer == 0) & (chip == 1))
        def _():
            fsend(0, core).start()

        @pl.when((layer == 0) & (me != 0))
        def _():
            fsend(1, core).start()

        @pl.when(jnp.where(chip == 0, (layer == 0) & (me == 1), layer == 1))
        def _():
            fsend(2, core).start()

        @pl.when((layer == 0) & (me == 1))
        def _():
            for k in range(3):
                fcopy(k).start()

        refill(layer * CHUNKS + 7)

        def ffn_step(turn, carry):
            serve0 = (layer == 2) | (turn == 1)
            serve1 = (layer != 2) & (turn == 0)
            serve = jnp.where(chip == 0, serve0, serve1)
            tl = jnp.where(chip == 0, jnp.where(layer == 2, 1, layer), jnp.where(layer == 1, 2, layer))
            todo0 = jnp.where(turn == 0, layer < 3, layer == 0) & ((layer > 0) | (me == 0))
            todo1 = jnp.where(turn == 0, layer > 0, layer == 3)
            todo = jnp.where(chip == 0, todo0, todo1)

            @pl.when(todo)
            def _():
                idx = lax.rem(tl, 2)
                fslot = 2 * idx + jnp.where(serve, 1, 0)
                both = tl == 0

                @pl.when(serve)
                def _():
                    for half in range(2):
                        send_h(0, half, me, fslot, 0).wait_recv()

                @pl.when(both)
                def _():
                    for half in range(2):
                        send_h(0, half, me, fslot, 1).wait_recv()

                first = jnp.where(serve, 1, 0) == chip

                @pl.when(first & (idx == core))
                def _():
                    for k in range(3):
                        fcopy(k).wait()

                @pl.when(first & (idx != core))
                def _():
                    for k in range(3):
                        fsend(k, idx).wait_recv()

                def ffn(count):
                    rows_h = hin[fslot, 0:count].reshape(count * ROWS, D)
                    n2 = rms(rows_h, gf[pl.ds(tl, 1), :])
                    zrows = slice(0, count * ROWS)
                    for b in range(FFN // FBLK):
                        cols = slice(b * FBLK, (b + 1) * FBLK)
                        a = jnp.dot(n2, fg[idx, :, cols], preferred_element_type=F32)
                        u = jnp.dot(n2, fu[idx, :, cols], preferred_element_type=F32)
                        zbuf[zrows, cols] = (a * jax.nn.sigmoid(a) * u).astype(BF16)
                    down = jnp.dot(zbuf[zrows, :], fd[idx], preferred_element_type=F32)
                    xo[fslot, 0:count] = (rows_h.astype(F32) + down).astype(BF16).reshape(count, ROWS, D)

                @pl.when(both)
                def _():
                    ffn(2)

                @pl.when(jnp.logical_not(both))
                def _():
                    ffn(1)

                @pl.when(serve)
                def _():
                    send_x(tl, peer, fslot, 0).start()

                @pl.when(jnp.logical_not(serve))
                def _():
                    xbuf[tl + 1] = xo[fslot, 0]

                @pl.when(both)
                def _():
                    send_x(tl, jnp.where(serve, 3, 1), fslot, 1).start()
            return carry

        refill(layer * CHUNKS + 8)
        lax.fori_loop(0, 2, ffn_step, 0)
        refill(layer * CHUNKS + 9)
        return carry

    lax.fori_loop(0, LAYERS, layer_step, 0)

    @pl.when(chip == 0)
    def _():
        send_x(LAYERS - 1, me, 0, 0).wait_recv()

    out[...] = xbuf[LAYERS]

    for layer in range(LAYERS):
        @pl.when(jnp.logical_not(is_local(layer)))
        def _():
            for half in range(2):
                send_h(layer, half, 0, 0, 0).wait_send()

    @pl.when(me != 0)
    def _():
        send_x(0, me, 3, 0).wait_send()
        for k in range(3):
            fsend(k, core).wait_send()

    @pl.when(chip == 1)
    def _():
        send_x(0, me, 1, 0).wait_send()

    @pl.when(me == 0)
    def _():
        for slot, pos in ((0, 1), (1, 0), (1, 1), (3, 0)):
            send_x(0, me, slot, pos).wait_send()


def solution(mesh):
    row_spec = P(('grp', 'data'), None)
    rep_spec = P()
    cache_spec = P(None, ('grp', 'data'))
    len_spec = P(('grp', 'data'))
    owned_spec = P('data')

    def per_device(hidden, w_qkv, w_out, norm_attn, norm_ffn, k_cache, v_cache, seq_lens, w_gate, w_up, w_down):
        kc = k_cache.reshape(LAYERS, ROWS, 2 * CACHE, HD)
        vc = v_cache.reshape(LAYERS, ROWS, 2 * CACHE, HD)
        vm = pl.BlockSpec(memory_space=pltpu.VMEM)
        anys = pl.BlockSpec(memory_space=pl.ANY)
        dma = pltpu.SemaphoreType.DMA
        return pl.pallas_call(
            kernel,
            out_shape=pltpu.VMEM((ROWS, D), BF16),
            in_specs=[anys] * 11,
            out_specs=vm,
            scratch_shapes=[
                pltpu.VMEM((SLOTS, CHUNK, 2 * CACHE, HD), BF16),
                pltpu.VMEM((SLOTS, CHUNK, 2 * CACHE, HD), BF16),
                pltpu.VMEM((2, D, QKV), BF16),
                pltpu.VMEM((2, D, D), BF16),
                pltpu.VMEM((2, D, FFN), BF16),
                pltpu.VMEM((2, D, FFN), BF16),
                pltpu.VMEM((2, FFN, D), BF16),
                pltpu.VMEM((ROWS * 8, HD), F32),
                pltpu.VMEM((ROWS * 8, HD), F32),
                pltpu.VMEM((ROWS * 8, HD), F32),
                pltpu.VMEM((ROWS * 8, HD), F32),
                pltpu.VMEM((ROWS * 8, HD), F32),
                pltpu.VMEM((LAYERS + 1, ROWS, D), BF16),
                pltpu.VMEM((LAYERS, ROWS, D), BF16),
                pltpu.VMEM((4, 2, ROWS, D), BF16),
                pltpu.VMEM((4, 2, ROWS, D), BF16),
                pltpu.VMEM((2 * ROWS, FFN), BF16),
                dma((SLOTS,)), dma((SLOTS,)), dma((2, 2)), dma((3,)), dma((3,)), dma((3,)),
                dma((LAYERS, 2)), dma((4, 2, 2)), dma((4, 2)), dma((LAYERS,)),
                pltpu.VMEM((LAYERS, D), F32), pltpu.VMEM((LAYERS, D), F32), pltpu.VMEM((1, ROWS), jnp.int32), dma((4,)),
            ],
            compiler_params=pltpu.CompilerParams(collective_id=0, has_side_effects=True, vmem_limit_bytes=64000000),
        )(hidden, norm_attn, norm_ffn, seq_lens.reshape(1, ROWS), w_qkv, w_out, kc, vc, w_gate, w_up, w_down)

    return jax.shard_map(per_device, mesh=mesh, in_specs=(row_spec, rep_spec, rep_spec, rep_spec, rep_spec, cache_spec, cache_spec, len_spec, owned_spec, owned_spec, owned_spec), out_specs=row_spec, check_vma=False)
```

```python
import jax
import jax.numpy as jnp
from jax import lax
from jax.experimental import pallas as pl
from jax.experimental.pallas import tpu as pltpu
from jax.sharding import PartitionSpec as P

NORM_EPS = 1e-5
EXP_SCALE = 1.4426950408889634 * 128 ** -0.5
F32 = jnp.float32
BF16 = jnp.bfloat16
LAYERS = 4
ROWS = 64
D = 768
HD = 128
HEADS = 6
CACHE = 256
QKV = 1280
FFN = 2048
CHUNK = 16
CHUNKS = ROWS // CHUNK
SLOTS = 6
HALF = ROWS // 2
FBLK = 512
NT = (((1,), (1,)), ((), ()))


def rms(rows_bf16, gain):
    vals = rows_bf16.astype(F32)
    inv = lax.rsqrt(jnp.mean(vals * vals, axis=-1, keepdims=True) + NORM_EPS)
    return (vals * inv * gain).astype(BF16)


def kernel(hid_in, ga_in, gf_in, lens_in, wqkv, wout, kc, vc, wg, wu, wd, out,
           kbuf, vbuf, qkvw, outw, fg, fu, fd, q3, k3, v3, o3, len3, xbuf, hbuf, hin, xo, zbuf,
           ksem, vsem, wsem, fsem, fs_sem, fr_sem, hs_sem, hr_sem, xs_sem, xr_sem, ga, gf, lens, isem):
    me = lax.axis_index("data")
    chip, core = lax.shift_right_logical(me, 1), lax.rem(me, 2)
    mate, peer = chip * 2 + (1 - core), 3 - me
    mesh_id = pl.DeviceIdType.MESH

    def kcopy(c, which):
        layer, part, slot = lax.shift_right_logical(jnp.int32(c), 2), lax.rem(jnp.int32(c), CHUNKS), lax.rem(jnp.int32(c), SLOTS)
        src = pl.ds(pl.multiple_of(part * CHUNK, CHUNK), CHUNK)
        if which == 0:
            return pltpu.make_async_copy(kc.at[layer, src], kbuf.at[slot], ksem.at[slot])
        return pltpu.make_async_copy(vc.at[layer, src], vbuf.at[slot], vsem.at[slot])

    def wcopy(layer, which):
        slot = lax.rem(jnp.int32(layer), 2)
        if which == 0:
            return pltpu.make_async_copy(wqkv.at[layer], qkvw.at[slot], wsem.at[slot, 0])
        return pltpu.make_async_copy(wout.at[layer], outw.at[slot], wsem.at[slot, 1])

    ffn_parts = ((wg, fg), (wu, fu), (wd, fd))

    def fcopy(k):
        return pltpu.make_async_copy(ffn_parts[k][0].at[0], ffn_parts[k][1].at[core], fsem.at[k])

    def fsend(k, idx):
        return pltpu.make_async_remote_copy(
            src_ref=ffn_parts[k][0].at[0], dst_ref=ffn_parts[k][1].at[idx], send_sem=fs_sem.at[k], recv_sem=fr_sem.at[k],
            device_id={"data": mate}, device_id_type=mesh_id)

    def send_h(layer, half, dst, slot, pos):
        rows = pl.ds(pl.multiple_of(half * HALF, HALF), HALF)
        return pltpu.make_async_remote_copy(
            src_ref=hbuf.at[layer, rows], dst_ref=hin.at[slot, pos, rows],
            send_sem=hs_sem.at[layer, half], recv_sem=hr_sem.at[slot, pos, half],
            device_id={"data": dst}, device_id_type=mesh_id)

    def send_x(layer, dst, slot, pos):
        return pltpu.make_async_remote_copy(
            src_ref=xo.at[slot, pos], dst_ref=xbuf.at[layer + 1], send_sem=xs_sem.at[slot, pos], recv_sem=xr_sem.at[layer],
            device_id={"data": dst}, device_id_type=mesh_id)

    small = [pltpu.make_async_copy(src, dst, isem.at[k]) for k, (src, dst) in enumerate(
        ((hid_in, xbuf.at[0]), (ga_in, ga), (gf_in, gf), (lens_in, lens)))]
    for cp in small:
        cp.start()
    wcopy(0, 0).start()
    for c in range(3):
        for which in range(2):
            kcopy(c, which).start()

    barrier = pltpu.get_barrier_semaphore()
    for step in range(1, 4):
        pl.semaphore_signal(barrier, inc=1, device_id={"data": lax.rem(me + step, 4)}, device_id_type=mesh_id)
    for cp in small:
        cp.wait()

    pick = (lax.broadcasted_iota(jnp.int32, (ROWS * 8, ROWS), 0) // 8 == lax.broadcasted_iota(jnp.int32, (ROWS * 8, ROWS), 1))
    lrow = jnp.broadcast_to(lens[...].astype(F32), (HD, ROWS)).astype(BF16)
    len3[...] = 2.0 * lax.dot_general(pick.astype(F32).astype(BF16), lrow, NT, preferred_element_type=F32)
    zrow = jnp.zeros((ROWS, HD), F32)
    for j in (6, 7):
        for ref in (q3, k3, v3):
            ref[pl.ds(j, ROWS, stride=8), :] = zrow
    pl.semaphore_wait(barrier, 3)

    @pl.when(me == 1)
    def _():
        fsend(0, core).start()

    def is_local(layer):
        return (chip == layer // 2) & ((layer > 0) | (me == 0))

    def layer_step(layer, carry):
        wslot = lax.rem(jnp.int32(layer), 2)
        local = is_local(layer)
        dst = jnp.where(layer == 0, 0, peer)
        slot = jnp.where((layer == 0) & (me == 1), 0, 2 * wslot + 1)
        pos = jnp.where(layer == 0, core, 0)
        wcopy(layer, 0).wait()

        @pl.when((layer > 0) & jnp.logical_not(is_local(layer - 1)))
        def _():
            send_x(layer - 1, me, 0, 0).wait_recv()

        normed = rms(xbuf[layer], ga[pl.ds(layer, 1), :])
        qkv = jnp.dot(normed, qkvw[wslot], preferred_element_type=F32).astype(BF16).astype(F32)
        for j in range(HEADS):
            rows8 = pl.ds(j, ROWS, stride=8)
            kv = j * 2 // HEADS
            q3[rows8, :] = qkv[:, j * HD:(j + 1) * HD]
            k3[rows8, :] = qkv[:, (HEADS + kv) * HD:(HEADS + kv + 1) * HD]
            v3[rows8, :] = qkv[:, (HEADS + 2 + kv) * HD:(HEADS + 3 + kv) * HD]

        def refill(c, ok=True):
            @pl.when((c < LAYERS * CHUNKS) & ok)
            def _():
                for which in range(2):
                    kcopy(c, which).start()

        col8 = lax.broadcasted_iota(jnp.int32, (8, 2 * CACHE), 1)
        kv8 = jnp.where(lax.broadcasted_iota(jnp.int32, (8, 2 * CACHE), 0) < HEADS // 2, 0, 1)
        cols8 = jnp.where((col8 & 1) == kv8, col8.astype(F32), 4.0 * CACHE)[None]

        def chunk_math(part):
            cslot = lax.rem(layer * CHUNKS + part, SLOTS)
            rows = pl.ds(pl.multiple_of(part * (CHUNK * 8), CHUNK * 8), CHUNK * 8)
            qc = q3[rows, :]
            s_self = jnp.sum(qc * k3[rows, :], axis=-1, keepdims=True).reshape(CHUNK, 8, 1)
            zero = jnp.zeros((8, HD), F32)
            scores = []
            for i in range(CHUNK // 2):
                qa = qc[16 * i:16 * i + 8]
                qb = qc[16 * i + 8:16 * i + 16]
                lhs = jnp.concatenate([jnp.concatenate([qa, zero], 1), jnp.concatenate([zero, qb], 1)], 0).astype(BF16)
                keys = jnp.concatenate([kbuf[cslot, 2 * i], kbuf[cslot, 2 * i + 1]], 1)
                scores.append(lax.dot_general(lhs, keys, NT, preferred_element_type=F32))
            s = jnp.concatenate(scores, 0).reshape(CHUNK, 8, 2 * CACHE)
            lim = jnp.concatenate([len3[rows, :].reshape(CHUNK, 8, HD)] * (2 * CACHE // HD), 2)
            s = jnp.where(cols8 < lim, s, -1e30 * HD ** 0.5)
            top = jnp.maximum(jnp.max(s, axis=-1, keepdims=True), s_self)
            e = jnp.exp2((s - top) * EXP_SCALE)
            e_self = jnp.exp2((s_self - top) * EXP_SCALE)
            inv = 1.0 / (jnp.sum(e, axis=-1, keepdims=True) + e_self)
            p = (e * inv).reshape(CHUNK * 8, 2 * CACHE).astype(BF16)
            self_out = (e_self * inv).astype(BF16).astype(F32).reshape(CHUNK * 8, 1) * v3[rows, :]
            outs = []
            for i in range(CHUNK // 2):
                vals = jnp.concatenate([vbuf[cslot, 2 * i], vbuf[cslot, 2 * i + 1]], 1)
                o = jnp.dot(p[16 * i:16 * i + 16], vals, preferred_element_type=F32)
                outs += [o[0:8, 0:HD], o[8:16, HD:2 * HD]]
            o3[rows, :] = jnp.concatenate(outs, 0) + self_out

        def chunk_pair(part):
            @pl.when(layer == 0)
            def _():
                def one(k, carry):
                    for which in range(2):
                        kcopy(part + k, which).wait()
                    chunk_math(part + k)
                    return carry

                lax.fori_loop(0, 2, one, 0)

            @pl.when(layer > 0)
            def _():
                for k in range(2):
                    for which in range(2):
                        kcopy(layer * CHUNKS + part + k, which).wait()
                for k in range(2):
                    chunk_math(part + k)

        def mid_rows(base, rows, count):
            attn = jnp.concatenate([o3[pl.ds(base + j, count, stride=8), :] for j in range(HEADS)], 1).astype(BF16)
            proj = jnp.dot(attn, outw[wslot], preferred_element_type=F32)
            return (xbuf[layer, rows].astype(F32) + proj).astype(BF16)

        def half_att(half, carry):
            @pl.when(half == 0)
            def _():
                @pl.when(layer == 0)
                def _():
                    for which in range(2):
                        kcopy(3, which).start()
                    wcopy(0, 1).start()

                @pl.when(jnp.where(me == 0, layer == 0, (chip == 1) & (layer == 1)))
                def _():
                    for k in range(3):
                        fcopy(k).start()

            @pl.when(half == 1)
            def _():
                @pl.when(layer == 0)
                def _():
                    for c in (4, 5):
                        for which in range(2):
                            kcopy(c, which).start()

                refill(layer * CHUNKS + 6)

            chunk_pair(half * (CHUNKS // 2))

            @pl.when(half == 0)
            def _():
                wcopy(layer, 1).wait()

            @pl.when(jnp.logical_not(local))
            def _():
                rows = pl.ds(pl.multiple_of(half * HALF, HALF), HALF)
                hbuf[layer, rows] = mid_rows(half * (HALF * 8), rows, HALF)
                send_h(layer, half, dst, slot, pos).start()
            return carry

        lax.fori_loop(0, 2, half_att, 0)

        @pl.when(local)
        def _():
            hin[2 * wslot, 0] = mid_rows(0, pl.ds(0, ROWS), ROWS)

        @pl.when(layer + 1 < LAYERS)
        def _():
            for which in range(2):
                wcopy(layer + 1, which).start()

        @pl.when((layer == 0) & (chip == 1))
        def _():
            fsend(0, core).start()

        @pl.when((layer == 0) & (me != 0))
        def _():
            fsend(1, core).start()

        @pl.when(jnp.where(chip == 0, (layer == 0) & (me == 1), layer == 1))
        def _():
            fsend(2, core).start()

        @pl.when((layer == 0) & (me == 1))
        def _():
            for k in range(3):
                fcopy(k).start()

        refill(layer * CHUNKS + 7)

        def ffn_step(turn, carry):
            serve0 = (layer == 2) | (turn == 1)
            serve1 = (layer != 2) & (turn == 0)
            serve = jnp.where(chip == 0, serve0, serve1)
            tl = jnp.where(chip == 0, jnp.where(layer == 2, 1, layer), jnp.where(layer == 1, 2, layer))
            todo0 = jnp.where(turn == 0, layer < 3, layer == 0) & ((layer > 0) | (me == 0))
            todo1 = jnp.where(turn == 0, layer > 0, layer == 3)
            todo = jnp.where(chip == 0, todo0, todo1)

            @pl.when(todo)
            def _():
                idx = lax.rem(tl, 2)
                fslot = 2 * idx + jnp.where(serve, 1, 0)
                both = tl == 0

                @pl.when(serve)
                def _():
                    for half in range(2):
                        send_h(0, half, me, fslot, 0).wait_recv()

                @pl.when(both)
                def _():
                    for half in range(2):
                        send_h(0, half, me, fslot, 1).wait_recv()

                first = jnp.where(serve, 1, 0) == chip

                @pl.when(first & (idx == core))
                def _():
                    for k in range(3):
                        fcopy(k).wait()

                @pl.when(first & (idx != core))
                def _():
                    for k in range(3):
                        fsend(k, idx).wait_recv()

                def ffn(count):
                    rows_h = hin[fslot, 0:count].reshape(count * ROWS, D)
                    n2 = rms(rows_h, gf[pl.ds(tl, 1), :])
                    zrows = slice(0, count * ROWS)
                    for b in range(FFN // FBLK):
                        cols = slice(b * FBLK, (b + 1) * FBLK)
                        a = jnp.dot(n2, fg[idx, :, cols], preferred_element_type=F32)
                        u = jnp.dot(n2, fu[idx, :, cols], preferred_element_type=F32)
                        zbuf[zrows, cols] = (a * jax.nn.sigmoid(a) * u).astype(BF16)
                    down = jnp.dot(zbuf[zrows, :], fd[idx], preferred_element_type=F32)
                    xo[fslot, 0:count] = (rows_h.astype(F32) + down).astype(BF16).reshape(count, ROWS, D)

                @pl.when(both)
                def _():
                    ffn(2)

                @pl.when(jnp.logical_not(both))
                def _():
                    ffn(1)

                @pl.when(serve)
                def _():
                    send_x(tl, jnp.where(both, 2, peer), fslot, 0).start()

                @pl.when(jnp.logical_not(serve))
                def _():
                    xbuf[tl + 1] = xo[fslot, 0]

                @pl.when(both)
                def _():
                    send_x(tl, jnp.where(serve, 3, 1), fslot, 1).start()
            return carry

        refill(layer * CHUNKS + 8)
        lax.fori_loop(0, 2, ffn_step, 0)
        refill(layer * CHUNKS + 9)
        return carry

    lax.fori_loop(0, LAYERS, layer_step, 0)

    @pl.when(chip == 0)
    def _():
        send_x(LAYERS - 1, me, 0, 0).wait_recv()

    out[...] = xbuf[LAYERS]

    for layer in range(LAYERS):
        @pl.when(jnp.logical_not(is_local(layer)))
        def _():
            for half in range(2):
                send_h(layer, half, 0, 0, 0).wait_send()

    @pl.when(me != 0)
    def _():
        send_x(0, me, 3, 0).wait_send()
        for k in range(3):
            fsend(k, core).wait_send()

    @pl.when(chip == 1)
    def _():
        send_x(0, me, 1, 0).wait_send()

    @pl.when(me == 0)
    def _():
        for slot, pos in ((0, 1), (1, 0), (1, 1), (3, 0)):
            send_x(0, me, slot, pos).wait_send()


def solution(mesh):
    row_spec = P(('grp', 'data'), None)
    rep_spec = P()
    cache_spec = P(None, ('grp', 'data'))
    len_spec = P(('grp', 'data'))
    owned_spec = P('data')

    def per_device(hidden, w_qkv, w_out, norm_attn, norm_ffn, k_cache, v_cache, seq_lens, w_gate, w_up, w_down):
        kc = k_cache.reshape(LAYERS, ROWS, 2 * CACHE, HD)
        vc = v_cache.reshape(LAYERS, ROWS, 2 * CACHE, HD)
        vm = pl.BlockSpec(memory_space=pltpu.VMEM)
        anys = pl.BlockSpec(memory_space=pl.ANY)
        dma = pltpu.SemaphoreType.DMA
        return pl.pallas_call(
            kernel,
            out_shape=pltpu.VMEM((ROWS, D), BF16),
            in_specs=[anys] * 11,
            out_specs=vm,
            scratch_shapes=[
                pltpu.VMEM((SLOTS, CHUNK, 2 * CACHE, HD), BF16),
                pltpu.VMEM((SLOTS, CHUNK, 2 * CACHE, HD), BF16),
                pltpu.VMEM((2, D, QKV), BF16),
                pltpu.VMEM((2, D, D), BF16),
                pltpu.VMEM((2, D, FFN), BF16),
                pltpu.VMEM((2, D, FFN), BF16),
                pltpu.VMEM((2, FFN, D), BF16),
                pltpu.VMEM((ROWS * 8, HD), F32),
                pltpu.VMEM((ROWS * 8, HD), F32),
                pltpu.VMEM((ROWS * 8, HD), F32),
                pltpu.VMEM((ROWS * 8, HD), F32),
                pltpu.VMEM((ROWS * 8, HD), F32),
                pltpu.VMEM((LAYERS + 1, ROWS, D), BF16),
                pltpu.VMEM((LAYERS, ROWS, D), BF16),
                pltpu.VMEM((4, 2, ROWS, D), BF16),
                pltpu.VMEM((4, 2, ROWS, D), BF16),
                pltpu.VMEM((2 * ROWS, FFN), BF16),
                dma((SLOTS,)), dma((SLOTS,)), dma((2, 2)), dma((3,)), dma((3,)), dma((3,)),
                dma((LAYERS, 2)), dma((4, 2, 2)), dma((4, 2)), dma((LAYERS,)),
                pltpu.VMEM((LAYERS, D), F32), pltpu.VMEM((LAYERS, D), F32), pltpu.VMEM((1, ROWS), jnp.int32), dma((4,)),
            ],
            compiler_params=pltpu.CompilerParams(collective_id=0, has_side_effects=True, vmem_limit_bytes=64000000),
        )(hidden, norm_attn, norm_ffn, seq_lens.reshape(1, ROWS), w_qkv, w_out, kc, vc, w_gate, w_up, w_down)

    return jax.shard_map(per_device, mesh=mesh, in_specs=(row_spec, rep_spec, rep_spec, rep_spec, rep_spec, cache_spec, cache_spec, len_spec, owned_spec, owned_spec, owned_spec), out_specs=row_spec, check_vma=False)
```
